256 devices in a mesh: data: 256 (over z, y, x, core).
Axes of the slice: x: 4, y: 4, z: 8, core: 2. Of those that a mesh axis runs over, the one named last changes fastest.
Arguments:
- w_one: float32 [6, 512, 1024], P(None, 'data')
- w_two: float32 [6, 1024, 512], P(None, 'data')
- mom_one: float32 [6, 512, 1024], P(None, 'data')
- mom_two: float32 [6, 1024, 512], P(None, 'data')
- x_zero: bfloat16 [196608, 512], P('data')
- y_zero: bfloat16 [196608, 512], P('data')
- x_one: bfloat16 [196608, 512], P('data')
- y_one: bfloat16 [196608, 512], P('data')
Outputs:
- output 1: float32 [6, 512, 1024], P(None, 'data')
- output 2: float32 [6, 1024, 512], P(None, 'data')
- output 3: float32 [6, 512, 1024], P(None, 'data')
- output 4: float32 [6, 1024, 512], P(None, 'data')
- output 5: float32 [196608], P('data')
- output 6: float32 [196608, 512], P('data')
All inputs are finite; a program needn't handle non-finite values.
Results may differ from the reference program's by a relative error of at most 0.00922473.
Values are sent between devices in bfloat16 or wider.
A program may use at most 768 MiB of HBM per device.

```python
import jax
import jax.numpy as jnp
from jax import lax

DATA_DEVS = 256
TOK_DEV = 768
LAYERS = 6
D_MODEL = 512
D_FF = 1024

BATCH = DATA_DEVS * TOK_DEV
LEARN_RATE = 0.1
MOMENTUM = 0.9


def draw_rows(key_vals, key_shift, centre, spread):
    base_vals = jax.random.normal(key_vals, (DATA_DEVS, TOK_DEV, D_MODEL), jnp.float32)
    col_shift = jax.random.normal(key_shift, (DATA_DEVS, 1, D_MODEL), jnp.float32)
    return (spread * base_vals + centre + 0.5 * col_shift).reshape(BATCH, D_MODEL).astype(jnp.bfloat16)


def setup_inputs(seed: int = 0) -> dict:
    key_list = jax.random.split(jax.random.key(seed), 16)
    w_one = jax.random.normal(key_list[0], (LAYERS, D_MODEL, D_FF), jnp.float32) * D_MODEL ** -0.5
    w_two = jax.random.normal(key_list[1], (LAYERS, D_FF, D_MODEL), jnp.float32) * (D_FF * LAYERS) ** -0.5
    scale_one = 0.3 * (D_MODEL * D_FF * LAYERS) ** -0.5
    row_one = 1.0 + 0.5 * jax.random.normal(key_list[2], (LAYERS, D_MODEL, 1), jnp.float32)
    col_one = jax.random.normal(key_list[3], (LAYERS, 1, D_FF), jnp.float32)
    mom_one = scale_one * (row_one * col_one + 0.5 * jax.random.normal(key_list[4], (LAYERS, D_MODEL, D_FF), jnp.float32))
    scale_two = 0.3 / D_MODEL
    row_two = 1.0 + 0.5 * jax.random.normal(key_list[5], (LAYERS, D_FF, 1), jnp.float32)
    col_two = jax.random.normal(key_list[6], (LAYERS, 1, D_MODEL), jnp.float32)
    mom_two = scale_two * (row_two * col_two + 0.5 * jax.random.normal(key_list[7], (LAYERS, D_FF, D_MODEL), jnp.float32))
    return {
        "w_one": w_one,
        "w_two": w_two,
        "mom_one": mom_one,
        "mom_two": mom_two,
        "x_zero": draw_rows(key_list[8], key_list[9], 0.6, 0.8),
        "y_zero": draw_rows(key_list[10], key_list[11], -0.5, 0.5),
        "x_one": draw_rows(key_list[12], key_list[13], 0.6, 0.8),
        "y_one": draw_rows(key_list[14], key_list[15], -0.5, 0.5),
    }


def run_stack(w_one_b, w_two_b, h_start):
    def layer_step(h_cur, weights):
        w_in, w_out = weights
        act_in = h_cur.astype(jnp.bfloat16)
        pre_act = jnp.dot(act_in, w_in, preferred_element_type=jnp.float32)
        hidden = jax.nn.gelu(pre_act).astype(jnp.bfloat16)
        h_next = h_cur + jnp.dot(hidden, w_out, preferred_element_type=jnp.float32)
        return h_next, (act_in, pre_act, hidden)
    return lax.scan(layer_step, h_start, (w_one_b, w_two_b))


def local_grads(w_one_b, w_two_b, x_rows, y_rows):
    h_end, saved_vals = run_stack(w_one_b, w_two_b, x_rows.astype(jnp.float32))
    d_start = (h_end - y_rows.astype(jnp.float32)) / (BATCH * D_MODEL)

    def back_step(d_state, layer_vals):
        w_in, w_out, act_in, pre_act, hidden = layer_vals
        d_low = d_state.astype(jnp.bfloat16)
        grad_out = jnp.dot(hidden.T, d_low, preferred_element_type=jnp.float32).astype(jnp.bfloat16)
        d_hidden = jnp.dot(d_low, w_out.T, preferred_element_type=jnp.float32)
        d_pre = jax.vjp(jax.nn.gelu, pre_act)[1](d_hidden)[0].astype(jnp.bfloat16)
        grad_in = jnp.dot(act_in.T, d_pre, preferred_element_type=jnp.float32).astype(jnp.bfloat16)
        d_next = d_state + jnp.dot(d_pre, w_in.T, preferred_element_type=jnp.float32)
        return d_next, (grad_in, grad_out)

    act_ins, pre_acts, hiddens = saved_vals
    return lax.scan(back_step, d_start, (w_one_b, w_two_b, act_ins, pre_acts, hiddens), reverse=True)[1]


def reference(w_one, w_two, mom_one, mom_two, x_zero, y_zero, x_one, y_one):
    w_one_b = w_one.astype(jnp.bfloat16)
    w_two_b = w_two.astype(jnp.bfloat16)
    x_dev = x_zero.reshape(DATA_DEVS, TOK_DEV, D_MODEL)
    y_dev = y_zero.reshape(DATA_DEVS, TOK_DEV, D_MODEL)

    def add_device(acc_pair, row_pair):
        grad_in, grad_out = local_grads(w_one_b, w_two_b, row_pair[0], row_pair[1])
        return (acc_pair[0] + grad_in.astype(jnp.float32), acc_pair[1] + grad_out.astype(jnp.float32)), None

    zeros_pair = (jnp.zeros(w_one.shape, jnp.float32), jnp.zeros(w_two.shape, jnp.float32))
    grad_sums = lax.scan(add_device, zeros_pair, (x_dev, y_dev))[0]
    new_mom_one = MOMENTUM * mom_one + grad_sums[0].astype(jnp.bfloat16).astype(jnp.float32)
    new_mom_two = MOMENTUM * mom_two + grad_sums[1].astype(jnp.bfloat16).astype(jnp.float32)
    new_w_one = w_one - LEARN_RATE * new_mom_one
    new_w_two = w_two - LEARN_RATE * new_mom_two
    next_one_b = new_w_one.astype(jnp.bfloat16)
    next_two_b = new_w_two.astype(jnp.bfloat16)

    def device_forward(x_rows):
        return run_stack(next_one_b, next_two_b, x_rows.astype(jnp.float32))[0]

    h_last = lax.map(device_forward, x_one.reshape(DATA_DEVS, TOK_DEV, D_MODEL)).reshape(BATCH, D_MODEL)
    loss_rows = jnp.sum(jnp.square(h_last - y_one.astype(jnp.float32)), axis=1) / (2 * D_MODEL)
    return new_w_one, new_w_two, new_mom_one, new_mom_two, loss_rows, h_last
```

```python
import functools
import jax, jax.numpy as jnp
from jax import lax
from jax.experimental import pallas as pl
from jax.experimental.pallas import tpu as pltpu
from jax.sharding import PartitionSpec as P

LEARN_RATE = 0.1
MOMENTUM = 0.9
F32, BF16 = jnp.float32, jnp.bfloat16
GRID = (8, 4, 4, 2)


def start_copy(src, dst, send_sem, recv_sem, dev):
    pltpu.make_async_remote_copy(src_ref=src, dst_ref=dst, send_sem=send_sem, recv_sem=recv_sem,
                                 device_id=(dev,), device_id_type=pl.DeviceIdType.MESH).start()


def wait_bytes(ref, sem):
    pltpu.make_async_copy(ref, ref, sem).wait()


class Place:
    def __init__(self, grid):
        self.grid = grid
        nz, ny, nx, nc = grid
        me = lax.axis_index("data")
        self.me = me
        self.c = lax.rem(me, nc)
        self.x = lax.rem(me // nc, nx)
        self.y = lax.rem(me // (nc * nx), ny)
        self.z = me // (nc * nx * ny)
        self.sign = 1 - 2 * self.c
        self.size = {"z": nz, "y": ny, "x": nx}
        self.pos = {"z": self.z, "y": self.y, "x": self.x}
        self.stride = {"z": ny * nx * nc, "y": nx * nc, "x": nc}
        self.sib = me + 1 - 2 * self.c
        self.m = lax.rem(me, nc * nx)
        self.base = me - self.m

    def wrap(self, v, d):
        n = self.size[d]
        return lax.rem(v + 2 * n, n)

    def dev(self, d, v):
        return self.me + (v - self.pos[d]) * self.stride[d]


ORDERS = (("z", "x", "y"), ("z", "y", "x"), ("x", "y", "z"))


def block_of(buf, u, pl_, done, d, v):
    idx = []
    for k in ("z", "y", "x"):
        if k in done:
            idx.append(slice(None))
        elif k == d:
            idx.append(v)
        else:
            idx.append(pl_.pos[k])
    return buf.at[(u, *idx, pl_.c)]


class Gather:
    def __init__(self, place, buf, u, order, send_sem, recv_sem):
        self.p, self.buf, self.u, self.order = place, buf, u, order
        self.send_sem, self.recv_sem = send_sem, recv_sem
        n2, n3 = place.size[order[1]], place.size[order[2]]
        self.sem_of = {1: 1, 2: 1 + max(n2 - 1, 1)}
        self.last_sem = self.sem_of[2] + max(n3 - 1, 1)

    def block(self, stage, v):
        return block_of(self.buf, self.u, self.p, self.order[:stage], self.order[stage], v)

    def direct_start(self):
        p, d = self.p, self.order[0]
        own = self.block(0, p.pos[d])
        for k in range(1, p.size[d]):
            start_copy(own, own, self.send_sem.at[self.u, 0], self.recv_sem.at[self.u, 0], p.dev(d, p.wrap(p.pos[d] + k, d)))

    def many(self, stage):
        p, d = self.p, self.order[stage]
        return self.block(stage, pl.ds(0, p.size[d] - 1))

    def direct_wait(self):
        if self.p.size[self.order[0]] > 1:
            wait_bytes(self.many(0), self.recv_sem.at[self.u, 0])

    def ring_send(self, stage, way, step):
        p, d = self.p, self.order[stage]
        n = p.size[d]
        s = p.sign * way
        ref = self.block(stage, p.wrap(p.pos[d] - (step - 1) * s, d))
        sem = self.sem_of[stage] + (step - 1 if way == 1 else n // 2 + step - 1)
        start_copy(ref, ref, self.send_sem.at[self.u, stage], self.recv_sem.at[self.u, sem], p.dev(d, p.wrap(p.pos[d] + s, d)))

    def ring_wait(self, stage, way, step):
        p, d = self.p, self.order[stage]
        n = p.size[d]
        s = p.sign * way
        sem = self.sem_of[stage] + (step - 1 if way == 1 else n // 2 + step - 1)
        wait_bytes(self.block(stage, p.wrap(p.pos[d] - step * s, d)), self.recv_sem.at[self.u, sem])

    def hops(self, stage):
        n = self.p.size[self.order[stage]]
        return n // 2, (n - 1) // 2

    def ring_start(self, stage):
        far, near = self.hops(stage)
        if far:
            self.ring_send(stage, 1, 1)
        if near:
            self.ring_send(stage, -1, 1)

    def ring_step(self, stage, step):
        far, near = self.hops(stage)
        for way, n in ((1, far), (-1, near)):
            if step <= n:
                self.ring_wait(stage, way, step)
                if step < n:
                    self.ring_send(stage, way, step + 1)

    def swap_ref(self, c):
        return self.buf.at[self.u, :, :, :, c]

    def swap_start(self):
        ref = self.swap_ref(self.p.c)
        start_copy(ref, ref, self.send_sem.at[self.u, 3], self.recv_sem.at[self.u, self.last_sem], self.p.sib)

    def swap_wait(self):
        wait_bytes(self.swap_ref(1 - self.p.c), self.recv_sem.at[self.u, self.last_sem])

    def events(self):
        out = [self.direct_start]

        def first():
            self.direct_wait()
            self.ring_start(1)

        out.append(first)
        for stage in (1, 2):
            far = self.hops(stage)[0]
            for step in range(1, far + 1):
                def ev(stage=stage, step=step, last=step == far):
                    self.ring_step(stage, step)
                    if last:
                        if stage == 1:
                            self.ring_start(2)
                        else:
                            self.swap_start()
                out.append(ev)
            if far == 0:
                def ev0(stage=stage):
                    if stage == 1:
                        self.ring_start(2)
                    else:
                        self.swap_start()
                out.append(ev0)
        out.append(self.swap_wait)
        return out

    def drain(self):
        for stage in range(3):
            if self.p.size[self.order[stage]] > 1:
                wait_bytes(self.many(stage), self.send_sem.at[self.u, stage])
        wait_bytes(self.swap_ref(self.p.c), self.send_sem.at[self.u, 3])


def enter(p):
    barrier = pltpu.get_barrier_semaphore()
    peers = []
    group = p.grid[2] * p.grid[3]
    for k in range(1, group):
        peers.append(p.base + lax.rem(p.m + k, group))
    for d in ("y", "z"):
        for k in range(1, p.size[d]):
            peers.append(p.dev(d, p.wrap(p.pos[d] + k, d)))
    for peer in peers:
        pl.semaphore_signal(barrier, inc=1, device_id=(peer,), device_id_type=pl.DeviceIdType.MESH)
    pl.semaphore_wait(barrier, len(peers))


def to_tiles_start(p, src1, src2, r1, r2, sems, k0):
    group = p.grid[2] * p.grid[3]
    half = group // 2
    pltpu.make_async_copy(src1.at[:, :, pl.ds(pl.multiple_of(p.m * 128, 128), 128)], r1.at[p.m], sems.at[k0 + 1]).start()
    for k in range(1, group):
        j = lax.rem(p.m + k, group)
        start_copy(src1.at[:, :, pl.ds(pl.multiple_of(j * 128, 128), 128)], r1.at[p.m], sems.at[k0], sems.at[k0 + 1], p.base + j)
    hb = (p.m // half) * half
    mm = p.m - hb
    pltpu.make_async_copy(src2.at[:, :, pl.ds(pl.multiple_of(mm * 128, 128), 128)], r2.at[mm], sems.at[k0 + 3]).start()
    for k in range(1, half):
        j = lax.rem(mm + k, half)
        start_copy(src2.at[:, :, pl.ds(pl.multiple_of(j * 128, 128), 128)], r2.at[mm], sems.at[k0 + 2], sems.at[k0 + 3], p.base + hb + j)


def to_tiles_wait(p, r1, r2, sems, k0):
    wait_bytes(r1.at[pl.ds(0, r1.shape[0] - 1)], sems.at[k0])
    wait_bytes(r1, sems.at[k0 + 1])
    wait_bytes(r2.at[pl.ds(0, r2.shape[0] - 1)], sems.at[k0 + 2])
    wait_bytes(r2, sems.at[k0 + 3])


def to_tiles(r1, r2, tiles):
    layers = r1.shape[1]
    for l in range(layers):
        for m in range(r1.shape[0]):
            tiles[2 * l, 2 * m:2 * m + 2, :] = r1[m, l]
        for m in range(r2.shape[0]):
            tiles[2 * l + 1, 4 * m:4 * m + 4, :] = r2[m, l]

def ag_kernel(grid, w1, w2, out, wbuf, r1, r2, tiles, ssem, rsem, tsem, osem):
    p = Place(grid)
    units = wbuf.shape[0]
    enter(p)
    to_tiles_start(p, w1, w2, r1, r2, tsem, 0)
    to_tiles_wait(p, r1, r2, tsem, 0)
    to_tiles(r1, r2, tiles)
    for u in range(units):
        wbuf[u, p.z, p.y, p.x, p.c] = tiles[u].astype(BF16)
    gs = [Gather(p, wbuf, u, ORDERS[u % 3], ssem, rsem) for u in range(units)]
    todo = []
    for u, g in enumerate(gs):
        for k, ev in enumerate(g.events()):
            todo.append((2.0 * u + 3.0 * k, u, k, ev))
    todo.sort(key=lambda t: t[:3])
    for _, u, k, ev in todo:
        ev()
        if k == len(gs[u].events()) - 1:
            pltpu.make_async_copy(wbuf.at[u], out.at[u], osem.at[u]).start()
    for g in gs:
        g.drain()
    for u in range(units):
        pltpu.make_async_copy(wbuf.at[u], out.at[u], osem.at[u]).wait()

def gather_all(grid, w1, w2, cid):
    layers = w1.shape[0]
    units = 2 * layers
    group = grid[2] * grid[3]
    ANY = pl.BlockSpec(memory_space=pl.ANY)
    out = pl.pallas_call(
        functools.partial(ag_kernel, grid),
        out_shape=jax.ShapeDtypeStruct((units, *grid, 16, 128), BF16),
        in_specs=[ANY, ANY], out_specs=ANY,
        scratch_shapes=[pltpu.VMEM((units, *grid, 16, 128), BF16),
            pltpu.VMEM((group, layers, 2, 128), F32), pltpu.VMEM((group // 2, layers, 4, 128), F32),
            pltpu.VMEM((units, 16, 128), F32),
            pltpu.SemaphoreType.DMA((units, 4)), pltpu.SemaphoreType.DMA((units, 12)), pltpu.SemaphoreType.DMA((4,)),
            pltpu.SemaphoreType.DMA((units,))],
        compiler_params=pltpu.CompilerParams(collective_id=cid, has_side_effects=True, vmem_limit_bytes=40 * 2**20),
        name="weights_gather")(w1, w2)
    nz, ny, nx, nc = grid
    out = out.reshape(layers, 2, nz * ny, nx * nc, 16, 128)
    full1 = out[:, 0].transpose(0, 1, 3, 2, 4).reshape(layers, nz * ny * 16, nx * nc * 128)
    o2 = out[:, 1].reshape(layers, nz * ny, 2, nx * nc // 2, 16, 128)
    full2 = o2.transpose(0, 1, 2, 4, 3, 5).reshape(layers, nz * ny * 32, nx * nc // 2 * 128)
    return full1, full2


def run_stack(w_one_b, w_two_b, h_cur):
    saved_vals = []
    for layer_idx in range(w_one_b.shape[0]):
        act_in = h_cur.astype(jnp.bfloat16)
        pre_act = jnp.dot(act_in, w_one_b[layer_idx], preferred_element_type=jnp.float32)
        hidden, gelu_back = jax.vjp(jax.nn.gelu, pre_act)
        hidden = hidden.astype(jnp.bfloat16)
        h_cur = h_cur + jnp.dot(hidden, w_two_b[layer_idx], preferred_element_type=jnp.float32)
        saved_vals.append((act_in, hidden, gelu_back))
    return h_cur, saved_vals


def layer_grads(d_state, w_out, layer_vals):
    act_in, hidden, gelu_back = layer_vals
    d_low = d_state.astype(jnp.bfloat16)
    grad_out = jnp.einsum("tf,td->fd", hidden, d_low, preferred_element_type=jnp.float32).astype(jnp.bfloat16)
    d_hidden = jnp.einsum("td,fd->tf", d_low, w_out, preferred_element_type=jnp.float32)
    d_pre = gelu_back(d_hidden)[0].astype(jnp.bfloat16)
    grad_in = jnp.einsum("td,tf->df", act_in, d_pre, preferred_element_type=jnp.float32).astype(jnp.bfloat16)
    return grad_in, grad_out, d_pre


def solution(mesh):
    n_dev = mesh.shape["data"]
    w_spec = P(None, "data", None)
    row_spec = P("data", None)

    def device_step(w_one, w_two, mom_one, mom_two, x_zero, y_zero, x_one, y_one):
        layers = w_one.shape[0]
        tok_dev, d_model = x_zero.shape
        w_one_b, w_two_b = gather_all(GRID, w_one, w_two, 0)
        h_end, saved_vals = run_stack(w_one_b, w_two_b, x_zero.astype(jnp.float32))
        d_state = (h_end - y_zero.astype(jnp.float32)) / (n_dev * tok_dev * d_model)
        shard_in = [None] * layers
        shard_out = [None] * layers
        for layer_idx in reversed(range(layers)):
            grad_in, grad_out, d_pre = layer_grads(d_state, w_two_b[layer_idx], saved_vals[layer_idx])
            shard_out[layer_idx] = lax.psum_scatter(grad_out, "data", scatter_dimension=0, tiled=True)
            shard_in[layer_idx] = lax.psum_scatter(grad_in, "data", scatter_dimension=0, tiled=True)
            if layer_idx > 0:
                d_state = d_state + jnp.einsum("tf,df->td", d_pre, w_one_b[layer_idx], preferred_element_type=jnp.float32)
        new_mom_one = MOMENTUM * mom_one + jnp.stack(shard_in).astype(jnp.float32)
        new_mom_two = MOMENTUM * mom_two + jnp.stack(shard_out).astype(jnp.float32)
        new_w_one = w_one - LEARN_RATE * new_mom_one
        new_w_two = w_two - LEARN_RATE * new_mom_two
        next_one_b, next_two_b = gather_all(GRID, new_w_one, new_w_two, 1)
        h_last = run_stack(next_one_b, next_two_b, x_one.astype(jnp.float32))[0]
        loss_rows = jnp.sum(jnp.square(h_last - y_one.astype(jnp.float32)), axis=1) / (2 * d_model)
        return new_w_one, new_w_two, new_mom_one, new_mom_two, loss_rows, h_last

    return jax.shard_map(device_step, mesh=mesh, in_specs=(w_spec, w_spec, w_spec, w_spec, row_spec, row_spec, row_spec, row_spec), out_specs=(w_spec, w_spec, w_spec, w_spec, P("data"), row_spec), check_vma=False)
```

```python
import functools
import jax
import jax.numpy as jnp
from jax import lax
from jax.experimental import pallas as pl
from jax.experimental.pallas import tpu as pltpu
from jax.sharding import PartitionSpec as P

LEARN_RATE = 0.1
MOMENTUM = 0.9
F32, BF16 = jnp.float32, jnp.bfloat16
GRID = (8, 4, 4, 2)
ORDERS = (("z", "x", "y"), ("z", "y", "x"), ("x", "y", "z"))
GELU_SCALE = 0.7978845608028654
GELU_CUBE = 0.044715
ROWS = 256
G_SLOTS = 6
LANES = 128
SPILLED = 4


def start_copy(src, dst, send_sem, recv_sem, dev):
    pltpu.make_async_remote_copy(src_ref=src, dst_ref=dst, send_sem=send_sem, recv_sem=recv_sem,
                                 device_id=(dev,), device_id_type=pl.DeviceIdType.MESH).start()


def wait_bytes(ref, sem):
    pltpu.make_async_copy(ref, ref, sem).wait()


class Place:
    def __init__(self, grid):
        self.grid = grid
        nz, ny, nx, nc = grid
        me = lax.axis_index("data")
        self.me = me
        self.c = lax.rem(me, nc)
        self.x = lax.rem(me // nc, nx)
        self.y = lax.rem(me // (nc * nx), ny)
        self.z = me // (nc * nx * ny)
        self.sign = 1 - 2 * self.c
        self.size = {"z": nz, "y": ny, "x": nx}
        self.pos = {"z": self.z, "y": self.y, "x": self.x}
        self.stride = {"z": ny * nx * nc, "y": nx * nc, "x": nc}
        self.sib = me + 1 - 2 * self.c
        self.m = lax.rem(me, nc * nx)
        self.base = me - self.m

    def wrap(self, v, d):
        n = self.size[d]
        return lax.rem(v + 2 * n, n)

    def dev(self, d, v):
        return self.me + (v - self.pos[d]) * self.stride[d]

    def far(self, d):
        return self.size[d] // 2

    def near(self, d):
        return (self.size[d] - 1) // 2


def block_of(buf, lead, place, done, d, v, tail=()):
    idx = []
    for k in ("z", "y", "x"):
        if k in done:
            idx.append(slice(None))
        elif k == d:
            idx.append(v)
        else:
            idx.append(place.pos[k])
    return buf.at[(*lead, *idx, *tail)]


def ring_sem(place, d, way, step):
    return step - 1 if way == 1 else place.far(d) + step - 1


class Gather:
    def __init__(self, place, buf, u, order, send_sem, recv_sem):
        self.p, self.buf, self.u, self.order = place, buf, u, order
        self.send_sem, self.recv_sem = send_sem, recv_sem
        self.first_sem = {1: 1, 2: 1 + max(place.size[order[1]] - 1, 1)}
        self.last_sem = self.first_sem[2] + max(place.size[order[2]] - 1, 1)

    def block(self, stage, v):
        return block_of(self.buf, (self.u,), self.p, self.order[:stage], self.order[stage], v, (self.p.c,))

    def many(self, stage):
        return self.block(stage, pl.ds(0, self.p.size[self.order[stage]] - 1))

    def direct_start(self):
        p, d = self.p, self.order[0]
        own = self.block(0, p.pos[d])
        for k in range(1, p.size[d]):
            start_copy(own, own, self.send_sem.at[self.u, 0], self.recv_sem.at[self.u, 0], p.dev(d, p.wrap(p.pos[d] + k, d)))

    def direct_wait(self):
        if self.p.size[self.order[0]] > 1:
            wait_bytes(self.many(0), self.recv_sem.at[self.u, 0])

    def ring_send(self, stage, way, step):
        p, d = self.p, self.order[stage]
        s = p.sign * way
        ref = self.block(stage, p.wrap(p.pos[d] - (step - 1) * s, d))
        sem = self.first_sem[stage] + ring_sem(p, d, way, step)
        start_copy(ref, ref, self.send_sem.at[self.u, stage], self.recv_sem.at[self.u, sem], p.dev(d, p.wrap(p.pos[d] + s, d)))

    def ring_wait(self, stage, way, step):
        p, d = self.p, self.order[stage]
        ref = self.block(stage, p.wrap(p.pos[d] - step * p.sign * way, d))
        wait_bytes(ref, self.recv_sem.at[self.u, self.first_sem[stage] + ring_sem(p, d, way, step)])

    def ways(self, stage):
        d = self.order[stage]
        return ((1, self.p.far(d)), (-1, self.p.near(d)))

    def ring_start(self, stage):
        for way, n in self.ways(stage):
            if n:
                self.ring_send(stage, way, 1)

    def ring_step(self, stage, step):
        for way, n in self.ways(stage):
            if step <= n:
                self.ring_wait(stage, way, step)
                if step < n:
                    self.ring_send(stage, way, step + 1)

    def swap_ref(self, c):
        return self.buf.at[self.u, :, :, :, c]

    def swap_start(self):
        ref = self.swap_ref(self.p.c)
        start_copy(ref, ref, self.send_sem.at[self.u, 3], self.recv_sem.at[self.u, self.last_sem], self.p.sib)

    def swap_wait(self):
        wait_bytes(self.swap_ref(1 - self.p.c), self.recv_sem.at[self.u, self.last_sem])

    def events(self):
        out = [[self.direct_start], [self.direct_wait]]
        for stage in (1, 2):
            out[-1].append(functools.partial(self.ring_start, stage))
            for step in range(1, self.p.far(self.order[stage]) + 1):
                out.append([functools.partial(self.ring_step, stage, step)])
        out[-1].append(self.swap_start)
        out.append([self.swap_wait])
        return out

    def drain(self):
        for stage in range(3):
            if self.p.size[self.order[stage]] > 1:
                wait_bytes(self.many(stage), self.send_sem.at[self.u, stage])
        wait_bytes(self.swap_ref(self.p.c), self.send_sem.at[self.u, 3])


def add_into(dst, *srcs):
    total = dst[...].astype(F32)
    for s in srcs:
        total = total + s[...].astype(F32)
    dst[...] = total.astype(BF16)


class Reduce:
    def __init__(self, place, g, gslot, part, rings, rows, tiles, u, order, send_sem, recv_sem):
        self.p, self.g, self.gslot, self.part, self.u, self.order = place, g, gslot, part, u, order
        self.recv = {2: lambda k: rings[0].at[rings[1], k], 1: lambda k: rows.at[u, k, pl.ds(0, place.size[order[0]])]}
        self.tiles = tiles
        self.send_sem, self.recv_sem = send_sem, recv_sem
        self.first_sem = {2: 1, 1: 1 + max(place.size[order[2]] - 1, 1)}
        self.last_sem = self.first_sem[1] + max(place.size[order[1]] - 1, 1)

    def block(self, stage, v):
        return block_of(self.part, (self.u,), self.p, self.order[:stage], self.order[stage], v)

    def swap_start(self):
        start_copy(self.g.at[self.gslot, :, :, :, 1 - self.p.c], self.part.at[self.u],
                   self.send_sem.at[self.u, 3], self.recv_sem.at[self.u, 0], self.p.sib)

    def swap_wait(self):
        wait_bytes(self.part.at[self.u], self.recv_sem.at[self.u, 0])
        p = self.p

        def add(k, _):
            add_into(self.part.at[self.u, k], self.g.at[self.gslot, k, :, :, p.c])
            return 0

        lax.fori_loop(0, p.size["z"], add, 0)
        wait_bytes(self.part.at[self.u], self.send_sem.at[self.u, 3])

    def ways(self, stage):
        d = self.order[stage]
        return ((1, self.p.far(d)), (-1, self.p.near(d)))

    def ring_send(self, stage, way, step, n):
        p, d = self.p, self.order[stage]
        s = p.sign * way
        k = ring_sem(p, d, way, step)
        src = self.block(stage, p.wrap(p.pos[d] + n * s, d)) if step == 1 else self.recv[stage](k - 1)
        start_copy(src, self.recv[stage](k), self.send_sem.at[self.u, stage],
                   self.recv_sem.at[self.u, self.first_sem[stage] + k], p.dev(d, p.wrap(p.pos[d] + s, d)))

    def ring_start(self, stage):
        for way, n in self.ways(stage):
            if n:
                self.ring_send(stage, way, 1, n)

    def ring_step(self, stage, step):
        p, d = self.p, self.order[stage]
        ends = []
        for way, n in self.ways(stage):
            if step <= n:
                k = ring_sem(p, d, way, step)
                ref = self.recv[stage](k)
                wait_bytes(ref, self.recv_sem.at[self.u, self.first_sem[stage] + k])
                if step < n:
                    add_into(ref, self.block(stage, p.wrap(p.pos[d] + (n - step) * p.sign * way, d)))
                    self.ring_send(stage, way, step + 1, n)
        if step == p.far(d):
            for way, n in self.ways(stage):
                if n:
                    ends.append(self.recv[stage](ring_sem(p, d, way, n)))
            add_into(self.block(stage, p.pos[d]), *ends)

    def direct_start(self):
        p, d = self.p, self.order[0]
        for k in range(1, p.size[d]):
            v = p.wrap(p.pos[d] + k, d)
            start_copy(self.block(0, v), self.tiles.at[self.u, k - 1], self.send_sem.at[self.u, 0],
                       self.recv_sem.at[self.u, self.last_sem], p.dev(d, v))

    def direct_sum(self):
        n = self.p.size[self.order[0]]
        if n > 1:
            wait_bytes(self.tiles.at[self.u, pl.ds(0, n - 1)], self.recv_sem.at[self.u, self.last_sem])
        total = self.block(0, self.p.pos[self.order[0]])[...].astype(F32)
        for k in range(n - 1):
            total = total + self.tiles[self.u, k].astype(F32)
        return total.astype(BF16).astype(F32)

    def events(self):
        out = [[self.swap_wait]]
        for stage in (2, 1):
            out[-1].append(functools.partial(self.ring_start, stage))
            for step in range(1, self.p.far(self.order[stage]) + 1):
                out.append([functools.partial(self.ring_step, stage, step)])
        out[-1].append(self.direct_start)
        return out

    def drain(self):
        p = self.p
        for stage in (2, 1):
            n = p.size[self.order[stage]] - 1
            if n:
                wait_bytes(self.block(stage, pl.ds(0, n)), self.send_sem.at[self.u, stage])
        n = p.size[self.order[0]] - 1
        if n:
            wait_bytes(self.tiles.at[self.u, pl.ds(0, n)], self.send_sem.at[self.u, 0])


def enter(p):
    barrier = pltpu.get_barrier_semaphore()
    group = p.grid[2] * p.grid[3]
    peers = [p.base + lax.rem(p.m + k, group) for k in range(1, group)]
    for d in ("y", "z"):
        peers += [p.dev(d, p.wrap(p.pos[d] + k, d)) for k in range(1, p.size[d])]
    for peer in peers:
        pl.semaphore_signal(barrier, inc=1, device_id=(peer,), device_id_type=pl.DeviceIdType.MESH)
    pl.semaphore_wait(barrier, len(peers))


def lanes(ref, j):
    return ref.at[:, :, pl.ds(pl.multiple_of(j * LANES, LANES), LANES)]


class Shuffle:
    def __init__(self, place, one, two, sems, k0):
        self.p, self.one, self.two = place, one, two
        self.sem = lambda k: sems.at[k0 + k]
        self.group = place.grid[2] * place.grid[3]
        self.half = self.group // 2
        self.low = (place.m // self.half) * self.half
        self.mine = place.m - self.low

    def to_tiles_start(self, src1, src2):
        p = self.p
        pltpu.make_async_copy(lanes(src1, p.m), self.one.at[p.m], self.sem(1)).start()
        pltpu.make_async_copy(lanes(src2, self.mine), self.two.at[self.mine], self.sem(3)).start()
        for k in range(1, self.group):
            j = lax.rem(p.m + k, self.group)
            start_copy(lanes(src1, j), self.one.at[p.m], self.sem(0), self.sem(1), p.base + j)
        for k in range(1, self.half):
            j = lax.rem(self.mine + k, self.half)
            start_copy(lanes(src2, j), self.two.at[self.mine], self.sem(2), self.sem(3), p.base + self.low + j)

    def drain_sends(self):
        wait_bytes(self.one.at[pl.ds(0, self.group - 1)], self.sem(0))
        wait_bytes(self.two.at[pl.ds(0, self.half - 1)], self.sem(2))

    def to_tiles_finish(self, tiles):
        wait_bytes(self.one, self.sem(1))
        wait_bytes(self.two, self.sem(3))
        for l in range(self.one.shape[1]):
            for m in range(self.group):
                tiles[2 * l, 2 * m:2 * m + 2, :] = self.one[m, l]
            for m in range(self.half):
                tiles[2 * l + 1, 4 * m:4 * m + 4, :] = self.two[m, l]

    def put_rows(self, u, tile):
        if u % 2 == 0:
            for m in range(self.group):
                self.one[m, u // 2] = tile[2 * m:2 * m + 2, :]
        else:
            for m in range(self.half):
                self.two[m, u // 2] = tile[4 * m:4 * m + 4, :]

    def to_rows_start(self, dst1, dst2):
        p = self.p
        pltpu.make_async_copy(self.one.at[p.m], lanes(dst1, p.m), self.sem(1)).start()
        pltpu.make_async_copy(self.two.at[self.mine], lanes(dst2, self.mine), self.sem(3)).start()
        for k in range(1, self.group):
            j = lax.rem(p.m + k, self.group)
            start_copy(self.one.at[j], lanes(dst1, p.m), self.sem(0), self.sem(1), p.base + j)
        for k in range(1, self.half):
            j = lax.rem(self.mine + k, self.half)
            start_copy(self.two.at[j], lanes(dst2, self.mine), self.sem(2), self.sem(3), p.base + self.low + j)

    def to_rows_finish(self):
        wait_bytes(self.one, self.sem(1))
        wait_bytes(self.two, self.sem(3))
        self.drain_sends()


def w_one_of(wbuf, l):
    nz, ny, nx, nc = wbuf.shape[1:5]
    cols = [wbuf[2 * l, :, :, m // nc, m % nc].reshape(nz * ny * 16, LANES) for m in range(nx * nc)]
    return jnp.concatenate(cols, axis=1)


def w_two_of(wbuf, l):
    nz, ny, nx, nc = wbuf.shape[1:5]
    half = nx * nc // 2
    cols = []
    for b in range(half):
        pair = [wbuf[2 * l + 1, :, :, (r * half + b) // nc, b % nc].reshape(nz * ny, 1, 16, LANES) for r in range(2)]
        cols.append(jnp.concatenate(pair, axis=1).reshape(nz * ny * 32, LANES))
    return jnp.concatenate(cols, axis=1)


def contract(a, b, da, db):
    return lax.dot_general(a, b, (((da,), (db,)), ((), ())), preferred_element_type=F32)


def gelu_and_slope(u):
    u2 = u * u
    t = jnp.tanh(GELU_SCALE * (u + GELU_CUBE * (u * u2)))
    half = 0.5 * (1.0 + t)
    slope = half + (0.5 * u) * (1.0 - t * t) * (GELU_SCALE + (3.0 * GELU_CUBE * GELU_SCALE) * u2)
    return u * half, slope


def gelu(u):
    return u * (0.5 * (1.0 + jnp.tanh(GELU_SCALE * (u + GELU_CUBE * (u * u * u)))))


def row_tiles(total, body):
    size = min(ROWS, total)
    assert total % size == 0

    def step(t, _):
        body(pl.ds(pl.multiple_of(t * size, size), size))
        return 0

    lax.fori_loop(0, total // size, step, 0)


def step_kernel(grid, batch_scale, w1, w2, m1, m2, x0, y0, x1, y1, nw1, nw2, nm1, nm2, loss, hlast, spill,
                wbuf, slope, act, hid, h, dlow, g, part, ring_ab, ring_c, rows, tiles3,
                wone, wtwo, mone, mtwo, wt, mt, lossbuf,
                gsend, grecv, rsend, rrecv, shuf, local):
    p = Place(grid)
    layers = w1.shape[0]
    units = 2 * layers
    nz, ny, nx, nc = grid
    tok, d_model = h.shape
    d_ff = hid.shape[2]

    def load(src, dst, k):
        return pltpu.make_async_copy(src, dst, local.at[k])

    loads = {"x0": load(x0, act.at[0], 0), "y0": load(y0, dlow, 1),
             "x1": load(x1, act.at[layers - 1], 2), "y1": load(y1, act.at[layers - 2], 3)}
    loads["x0"].start()
    loads["y0"].start()
    enter(p)
    wshuf = Shuffle(p, wone, wtwo, shuf, 0)
    mshuf = Shuffle(p, mone, mtwo, shuf, 4)
    wshuf.to_tiles_start(w1, w2)
    mshuf.to_tiles_start(m1, m2)

    def own_tile(u):
        wbuf[u, p.z, p.y, p.x, p.c] = wt[u].astype(BF16)

    wshuf.to_tiles_finish(wt)
    for u in range(units):
        own_tile(u)
    loads["x0"].wait()
    h[...] = act[0].astype(F32)

    def spill_copy(l):
        return load(slope.at[l % 2], spill.at[l], 4 + l)

    def unspill_copy(l):
        return load(spill.at[l], slope.at[l % 2], 4 + l)

    def forward_one(l):
        if 2 <= l < SPILLED + 2 and l - 2 < SPILLED:
            spill_copy(l - 2).wait()

        def body(r):
            a = h[r, :].astype(BF16)
            if l:
                act[l, r, :] = a
            z, s = gelu_and_slope(jnp.dot(a, w_one_of(wbuf, l), preferred_element_type=F32))
            z = z.astype(BF16)
            slope[l % 2, r, :] = s
            hid[l, r, :] = z
            h[r, :] += jnp.dot(z, w_two_of(wbuf, l), preferred_element_type=F32)

        row_tiles(tok, body)
        if l < SPILLED and l + 2 < layers:
            spill_copy(l).start()

    def loss_slope():
        loads["y0"].wait()

        def body(r):
            d = (h[r, :] - dlow[r, :].astype(F32)) * batch_scale
            h[r, :] = d
            dlow[r, :] = d.astype(BF16)

        row_tiles(tok, body)

    gather_args = lambda u: (p, wbuf, u, ORDERS[u % 3], gsend, grecv)
    first = [Gather(*gather_args(u)) for u in range(units)]
    again = [Gather(*gather_args(u)) for u in range(units)]
    red = []
    for u in range(units):
        ring = (ring_c, u // 3) if u % 3 == 2 else (ring_ab, 2 * (u // 3) + u % 3)
        red.append(Reduce(p, g, (units - 1 - u) % G_SLOTS, part, ring, rows, tiles3, u, ORDERS[u % 3], rsend, rrecv))

    def grad_two(l):
        slot = red[2 * l + 1].gslot
        size = min(256, d_ff)
        zs = size // (ny * 32)

        def step(j, _):
            cols = pl.ds(pl.multiple_of(j * size, size), size)
            v = contract(hid[l, :, cols], dlow[...], 0, 0).astype(BF16).reshape(zs, ny, 2, 16, d_model)
            for b in range(nx * nc // 2):
                for r in range(2):
                    g[slot, pl.ds(j * zs, zs), :, (r * nx * nc // 2 + b) // nc, b % nc] = v[:, :, r, :, LANES * b:LANES * b + LANES]
            return 0

        lax.fori_loop(0, d_ff // size, step, 0)
        red[2 * l + 1].swap_start()

    def back_hidden(l):
        if l < SPILLED and l + 2 < layers:
            unspill_copy(l).wait()

        def body(r):
            q = contract(dlow[r, :], w_two_of(wbuf, l), 1, 1)
            v = (slope[l % 2, r, :] * q).astype(BF16)
            hid[l, r, :] = v
            if l:
                d = h[r, :] + contract(v, w_one_of(wbuf, l), 1, 1)
                h[r, :] = d
                dlow[r, :] = d.astype(BF16)

        row_tiles(tok, body)
        if 0 <= l - 2 < SPILLED:
            unspill_copy(l - 2).start()

    def grad_one(l):
        slot = red[2 * l].gslot
        size = min(256, d_model)
        zs = size // (ny * 16)

        def step(j, _):
            cols = pl.ds(pl.multiple_of(j * size, size), size)
            v = contract(act[l, :, cols], hid[l], 0, 0).astype(BF16).reshape(zs, ny, 16, d_ff)
            for m in range(nx * nc):
                g[slot, pl.ds(j * zs, zs), :, m // nc, m % nc] = v[:, :, :, LANES * m:LANES * m + LANES]
            return 0

        lax.fori_loop(0, d_model // size, step, 0)
        red[2 * l].swap_start()
        if l == layers - 1:
            loads["x1"].start()
        if l == layers - 2:
            loads["y1"].start()

    def update(u):
        total = red[u].direct_sum()
        mom = MOMENTUM * mt[u] + total
        w = wt[u] - LEARN_RATE * mom
        wbuf[u, p.z, p.y, p.x, p.c] = w.astype(BF16)
        wt[u] = w
        mt[u] = mom
        again[u].direct_start()

    def moments_ready():
        mshuf.to_tiles_finish(mt)
        mshuf.drain_sends()
        wshuf.drain_sends()

    def second_start():
        loads["x1"].wait()
        h[...] = act[layers - 1].astype(F32)

    def forward_two(l):
        last = l == layers - 1
        if last:
            loads["y1"].wait()

        def body(r):
            a = h[r, :].astype(BF16)
            z = gelu(jnp.dot(a, w_one_of(wbuf, l), preferred_element_type=F32)).astype(BF16)
            v = h[r, :] + jnp.dot(z, w_two_of(wbuf, l), preferred_element_type=F32)
            h[r, :] = v
            if last:
                e = v - act[layers - 2, r, :].astype(F32)
                e = e * e
                s = e[:, :LANES]
                for k in range(1, d_model // LANES):
                    s = s + e[:, LANES * k:LANES * k + LANES]
                lossbuf[:, r] = jnp.sum(s.T, axis=0, keepdims=True) * (1.0 / (2 * d_model))

        row_tiles(tok, body)

    def new_rows():
        for u in range(units):
            wshuf.put_rows(u, wt[u])
            mshuf.put_rows(u, mt[u])
        wshuf.to_rows_start(nw1, nw2)
        mshuf.to_rows_start(nm1, nm2)

    work = {}
    for u in range(units):
        for k, ev in enumerate(first[u].events()):
            work["a", u, k] = ev
        for k, ev in enumerate(red[u].events()):
            work["r", u, k] = ev
        work["u", u, 0] = [functools.partial(update, u)]
        for k, ev in enumerate(again[u].events()[1:]):
            work["b", u, k] = ev
        work["d", u, 0] = [first[u].drain]
    for l in range(layers):
        work["f", l, 0] = [functools.partial(forward_one, l)]
        work["g", l, 0] = [functools.partial(grad_two, l)]
        work["g", l, 1] = [functools.partial(back_hidden, l)]
        work["g", l, 2] = [functools.partial(grad_one, l)]
        work["s", l, 0] = [functools.partial(forward_two, l)]
    work["l", 0, 0] = [loss_slope]
    work["m", 0, 0] = [moments_ready]
    work["h", 0, 0] = [second_start]
    work["n", 0, 0] = [new_rows]
    for name in order_of(work, layers):
        for f in work[name]:
            f()
    out = [load(h, hlast, 0), load(lossbuf, loss, 1)]
    for c in out:
        c.start()
    for u in range(units):
        again[u].drain()
        red[u].drain()
    wshuf.to_rows_finish()
    mshuf.to_rows_finish()
    for c in out:
        c.wait()


def order_of(work, layers):
    units = 2 * layers
    out = []
    n = lambda tag, u: sum(1 for k in work if k[0] == tag and k[1] == u)
    for k in range(12):
        for u in range(units):
            if ("a", u, k) in work and k < n("a", u):
                out.append(("a", u, k))
    for l in range(layers):
        out.append(("f", l, 0))
    for u in range(units):
        out.append(("d", u, 0))
    out += [("m", 0, 0), ("l", 0, 0)]
    for l in reversed(range(layers)):
        out += [("g", l, 0), ("g", l, 1), ("g", l, 2)]
        out += [("r", 2 * l + 1, 0), ("r", 2 * l, 0)]
    for k in range(1, 12):
        for u in reversed(range(units)):
            if ("r", u, k) in work:
                out.append(("r", u, k))
    for u in range(units):
        out.append(("u", u, 0))
    for k in range(12):
        for u in range(units):
            if ("b", u, k) in work:
                out.append(("b", u, k))
    out.append(("h", 0, 0))
    out.append(("n", 0, 0))
    for l in range(layers):
        out.append(("s", l, 0))
    return out


def make_step(grid, layers, tok, d_model, d_ff, n_dev):
    nz, ny, nx, nc = grid
    units = 2 * layers
    group = nx * nc
    hbm = pl.BlockSpec(memory_space=pl.ANY)
    sds = jax.ShapeDtypeStruct
    tile = (16, LANES)
    dma = pltpu.SemaphoreType.DMA
    thirds = (units + 2) // 3
    outs = (sds((layers, 2, d_ff), F32), sds((layers, 4, d_model), F32), sds((layers, 2, d_ff), F32), sds((layers, 4, d_model), F32),
            sds((1, tok), F32), sds((tok, d_model), F32), sds((SPILLED, tok, d_ff), F32))
    shuffled = [pltpu.VMEM((group, layers, 2, LANES), F32), pltpu.VMEM((group // 2, layers, 4, LANES), F32)]
    scratch = [
        pltpu.VMEM((units, *grid, *tile), BF16),
        pltpu.VMEM((2, tok, d_ff), F32),
        pltpu.VMEM((layers, tok, d_model), BF16),
        pltpu.VMEM((layers, tok, d_ff), BF16),
        pltpu.VMEM((tok, d_model), F32),
        pltpu.VMEM((tok, d_model), BF16),
        pltpu.VMEM((G_SLOTS, *grid, *tile), BF16),
        pltpu.VMEM((units, nz, ny, nx, *tile), BF16),
        pltpu.VMEM((2 * thirds, nx - 1, nz, ny, *tile), BF16),
        pltpu.VMEM((thirds, nz - 1, ny, nx, *tile), BF16),
        pltpu.VMEM((units, max(ny, nx) - 1, max(nz, nx), *tile), BF16),
        pltpu.VMEM((units, max(nz, nx) - 1, *tile), BF16),
        *shuffled, *shuffled,
        pltpu.VMEM((units, *tile), F32), pltpu.VMEM((units, *tile), F32),
        pltpu.VMEM((1, tok), F32),
        dma((units, 4)), dma((units, 12)), dma((units, 4)), dma((units, 12)), dma((8,)), dma((4 + SPILLED,)),
    ]
    return pl.pallas_call(
        functools.partial(step_kernel, grid, 1.0 / (n_dev * tok * d_model)),
        out_shape=outs, in_specs=[hbm] * 8, out_specs=[hbm] * 7, scratch_shapes=scratch,
        compiler_params=pltpu.CompilerParams(collective_id=0, has_side_effects=True, vmem_limit_bytes=67043328),
        name="train_step")


def solution(mesh):
    n_dev = mesh.shape["data"]
    w_spec = P(None, "data", None)
    row_spec = P("data", None)

    def device_step(w_one, w_two, mom_one, mom_two, x_zero, y_zero, x_one, y_one):
        tok, d_model = x_zero.shape
        step = make_step(GRID, w_one.shape[0], tok, d_model, w_one.shape[2], n_dev)
        nw1, nw2, nm1, nm2, loss, h_last, _ = step(w_one, w_two, mom_one, mom_two, x_zero, y_zero, x_one, y_one)
        return nw1, nw2, nm1, nm2, loss.reshape(tok), h_last

    return jax.shard_map(device_step, mesh=mesh, in_specs=(w_spec, w_spec, w_spec, w_spec, row_spec, row_spec, row_spec, row_spec),
                         out_specs=(w_spec, w_spec, w_spec, w_spec, P("data"), row_spec), check_vma=False)
```

```python
import functools
import jax
import jax.numpy as jnp
from jax import lax
from jax.experimental import pallas as pl
from jax.experimental.pallas import tpu as pltpu
from jax.sharding import PartitionSpec as P

LEARN_RATE = 0.1
MOMENTUM = 0.9
F32, BF16 = jnp.float32, jnp.bfloat16
GRID = (8, 4, 4, 2)
ORDERS = (("z", "x", "y"), ("z", "y", "x"), ("x", "y", "z"))
GELU_SCALE = 0.7978845608028654
GELU_CUBE = 0.044715
ROWS = 256
G_SLOTS = 6
LANES = 128
SPILLED = 4

ORDER = (
    ("a", 4, 0), ("a", 11, 0), ("m", 0, 0), ("a", 2, 0), ("a", 6, 0), ("a", 3, 0), ("a", 0, 0), ("a", 1, 0), ("a", 7, 0), ("a", 5, 0), ("a", 8, 0),
    ("a", 11, 1), ("a", 9, 0), ("a", 10, 0), ("a", 2, 1), ("a", 5, 1), ("a", 8, 1), ("a", 11, 2), ("a", 4, 1), ("a", 6, 1), ("a", 2, 2), ("a", 3, 1),
    ("a", 0, 1), ("a", 5, 2), ("a", 8, 2), ("a", 11, 3), ("a", 1, 1), ("a", 7, 1), ("a", 6, 2), ("a", 2, 3), ("a", 9, 1), ("a", 3, 2), ("a", 4, 2),
    ("a", 5, 3), ("a", 10, 1), ("a", 0, 2), ("a", 8, 3), ("a", 1, 2), ("a", 6, 3), ("a", 11, 4), ("a", 7, 2), ("a", 4, 3), ("a", 2, 4), ("a", 0, 3),
    ("a", 1, 3), ("a", 5, 4), ("a", 3, 3), ("a", 7, 3), ("a", 11, 5), ("a", 8, 4), ("a", 2, 5), ("a", 10, 2), ("a", 9, 2), ("a", 0, 4), ("a", 1, 4),
    ("a", 5, 5), ("a", 11, 6), ("a", 6, 4), ("a", 4, 4), ("a", 7, 4), ("a", 3, 4), ("a", 8, 5), ("a", 0, 5), ("a", 1, 5), ("a", 9, 3), ("a", 10, 3),
    ("a", 2, 6), ("a", 5, 6), ("a", 0, 6), ("d", 0, 0), ("a", 6, 5), ("a", 1, 6), ("d", 1, 0), ("f", 0, 0), ("a", 3, 5), ("a", 11, 7), ("a", 7, 5),
    ("a", 6, 6), ("d", 6, 0), ("a", 5, 7), ("a", 2, 7), ("a", 4, 5), ("a", 9, 4), ("a", 3, 6), ("d", 3, 0), ("a", 11, 8), ("a", 8, 6), ("d", 11, 0),
    ("a", 7, 6), ("a", 10, 4), ("a", 5, 8), ("d", 5, 0), ("d", 7, 0), ("a", 2, 8), ("f", 1, 0), ("a", 4, 6), ("a", 9, 5), ("d", 4, 0), ("f", 2, 0),
    ("a", 9, 6), ("a", 10, 5), ("d", 9, 0), ("d", 2, 0), ("a", 8, 7), ("f", 3, 0), ("a", 10, 6), ("a", 8, 8), ("f", 4, 0), ("f", 5, 0), ("l", 0, 0),
    ("g", 5, 0), ("g", 5, 1), ("d", 8, 0), ("d", 10, 0), ("g", 5, 2), ("g", 4, 0), ("r", 11, 0), ("g", 4, 1), ("r", 10, 0), ("g", 4, 2), ("g", 3, 0),
    ("r", 11, 1), ("r", 9, 0), ("g", 3, 1), ("g", 3, 2), ("r", 10, 1), ("r", 8, 0), ("r", 11, 2), ("g", 2, 0), ("r", 7, 0), ("r", 9, 1), ("g", 2, 1),
    ("r", 8, 1), ("r", 6, 0), ("g", 1, 0), ("r", 11, 3), ("g", 1, 1), ("g", 0, 0), ("r", 11, 4), ("g", 0, 1), ("g", 0, 2), ("r", 11, 5), ("g", 1, 2),
    ("r", 5, 0), ("r", 6, 1), ("r", 8, 2), ("r", 9, 2), ("r", 1, 0), ("h", 0, 0), ("r", 11, 6), ("r", 0, 0), ("g", 2, 2), ("r", 2, 0), ("r", 7, 1),
    ("r", 3, 0), ("r", 9, 3), ("r", 5, 1), ("r", 4, 0), ("r", 8, 3), ("r", 2, 1), ("r", 0, 1), ("r", 6, 2), ("u", 11, 0), ("r", 5, 2), ("r", 1, 1),
    ("r", 7, 2), ("r", 8, 4), ("r", 9, 4), ("r", 3, 1), ("r", 2, 2), ("r", 0, 2), ("r", 10, 2), ("r", 4, 1), ("r", 5, 3), ("r", 7, 3), ("r", 8, 5),
    ("r", 6, 3), ("b", 11, 0), ("r", 1, 2), ("r", 3, 2), ("r", 2, 3), ("r", 0, 3), ("r", 10, 3), ("r", 5, 4), ("r", 7, 4), ("r", 8, 6), ("u", 9, 0),
    ("b", 11, 1), ("r", 4, 2), ("r", 6, 4), ("r", 1, 3), ("r", 3, 3), ("r", 2, 4), ("r", 0, 4), ("r", 5, 5), ("b", 11, 2), ("u", 8, 0), ("r", 4, 3),
    ("r", 1, 4), ("r", 3, 4), ("r", 2, 5), ("r", 5, 6), ("u", 7, 0), ("b", 9, 0), ("r", 4, 4), ("u", 6, 0), ("b", 8, 0), ("r", 2, 6), ("u", 0, 0),
    ("u", 5, 0), ("b", 11, 3), ("b", 9, 1), ("b", 8, 1), ("u", 1, 0), ("u", 3, 0), ("u", 2, 0), ("b", 7, 0), ("b", 5, 0), ("r", 10, 4), ("u", 4, 0),
    ("b", 8, 2), ("b", 9, 2), ("b", 6, 0), ("b", 0, 0), ("b", 2, 0), ("b", 5, 1), ("b", 11, 4), ("b", 6, 1), ("b", 1, 0), ("b", 0, 1), ("b", 3, 0),
    ("b", 7, 1), ("b", 8, 3), ("u", 10, 0), ("n", 0, 0), ("b", 5, 2), ("b", 2, 1), ("b", 4, 0), ("b", 1, 1), ("b", 7, 2), ("b", 0, 2), ("b", 3, 1),
    ("b", 8, 4), ("b", 2, 2), ("b", 4, 1), ("b", 1, 2), ("b", 5, 3), ("b", 9, 3), ("b", 8, 5), ("b", 10, 0), ("b", 3, 2), ("b", 4, 2), ("b", 0, 3),
    ("b", 2, 3), ("b", 9, 4), ("b", 5, 4), ("b", 1, 3), ("b", 8, 6), ("b", 9, 5), ("b", 11, 5), ("b", 2, 4), ("b", 8, 7), ("b", 10, 1), ("b", 7, 3),
    ("b", 6, 2), ("b", 3, 3), ("b", 4, 3), ("b", 5, 5), ("b", 11, 6), ("b", 0, 4), ("b", 1, 4), ("b", 10, 2), ("b", 2, 5), ("b", 11, 7), ("b", 7, 4),
    ("b", 0, 5), ("b", 1, 5), ("s", 0, 0), ("b", 5, 6), ("b", 4, 4), ("b", 2, 6), ("b", 7, 5), ("b", 3, 4), ("b", 6, 3), ("b", 5, 7), ("b", 10, 3),
    ("b", 4, 5), ("b", 2, 7), ("b", 3, 5), ("s", 1, 0), ("b", 6, 4), ("s", 2, 0), ("b", 6, 5), ("b", 10, 4), ("s", 3, 0), ("b", 10, 5), ("s", 4, 0),
    ("s", 5, 0),
)


def start_copy(src, dst, send_sem, recv_sem, dev):
    pltpu.make_async_remote_copy(src_ref=src, dst_ref=dst, send_sem=send_sem, recv_sem=recv_sem,
                                 device_id=(dev,), device_id_type=pl.DeviceIdType.MESH).start()


def wait_bytes(ref, sem):
    pltpu.make_async_copy(ref, ref, sem).wait()


class Place:
    def __init__(self, grid):
        self.grid = grid
        nz, ny, nx, nc = grid
        me = lax.axis_index("data")
        self.me = me
        self.c = lax.rem(me, nc)
        self.x = lax.rem(me // nc, nx)
        self.y = lax.rem(me // (nc * nx), ny)
        self.z = me // (nc * nx * ny)
        self.sign = 1 - 2 * self.c
        self.size = {"z": nz, "y": ny, "x": nx}
        self.pos = {"z": self.z, "y": self.y, "x": self.x}
        self.stride = {"z": ny * nx * nc, "y": nx * nc, "x": nc}
        self.sib = me + 1 - 2 * self.c
        self.m = lax.rem(me, nc * nx)
        self.base = me - self.m

    def wrap(self, v, d):
        n = self.size[d]
        return lax.rem(v + 2 * n, n)

    def dev(self, d, v):
        return self.me + (v - self.pos[d]) * self.stride[d]

    def far(self, d):
        return self.size[d] // 2

    def near(self, d):
        return (self.size[d] - 1) // 2


def block_of(buf, lead, place, done, d, v, tail=()):
    idx = []
    for k in ("z", "y", "x"):
        if k in done:
            idx.append(slice(None))
        elif k == d:
            idx.append(v)
        else:
            idx.append(place.pos[k])
    return buf.at[(*lead, *idx, *tail)]


def ring_sem(place, d, way, step):
    return step - 1 if way == 1 else place.far(d) + step - 1


class Gather:
    def __init__(self, place, buf, u, order, send_sem, recv_sem):
        self.p, self.buf, self.u, self.order = place, buf, u, order
        self.send_sem, self.recv_sem = send_sem, recv_sem
        self.first_sem = {1: 1, 2: 1 + max(place.size[order[1]] - 1, 1)}
        self.last_sem = self.first_sem[2] + max(place.size[order[2]] - 1, 1)

    def block(self, stage, v):
        return block_of(self.buf, (self.u,), self.p, self.order[:stage], self.order[stage], v, (self.p.c,))

    def many(self, stage):
        return self.block(stage, pl.ds(0, self.p.size[self.order[stage]] - 1))

    def direct_start(self):
        p, d = self.p, self.order[0]
        own = self.block(0, p.pos[d])
        for k in range(1, p.size[d]):
            start_copy(own, own, self.send_sem.at[self.u, 0], self.recv_sem.at[self.u, 0], p.dev(d, p.wrap(p.pos[d] + k, d)))

    def direct_wait(self):
        if self.p.size[self.order[0]] > 1:
            wait_bytes(self.many(0), self.recv_sem.at[self.u, 0])

    def ring_send(self, stage, way, step):
        p, d = self.p, self.order[stage]
        s = p.sign * way
        ref = self.block(stage, p.wrap(p.pos[d] - (step - 1) * s, d))
        sem = self.first_sem[stage] + ring_sem(p, d, way, step)
        start_copy(ref, ref, self.send_sem.at[self.u, stage], self.recv_sem.at[self.u, sem], p.dev(d, p.wrap(p.pos[d] + s, d)))

    def ring_wait(self, stage, way, step):
        p, d = self.p, self.order[stage]
        ref = self.block(stage, p.wrap(p.pos[d] - step * p.sign * way, d))
        wait_bytes(ref, self.recv_sem.at[self.u, self.first_sem[stage] + ring_sem(p, d, way, step)])

    def ways(self, stage):
        d = self.order[stage]
        return ((1, self.p.far(d)), (-1, self.p.near(d)))

    def ring_start(self, stage):
        for way, n in self.ways(stage):
            if n:
                self.ring_send(stage, way, 1)
        if stage == 2:
            self.swap_start(0)

    def ring_step(self, stage, step):
        for way, n in self.ways(stage):
            if step <= n:
                self.ring_wait(stage, way, step)
                if step < n:
                    self.ring_send(stage, way, step + 1)
                if stage == 2:
                    self.swap_start(step * way)

    def swap_ref(self, c):
        return self.buf.at[self.u, :, :, :, c]

    def swap_start(self, k):
        d = self.order[2]
        ref = self.block(2, self.p.wrap(self.p.pos[d] - k * self.p.sign, d))
        start_copy(ref, ref, self.send_sem.at[self.u, 3], self.recv_sem.at[self.u, self.last_sem], self.p.sib)

    def swap_wait(self):
        wait_bytes(self.swap_ref(1 - self.p.c), self.recv_sem.at[self.u, self.last_sem])

    def events(self):
        out = [[self.direct_start], [self.direct_wait]]
        for stage in (1, 2):
            out[-1].append(functools.partial(self.ring_start, stage))
            for step in range(1, self.p.far(self.order[stage]) + 1):
                out.append([functools.partial(self.ring_step, stage, step)])
        out.append([self.swap_wait])
        return out

    def drain(self):
        for stage in range(3):
            if self.p.size[self.order[stage]] > 1:
                wait_bytes(self.many(stage), self.send_sem.at[self.u, stage])
        wait_bytes(self.swap_ref(self.p.c), self.send_sem.at[self.u, 3])


def add_into(dst, *srcs):
    total = dst[...].astype(F32)
    for s in srcs:
        total = total + s[...].astype(F32)
    dst[...] = total.astype(BF16)


class Reduce:
    def __init__(self, place, g, gslot, part, rings, rows, tiles, u, order, send_sem, recv_sem):
        self.p, self.g, self.gslot, self.part, self.u, self.order = place, g, gslot, part, u, order
        self.recv = {2: lambda k: rings[0].at[rings[1], k], 1: lambda k: rows.at[u, k, pl.ds(0, place.size[order[0]])]}
        self.tiles = tiles
        self.send_sem, self.recv_sem = send_sem, recv_sem
        self.first_sem = {2: 1, 1: 1 + max(place.size[order[2]] - 1, 1)}
        self.last_sem = self.first_sem[1] + max(place.size[order[1]] - 1, 1)

    def block(self, stage, v):
        return block_of(self.part, (self.u,), self.p, self.order[:stage], self.order[stage], v)

    def swap_start(self):
        start_copy(self.g.at[self.gslot, :, :, :, 1 - self.p.c], self.part.at[self.u],
                   self.send_sem.at[self.u, 3], self.recv_sem.at[self.u, 0], self.p.sib)

    def swap_wait(self):
        wait_bytes(self.part.at[self.u], self.recv_sem.at[self.u, 0])
        p = self.p

        def add(k, _):
            add_into(self.part.at[self.u, k], self.g.at[self.gslot, k, :, :, p.c])
            return 0

        lax.fori_loop(0, p.size["z"], add, 0)
        wait_bytes(self.part.at[self.u], self.send_sem.at[self.u, 3])

    def ways(self, stage):
        d = self.order[stage]
        return ((1, self.p.far(d)), (-1, self.p.near(d)))

    def ring_send(self, stage, way, step, n):
        p, d = self.p, self.order[stage]
        s = p.sign * way
        k = ring_sem(p, d, way, step)
        src = self.block(stage, p.wrap(p.pos[d] + n * s, d)) if step == 1 else self.recv[stage](k - 1)
        start_copy(src, self.recv[stage](k), self.send_sem.at[self.u, stage],
                   self.recv_sem.at[self.u, self.first_sem[stage] + k], p.dev(d, p.wrap(p.pos[d] + s, d)))

    def ring_start(self, stage):
        for way, n in self.ways(stage):
            if n:
                self.ring_send(stage, way, 1, n)

    def ring_step(self, stage, step):
        p, d = self.p, self.order[stage]
        ends = []
        for way, n in self.ways(stage):
            if step <= n:
                k = ring_sem(p, d, way, step)
                ref = self.recv[stage](k)
                wait_bytes(ref, self.recv_sem.at[self.u, self.first_sem[stage] + k])
                if step < n:
                    add_into(ref, self.block(stage, p.wrap(p.pos[d] + (n - step) * p.sign * way, d)))
                    self.ring_send(stage, way, step + 1, n)
        if step == p.far(d):
            for way, n in self.ways(stage):
                if n:
                    ends.append(self.recv[stage](ring_sem(p, d, way, n)))
            add_into(self.block(stage, p.pos[d]), *ends)

    def direct_start(self):
        p, d = self.p, self.order[0]
        for k in range(1, p.size[d]):
            v = p.wrap(p.pos[d] + k, d)
            start_copy(self.block(0, v), self.tiles.at[self.u, k - 1], self.send_sem.at[self.u, 0],
                       self.recv_sem.at[self.u, self.last_sem], p.dev(d, v))

    def direct_sum(self):
        n = self.p.size[self.order[0]]
        if n > 1:
            wait_bytes(self.tiles.at[self.u, pl.ds(0, n - 1)], self.recv_sem.at[self.u, self.last_sem])
        total = self.block(0, self.p.pos[self.order[0]])[...].astype(F32)
        for k in range(n - 1):
            total = total + self.tiles[self.u, k].astype(F32)
        return total.astype(BF16).astype(F32)

    def events(self):
        out = [[self.swap_wait]]
        for stage in (2, 1):
            out[-1].append(functools.partial(self.ring_start, stage))
            for step in range(1, self.p.far(self.order[stage]) + 1):
                out.append([functools.partial(self.ring_step, stage, step)])
        out[-1].append(self.direct_start)
        return out

    def drain(self):
        p = self.p
        for stage in (2, 1):
            n = p.size[self.order[stage]] - 1
            if n:
                wait_bytes(self.block(stage, pl.ds(0, n)), self.send_sem.at[self.u, stage])
        n = p.size[self.order[0]] - 1
        if n:
            wait_bytes(self.tiles.at[self.u, pl.ds(0, n)], self.send_sem.at[self.u, 0])


def enter(p):
    barrier = pltpu.get_barrier_semaphore()
    group = p.grid[2] * p.grid[3]
    peers = [p.base + lax.rem(p.m + k, group) for k in range(1, group)]
    for d in ("y", "z"):
        peers += [p.dev(d, p.wrap(p.pos[d] + k, d)) for k in range(1, p.size[d])]
    for peer in peers:
        pl.semaphore_signal(barrier, inc=1, device_id=(peer,), device_id_type=pl.DeviceIdType.MESH)
    pl.semaphore_wait(barrier, len(peers))


def lanes(ref, j):
    return ref.at[:, :, pl.ds(pl.multiple_of(j * LANES, LANES), LANES)]


class Shuffle:
    def __init__(self, place, one, two, sems, k0):
        self.p, self.one, self.two = place, one, two
        self.sem = lambda k: sems.at[k0 + k]
        self.group = place.grid[2] * place.grid[3]
        self.half = self.group // 2
        self.low = (place.m // self.half) * self.half
        self.mine = place.m - self.low

    def to_tiles_start(self, src1, src2):
        p = self.p
        for k in range(1, self.group):
            j = lax.rem(p.m + k, self.group)
            start_copy(lanes(src1, j), self.one.at[p.m], self.sem(0), self.sem(1), p.base + j)
        for k in range(1, self.half):
            j = lax.rem(self.mine + k, self.half)
            start_copy(lanes(src2, j), self.two.at[self.mine], self.sem(2), self.sem(3), p.base + self.low + j)

    def to_tiles_own(self, src1, src2):
        p = self.p
        pltpu.make_async_copy(lanes(src1, p.m), self.one.at[p.m], self.sem(1)).start()
        pltpu.make_async_copy(lanes(src2, self.mine), self.two.at[self.mine], self.sem(3)).start()

    def drain_sends(self):
        wait_bytes(self.one.at[pl.ds(0, self.group - 1)], self.sem(0))
        wait_bytes(self.two.at[pl.ds(0, self.half - 1)], self.sem(2))

    def to_tiles_finish(self, tiles):
        wait_bytes(self.one, self.sem(1))
        wait_bytes(self.two, self.sem(3))
        for l in range(self.one.shape[1]):
            for m in range(self.group):
                tiles[2 * l, 2 * m:2 * m + 2, :] = self.one[m, l]
            for m in range(self.half):
                tiles[2 * l + 1, 4 * m:4 * m + 4, :] = self.two[m, l]

    def put_rows(self, u, tile):
        if u % 2 == 0:
            for m in range(self.group):
                self.one[m, u // 2] = tile[2 * m:2 * m + 2, :]
        else:
            for m in range(self.half):
                self.two[m, u // 2] = tile[4 * m:4 * m + 4, :]

    def to_rows_start(self, dst1, dst2):
        p = self.p
        pltpu.make_async_copy(self.one.at[p.m], lanes(dst1, p.m), self.sem(1)).start()
        pltpu.make_async_copy(self.two.at[self.mine], lanes(dst2, self.mine), self.sem(3)).start()
        for k in range(1, self.group):
            j = lax.rem(p.m + k, self.group)
            start_copy(self.one.at[j], lanes(dst1, p.m), self.sem(0), self.sem(1), p.base + j)
        for k in range(1, self.half):
            j = lax.rem(self.mine + k, self.half)
            start_copy(self.two.at[j], lanes(dst2, self.mine), self.sem(2), self.sem(3), p.base + self.low + j)

    def to_rows_finish(self):
        wait_bytes(self.one, self.sem(1))
        wait_bytes(self.two, self.sem(3))
        self.drain_sends()


def w_one_of(wbuf, l):
    nz, ny, nx, nc = wbuf.shape[1:5]
    cols = [wbuf[2 * l, :, :, m // nc, m % nc].reshape(nz * ny * 16, LANES) for m in range(nx * nc)]
    return jnp.concatenate(cols, axis=1)


def w_two_of(wbuf, l):
    nz, ny, nx, nc = wbuf.shape[1:5]
    half = nx * nc // 2
    cols = []
    for b in range(half):
        pair = [wbuf[2 * l + 1, :, :, (r * half + b) // nc, b % nc].reshape(nz * ny, 1, 16, LANES) for r in range(2)]
        cols.append(jnp.concatenate(pair, axis=1).reshape(nz * ny * 32, LANES))
    return jnp.concatenate(cols, axis=1)


def contract(a, b, da, db):
    return lax.dot_general(a, b, (((da,), (db,)), ((), ())), preferred_element_type=F32)


def gelu_and_slope(u):
    u2 = u * u
    t = jnp.tanh(GELU_SCALE * (u + GELU_CUBE * (u * u2)))
    half = 0.5 * (1.0 + t)
    slope = half + (0.5 * u) * (1.0 - t * t) * (GELU_SCALE + (3.0 * GELU_CUBE * GELU_SCALE) * u2)
    return u * half, slope


def gelu(u):
    return u * (0.5 * (1.0 + jnp.tanh(GELU_SCALE * (u + GELU_CUBE * (u * u * u)))))


def row_tiles(total, body):
    size = min(ROWS, total)
    assert total % size == 0

    def step(t, _):
        body(pl.ds(pl.multiple_of(t * size, size), size))
        return 0

    lax.fori_loop(0, total // size, step, 0)


def step_kernel(grid, batch_scale, w1, w2, m1, m2, x0, y0, x1, y1, nw1, nw2, nm1, nm2, loss, hlast, spill,
                wbuf, slope, act, hid, h, dlow, g, part, ring_ab, ring_c, rows, tiles3,
                wone, wtwo, mone, mtwo, wrow1, wrow2, wt, mt, lossbuf,
                gsend, grecv, rsend, rrecv, shuf, local):
    p = Place(grid)
    layers = w1.shape[0]
    units = 2 * layers
    nz, ny, nx, nc = grid
    tok, d_model = h.shape
    d_ff = hid.shape[2]

    def load(src, dst, k):
        return pltpu.make_async_copy(src, dst, local.at[k])

    loads = {"x0": load(x0, act.at[0], 0), "y0": load(y0, dlow, 1),
             "x1": load(x1, act.at[layers - 1], 2), "y1": load(y1, act.at[layers - 2], 3)}
    stage = [load(w1, wrow1, 2), load(w2, wrow2, 3)]
    wshuf = Shuffle(p, wone, wtwo, shuf, 0)
    mshuf = Shuffle(p, mone, mtwo, shuf, 4)
    for c in stage:
        c.start()
    wshuf.to_tiles_own(w1, w2)
    mshuf.to_tiles_own(m1, m2)
    loads["x0"].start()
    loads["y0"].start()
    enter(p)
    for c in stage:
        c.wait()
    wshuf.to_tiles_start(wrow1, wrow2)
    mshuf.to_tiles_start(m1, m2)

    def own_tile(u):
        wbuf[u, p.z, p.y, p.x, p.c] = wt[u].astype(BF16)

    wshuf.to_tiles_finish(wt)
    for u in range(units):
        own_tile(u)
    loads["x0"].wait()
    h[...] = act[0].astype(F32)

    def spill_copy(l):
        return load(slope.at[l % 2], spill.at[l], 4 + l)

    def unspill_copy(l):
        return load(spill.at[l], slope.at[l % 2], 4 + l)

    def forward_one(l):
        if 2 <= l < SPILLED + 2 and l - 2 < SPILLED:
            spill_copy(l - 2).wait()

        def body(r):
            a = h[r, :].astype(BF16)
            if l:
                act[l, r, :] = a
            z, s = gelu_and_slope(jnp.dot(a, w_one_of(wbuf, l), preferred_element_type=F32))
            z = z.astype(BF16)
            slope[l % 2, r, :] = s
            hid[l, r, :] = z
            h[r, :] += jnp.dot(z, w_two_of(wbuf, l), preferred_element_type=F32)

        row_tiles(tok, body)
        if l < SPILLED and l + 2 < layers:
            spill_copy(l).start()

    def loss_slope():
        loads["y0"].wait()

        def body(r):
            d = (h[r, :] - dlow[r, :].astype(F32)) * batch_scale
            h[r, :] = d
            dlow[r, :] = d.astype(BF16)

        row_tiles(tok, body)

    gather_args = lambda u: (p, wbuf, u, ORDERS[u % 3], gsend, grecv)
    slots = gradient_slots()
    first = [Gather(*gather_args(u)) for u in range(units)]
    again = [Gather(*gather_args(u)) for u in range(units)]
    red = []
    for u in range(units):
        ring = (ring_c, u // 3) if u % 3 == 2 else (ring_ab, 2 * (u // 3) + u % 3)
        red.append(Reduce(p, g, slots[u], part, ring, rows, tiles3, u, ORDERS[u % 3], rsend, rrecv))

    def grad_two(l):
        slot = red[2 * l + 1].gslot
        size = min(256, d_ff)
        zs = size // (ny * 32)

        def step(j, _):
            cols = pl.ds(pl.multiple_of(j * size, size), size)
            v = contract(hid[l, :, cols], dlow[...], 0, 0).astype(BF16).reshape(zs, ny, 2, 16, d_model)
            for b in range(nx * nc // 2):
                for r in range(2):
                    g[slot, pl.ds(j * zs, zs), :, (r * nx * nc // 2 + b) // nc, b % nc] = v[:, :, r, :, LANES * b:LANES * b + LANES]
            return 0

        lax.fori_loop(0, d_ff // size, step, 0)

    def back_hidden(l):
        if l < SPILLED and l + 2 < layers:
            unspill_copy(l).wait()

        def body(r):
            q = contract(dlow[r, :], w_two_of(wbuf, l), 1, 1)
            v = (slope[l % 2, r, :] * q).astype(BF16)
            hid[l, r, :] = v
            if l:
                d = h[r, :] + contract(v, w_one_of(wbuf, l), 1, 1)
                h[r, :] = d
                dlow[r, :] = d.astype(BF16)

        row_tiles(tok, body)
        red[2 * l + 1].swap_start()
        if 0 <= l - 2 < SPILLED:
            unspill_copy(l - 2).start()

    def grad_one(l):
        slot = red[2 * l].gslot
        size = min(256, d_model)
        zs = size // (ny * 16)

        def step(j, _):
            cols = pl.ds(pl.multiple_of(j * size, size), size)
            v = contract(act[l, :, cols], hid[l], 0, 0).astype(BF16).reshape(zs, ny, 16, d_ff)
            for m in range(nx * nc):
                g[slot, pl.ds(j * zs, zs), :, m // nc, m % nc] = v[:, :, :, LANES * m:LANES * m + LANES]
            return 0

        lax.fori_loop(0, d_model // size, step, 0)
        red[2 * l].swap_start()
        if l == layers - 1:
            loads["x1"].start()
        if l == layers - 2:
            loads["y1"].start()

    def update(u):
        total = red[u].direct_sum()
        mom = MOMENTUM * mt[u] + total
        w = wt[u] - LEARN_RATE * mom
        wbuf[u, p.z, p.y, p.x, p.c] = w.astype(BF16)
        wt[u] = w
        mt[u] = mom
        again[u].direct_start()

    def moments_ready():
        mshuf.to_tiles_finish(mt)
        mshuf.drain_sends()
        wshuf.drain_sends()

    def second_start():
        loads["x1"].wait()
        h[...] = act[layers - 1].astype(F32)

    def forward_two(l):
        last = l == layers - 1
        if last:
            loads["y1"].wait()

        def body(r):
            a = h[r, :].astype(BF16)
            z = gelu(jnp.dot(a, w_one_of(wbuf, l), preferred_element_type=F32)).astype(BF16)
            v = h[r, :] + jnp.dot(z, w_two_of(wbuf, l), preferred_element_type=F32)
            h[r, :] = v
            if last:
                e = v - act[layers - 2, r, :].astype(F32)
                e = e * e
                s = e[:, :LANES]
                for k in range(1, d_model // LANES):
                    s = s + e[:, LANES * k:LANES * k + LANES]
                lossbuf[:, r] = jnp.sum(s.T, axis=0, keepdims=True) * (1.0 / (2 * d_model))

        row_tiles(tok, body)

    def new_rows():
        for u in range(units):
            wshuf.put_rows(u, wt[u])
            mshuf.put_rows(u, mt[u])
        wshuf.to_rows_start(nw1, nw2)
        mshuf.to_rows_start(nm1, nm2)

    work = {}
    for u in range(units):
        for k, ev in enumerate(first[u].events()):
            work["a", u, k] = ev
        for k, ev in enumerate(red[u].events()):
            work["r", u, k] = ev
        work["u", u, 0] = [functools.partial(update, u)]
        for k, ev in enumerate(again[u].events()[1:]):
            work["b", u, k] = ev
        work["d", u, 0] = [first[u].drain]
    for l in range(layers):
        work["f", l, 0] = [functools.partial(forward_one, l)]
        work["g", l, 0] = [functools.partial(grad_two, l)]
        work["g", l, 1] = [functools.partial(back_hidden, l)]
        work["g", l, 2] = [functools.partial(grad_one, l)]
        work["s", l, 0] = [functools.partial(forward_two, l)]
    work["l", 0, 0] = [loss_slope]
    work["m", 0, 0] = [moments_ready]
    work["h", 0, 0] = [second_start]
    work["n", 0, 0] = [new_rows]
    for name in ORDER:
        for f in work.pop(name):
            f()
    assert not work
    out = [load(h, hlast, 0), load(lossbuf, loss, 1)]
    for c in out:
        c.start()
    for u in range(units):
        again[u].drain()
        red[u].drain()
    wshuf.to_rows_finish()
    mshuf.to_rows_finish()
    for c in out:
        c.wait()


def gradient_slots():
    free, held = list(range(G_SLOTS)), {}
    for tag, n, k in ORDER:
        if tag == "g" and k != 1:
            held[2 * n + (k == 0)] = free.pop(0)
        if tag == "r" and k == 0:
            free.append(held[n])
    return held


def make_step(grid, layers, tok, d_model, d_ff, n_dev):
    nz, ny, nx, nc = grid
    units = 2 * layers
    group = nx * nc
    hbm = pl.BlockSpec(memory_space=pl.ANY)
    sds = jax.ShapeDtypeStruct
    tile = (16, LANES)
    dma = pltpu.SemaphoreType.DMA
    thirds = (units + 2) // 3
    outs = (sds((layers, 2, d_ff), F32), sds((layers, 4, d_model), F32), sds((layers, 2, d_ff), F32), sds((layers, 4, d_model), F32),
            sds((1, tok), F32), sds((tok, d_model), F32), sds((SPILLED, tok, d_ff), F32))
    shuffled = [pltpu.VMEM((group, layers, 2, LANES), F32), pltpu.VMEM((group // 2, layers, 4, LANES), F32)]
    scratch = [
        pltpu.VMEM((units, *grid, *tile), BF16),
        pltpu.VMEM((2, tok, d_ff), F32),
        pltpu.VMEM((layers, tok, d_model), BF16),
        pltpu.VMEM((layers, tok, d_ff), BF16),
        pltpu.VMEM((tok, d_model), F32),
        pltpu.VMEM((tok, d_model), BF16),
        pltpu.VMEM((G_SLOTS, *grid, *tile), BF16),
        pltpu.VMEM((units, nz, ny, nx, *tile), BF16),
        pltpu.VMEM((2 * thirds, nx - 1, nz, ny, *tile), BF16),
        pltpu.VMEM((thirds, nz - 1, ny, nx, *tile), BF16),
        pltpu.VMEM((units, max(ny, nx) - 1, max(nz, nx), *tile), BF16),
        pltpu.VMEM((units, max(nz, nx) - 1, *tile), BF16),
        *shuffled, *shuffled,
        pltpu.VMEM((layers, 2, d_ff), F32), pltpu.VMEM((layers, 4, d_model), F32),
        pltpu.VMEM((units, *tile), F32), pltpu.VMEM((units, *tile), F32),
        pltpu.VMEM((1, tok), F32),
        dma((units, 4)), dma((units, 12)), dma((units, 4)), dma((units, 12)), dma((8,)), dma((4 + SPILLED,)),
    ]
    return pl.pallas_call(
        functools.partial(step_kernel, grid, 1.0 / (n_dev * tok * d_model)),
        out_shape=outs, in_specs=[hbm] * 8, out_specs=[hbm] * 7, scratch_shapes=scratch,
        compiler_params=pltpu.CompilerParams(collective_id=0, has_side_effects=True, vmem_limit_bytes=67043328),
        name="train_step")


def hand_over(*refs):
    n = len(refs) // 2
    for src, dst in zip(refs[:n], refs[n:]):
        if len(dst.shape) < len(src.shape):
            dst[...] = src[0, :]
        else:
            dst[...] = src[...]


def solution(mesh):
    n_dev = mesh.shape["data"]
    w_spec = P(None, "data", None)
    row_spec = P("data", None)

    def device_step(w_one, w_two, mom_one, mom_two, x_zero, y_zero, x_one, y_one):
        tok, d_model = x_zero.shape
        step = make_step(GRID, w_one.shape[0], tok, d_model, w_one.shape[2], n_dev)
        made = step(w_one, w_two, mom_one, mom_two, x_zero, y_zero, x_one, y_one)[:6]
        outs = [jax.ShapeDtypeStruct(v.shape, v.dtype) for v in made]
        outs[4] = jax.ShapeDtypeStruct((tok,), F32)
        vmem = pl.BlockSpec(memory_space=pltpu.VMEM)
        return pl.pallas_call(hand_over, out_shape=tuple(outs), in_specs=[vmem] * 6, out_specs=[vmem] * 6, name="hand_over")(*made)

    return jax.shard_map(device_step, mesh=mesh, in_specs=(w_spec, w_spec, w_spec, w_spec, row_spec, row_spec, row_spec, row_spec),
                         out_specs=(w_spec, w_spec, w_spec, w_spec, P("data"), row_spec), check_vma=False)
```

```python
import functools
import jax
import jax.numpy as jnp
from jax import lax
from jax.experimental import pallas as pl
from jax.experimental.pallas import tpu as pltpu
from jax.sharding import PartitionSpec as P

LEARN_RATE = 0.1
MOMENTUM = 0.9
F32, BF16 = jnp.float32, jnp.bfloat16
GRID = (8, 4, 4, 2)
ORDERS = (("z", "x", "y"), ("z", "y", "x"), ("x", "y", "z"))
GELU_SCALE = 0.7978845608028654
GELU_CUBE = 0.044715
G_SLOTS = 6
LANES = 128
SPILLED = 4

ORDER = (
    ("a", 8, 0), ("a", 9, 0), ("a", 1, 0), ("a", 0, 0), ("a", 2, 0), ("a", 4, 0), ("a", 3, 0), ("m", 0, 0), ("a", 5, 0), ("a", 11, 0), ("a", 7, 0),
    ("a", 8, 1), ("a", 10, 0), ("a", 6, 0), ("a", 2, 1), ("a", 5, 1), ("a", 11, 1), ("a", 9, 1), ("a", 1, 1), ("a", 0, 1), ("a", 8, 2), ("a", 4, 1),
    ("a", 2, 2), ("a", 3, 1), ("a", 5, 2), ("a", 7, 1), ("a", 11, 2), ("a", 10, 1), ("a", 6, 1), ("a", 1, 2), ("a", 8, 3), ("a", 0, 2), ("a", 2, 3),
    ("a", 4, 2), ("a", 3, 2), ("a", 5, 3), ("a", 7, 2), ("a", 11, 3), ("a", 1, 3), ("a", 0, 3), ("a", 2, 4), ("a", 8, 4), ("a", 6, 2), ("a", 5, 4),
    ("a", 4, 3), ("a", 3, 3), ("a", 11, 4), ("a", 0, 4), ("a", 2, 5), ("a", 7, 3), ("a", 0, 5), ("d", 0, 0), ("a", 9, 2), ("a", 1, 4), ("a", 8, 5),
    ("a", 10, 2), ("a", 5, 5), ("a", 6, 3), ("a", 4, 4), ("a", 1, 5), ("f", 0, 0), ("a", 2, 6), ("a", 3, 4), ("a", 7, 4), ("a", 4, 5), ("a", 11, 5),
    ("d", 1, 0), ("d", 4, 0), ("a", 5, 6), ("a", 8, 6), ("a", 9, 3), ("a", 2, 7), ("d", 2, 0), ("a", 3, 5), ("f", 1, 0), ("a", 8, 7), ("a", 6, 4),
    ("a", 7, 5), ("d", 7, 0), ("a", 10, 3), ("a", 5, 7), ("f", 2, 0), ("a", 9, 4), ("a", 6, 5), ("d", 6, 0), ("d", 3, 0), ("a", 11, 6), ("d", 8, 0),
    ("f", 3, 0), ("a", 9, 5), ("a", 10, 4), ("d", 9, 0), ("a", 11, 7), ("d", 11, 0), ("f", 4, 0), ("a", 10, 5), ("d", 10, 0), ("d", 5, 0),
    ("f", 5, 0), ("l", 0, 0), ("g", 5, 0), ("g", 5, 1), ("g", 4, 0), ("g", 4, 1), ("g", 4, 2), ("g", 5, 2), ("r", 11, 0), ("g", 3, 0), ("r", 8, 0),
    ("g", 3, 1), ("g", 3, 2), ("r", 11, 1), ("r", 10, 0), ("r", 9, 0), ("r", 8, 1), ("g", 2, 0), ("r", 7, 0), ("r", 6, 0), ("g", 2, 1), ("r", 11, 2),
    ("g", 1, 0), ("r", 8, 2), ("g", 1, 1), ("r", 10, 1), ("r", 5, 0), ("g", 0, 0), ("r", 6, 1), ("r", 7, 1), ("r", 8, 3), ("g", 1, 2), ("r", 3, 0),
    ("r", 11, 3), ("g", 0, 1), ("r", 5, 1), ("r", 6, 2), ("r", 8, 4), ("r", 7, 2), ("r", 2, 0), ("g", 0, 2), ("g", 2, 2), ("r", 1, 0), ("r", 10, 2),
    ("h", 0, 0), ("r", 5, 2), ("r", 3, 1), ("r", 8, 5), ("r", 6, 3), ("r", 2, 1), ("r", 4, 0), ("r", 0, 0), ("r", 7, 3), ("r", 5, 3), ("r", 1, 1),
    ("r", 10, 3), ("r", 11, 4), ("u", 8, 0), ("r", 2, 2), ("r", 9, 1), ("r", 3, 2), ("u", 6, 0), ("r", 5, 4), ("r", 4, 1), ("r", 0, 1), ("u", 7, 0),
    ("r", 1, 2), ("r", 2, 3), ("r", 11, 5), ("r", 9, 2), ("b", 8, 0), ("u", 10, 0), ("r", 3, 3), ("r", 5, 5), ("r", 4, 2), ("r", 0, 2), ("r", 2, 4),
    ("b", 6, 0), ("u", 11, 0), ("b", 7, 0), ("r", 1, 3), ("b", 8, 1), ("u", 5, 0), ("b", 10, 0), ("r", 4, 3), ("u", 3, 0), ("r", 0, 3), ("r", 2, 5),
    ("b", 6, 1), ("b", 5, 0), ("b", 7, 1), ("b", 8, 2), ("u", 1, 0), ("b", 11, 0), ("u", 2, 0), ("r", 9, 3), ("b", 10, 1), ("u", 4, 0), ("b", 8, 3),
    ("b", 6, 2), ("b", 3, 0), ("u", 0, 0), ("b", 5, 1), ("b", 2, 0), ("b", 11, 1), ("b", 1, 0), ("b", 7, 2), ("b", 8, 4), ("b", 6, 3), ("b", 10, 2),
    ("b", 4, 0), ("u", 9, 0), ("n", 0, 0), ("b", 2, 1), ("b", 5, 2), ("b", 6, 4), ("b", 3, 1), ("b", 0, 0), ("b", 7, 3), ("b", 1, 1), ("b", 11, 2),
    ("b", 8, 5), ("b", 7, 4), ("b", 10, 3), ("b", 8, 6), ("b", 10, 4), ("b", 2, 2), ("b", 4, 1), ("b", 9, 0), ("b", 0, 1), ("b", 5, 3), ("b", 3, 2),
    ("b", 11, 3), ("b", 1, 2), ("b", 2, 3), ("b", 5, 4), ("b", 0, 2), ("b", 4, 2), ("b", 11, 4), ("b", 3, 3), ("b", 2, 4), ("b", 9, 1), ("b", 1, 3),
    ("b", 5, 5), ("b", 3, 4), ("b", 0, 3), ("b", 11, 5), ("b", 4, 3), ("b", 1, 4), ("b", 5, 6), ("b", 2, 5), ("b", 0, 4), ("s", 0, 0), ("b", 2, 6),
    ("b", 11, 6), ("b", 4, 4), ("b", 9, 2), ("s", 1, 0), ("s", 2, 0), ("b", 9, 3), ("s", 3, 0), ("b", 9, 4), ("s", 4, 0), ("s", 5, 0),
)


def start_copy(src, dst, send_sem, recv_sem, dev):
    pltpu.make_async_remote_copy(src_ref=src, dst_ref=dst, send_sem=send_sem, recv_sem=recv_sem,
                                 device_id=(dev,), device_id_type=pl.DeviceIdType.MESH).start()


def wait_bytes(ref, sem):
    pltpu.make_async_copy(ref, ref, sem).wait()


class Place:
    def __init__(self, grid):
        self.grid = grid
        nz, ny, nx, nc = grid
        me = lax.axis_index("data")
        self.me = me
        self.c = lax.rem(me, nc)
        self.x = lax.rem(me // nc, nx)
        self.y = lax.rem(me // (nc * nx), ny)
        self.z = me // (nc * nx * ny)
        self.sign = 1 - 2 * self.c
        self.size = {"z": nz, "y": ny, "x": nx}
        self.pos = {"z": self.z, "y": self.y, "x": self.x}
        self.stride = {"z": ny * nx * nc, "y": nx * nc, "x": nc}
        self.sib = me + 1 - 2 * self.c
        self.m = lax.rem(me, nc * nx)
        self.base = me - self.m

    def wrap(self, v, d):
        n = self.size[d]
        return lax.rem(v + 2 * n, n)

    def dev(self, d, v):
        return self.me + (v - self.pos[d]) * self.stride[d]

    def far(self, d):
        return self.size[d] // 2

    def near(self, d):
        return (self.size[d] - 1) // 2


def block_of(buf, lead, place, done, d, v, tail=()):
    idx = []
    for k in ("z", "y", "x"):
        if k in done:
            idx.append(slice(None))
        elif k == d:
            idx.append(v)
        else:
            idx.append(place.pos[k])
    return buf.at[(*lead, *idx, *tail)]


def ring_sem(place, d, way, step):
    return step - 1 if way == 1 else place.far(d) + step - 1


class Gather:
    def __init__(self, place, buf, u, order, send_sem, recv_sem):
        self.p, self.buf, self.u, self.order = place, buf, u, order
        self.send_sem, self.recv_sem = send_sem, recv_sem
        self.last_sem = 2 + max(place.size[order[2]] - 1, 1)

    def block(self, stage, v):
        return block_of(self.buf, (self.u,), self.p, self.order[:stage], self.order[stage], v, (self.p.c,))

    def many(self, stage):
        return self.block(stage, pl.ds(0, self.p.size[self.order[stage]] - 1))

    def direct_start(self, stage):
        p, d = self.p, self.order[stage]
        own = self.block(stage, p.pos[d])
        for k in range(1, p.size[d]):
            start_copy(own, own, self.send_sem.at[self.u, stage], self.recv_sem.at[self.u, stage], p.dev(d, p.wrap(p.pos[d] + k, d)))

    def direct_wait(self, stage):
        if self.p.size[self.order[stage]] > 1:
            wait_bytes(self.many(stage), self.recv_sem.at[self.u, stage])

    def ring_send(self, way, step):
        p, d = self.p, self.order[2]
        s = p.sign * way
        ref = self.block(2, p.wrap(p.pos[d] - (step - 1) * s, d))
        start_copy(ref, ref, self.send_sem.at[self.u, 2], self.recv_sem.at[self.u, 2 + ring_sem(p, d, way, step)], p.dev(d, p.wrap(p.pos[d] + s, d)))

    def ways(self):
        d = self.order[2]
        return ((1, self.p.far(d)), (-1, self.p.near(d)))

    def ring_start(self):
        for way, n in self.ways():
            if n:
                self.ring_send(way, 1)
        self.swap_start(0)

    def ring_step(self, step):
        p, d = self.p, self.order[2]
        for way, n in self.ways():
            if step <= n:
                ref = self.block(2, p.wrap(p.pos[d] - step * p.sign * way, d))
                wait_bytes(ref, self.recv_sem.at[self.u, 2 + ring_sem(p, d, way, step)])
                if step < n:
                    self.ring_send(way, step + 1)
                self.swap_start(step * way)

    def swap_ref(self, c):
        return self.buf.at[self.u, :, :, :, c]

    def swap_start(self, k):
        d = self.order[2]
        ref = self.block(2, self.p.wrap(self.p.pos[d] - k * self.p.sign, d))
        start_copy(ref, ref, self.send_sem.at[self.u, 3], self.recv_sem.at[self.u, self.last_sem], self.p.sib)

    def swap_wait(self):
        wait_bytes(self.swap_ref(1 - self.p.c), self.recv_sem.at[self.u, self.last_sem])

    def events(self):
        part = functools.partial
        out = [[part(self.direct_start, 0)],
               [part(self.direct_wait, 0), part(self.direct_start, 1)],
               [part(self.direct_wait, 1), self.ring_start]]
        out += [[part(self.ring_step, step)] for step in range(1, self.p.far(self.order[2]) + 1)]
        return out + [[self.swap_wait]]

    def drain(self):
        for stage in range(3):
            if self.p.size[self.order[stage]] > 1:
                wait_bytes(self.many(stage), self.send_sem.at[self.u, stage])
        wait_bytes(self.swap_ref(self.p.c), self.send_sem.at[self.u, 3])


def add_into(dst, *srcs):
    total = dst[...].astype(F32)
    for s in srcs:
        total = total + s[...].astype(F32)
    dst[...] = total.astype(BF16)


class Reduce:
    def __init__(self, place, g, gslot, part, rings, rows, tiles, u, order, send_sem, recv_sem):
        self.p, self.g, self.gslot, self.part, self.u, self.order = place, g, gslot, part, u, order
        self.ring = lambda k: rings[0].at[rings[1], k]
        n0 = place.size[order[0]]
        self.rows = lambda k: rows.at[u, k, pl.ds(0, n0)]
        self.tiles = lambda k: tiles.at[u, k]
        self.send_sem, self.recv_sem = send_sem, recv_sem
        self.first_sem = 3

    def block(self, stage, v):
        return block_of(self.part, (self.u,), self.p, self.order[:stage], self.order[stage], v)

    def swap_start(self):
        start_copy(self.g.at[self.gslot, :, :, :, 1 - self.p.c], self.part.at[self.u],
                   self.send_sem.at[self.u, 3], self.recv_sem.at[self.u, 0], self.p.sib)

    def swap_wait(self):
        wait_bytes(self.part.at[self.u], self.recv_sem.at[self.u, 0])
        p = self.p

        def add(k, _):
            add_into(self.part.at[self.u, k], self.g.at[self.gslot, k, :, :, p.c])
            return 0

        lax.fori_loop(0, p.size["z"], add, 0)
        wait_bytes(self.part.at[self.u], self.send_sem.at[self.u, 3])

    def ways(self):
        d = self.order[2]
        return ((1, self.p.far(d)), (-1, self.p.near(d)))

    def ring_send(self, way, step, n):
        p, d = self.p, self.order[2]
        s = p.sign * way
        k = ring_sem(p, d, way, step)
        src = self.block(2, p.wrap(p.pos[d] + n * s, d)) if step == 1 else self.ring(k - 1)
        start_copy(src, self.ring(k), self.send_sem.at[self.u, 2], self.recv_sem.at[self.u, self.first_sem + k],
                   p.dev(d, p.wrap(p.pos[d] + s, d)))

    def ring_start(self):
        for way, n in self.ways():
            if n:
                self.ring_send(way, 1, n)

    def ring_step(self, step):
        p, d = self.p, self.order[2]
        for way, n in self.ways():
            if step <= n:
                k = ring_sem(p, d, way, step)
                wait_bytes(self.ring(k), self.recv_sem.at[self.u, self.first_sem + k])
                if step < n:
                    add_into(self.ring(k), self.block(2, p.wrap(p.pos[d] + (n - step) * p.sign * way, d)))
                    self.ring_send(way, step + 1, n)
        if step == p.far(d):
            add_into(self.block(2, p.pos[d]), *[self.ring(ring_sem(p, d, way, n)) for way, n in self.ways() if n])

    def direct_start(self, stage):
        p, d = self.p, self.order[stage]
        land = self.rows if stage == 1 else self.tiles
        for k in range(1, p.size[d]):
            v = p.wrap(p.pos[d] + k, d)
            start_copy(self.block(stage, v), land(k - 1), self.send_sem.at[self.u, stage], self.recv_sem.at[self.u, 1 + stage], p.dev(d, v))

    def direct_wait(self, stage, sems, first):
        n = self.p.size[self.order[stage]]
        if n > 1:
            wait_bytes((self.rows if stage == 1 else self.tiles)(pl.ds(0, n - 1)), sems.at[self.u, first])

    def row_sum(self):
        self.direct_wait(1, self.recv_sem, 2)
        n = self.p.size[self.order[1]]
        if n > 1:
            add_into(self.block(1, self.p.pos[self.order[1]]), *[self.rows(k) for k in range(n - 1)])

    def tile_sum(self):
        self.direct_wait(0, self.recv_sem, 1)
        total = self.block(0, self.p.pos[self.order[0]])[...].astype(F32)
        for k in range(self.p.size[self.order[0]] - 1):
            total = total + self.tiles(k)[...].astype(F32)
        return total.astype(BF16).astype(F32)

    def events(self):
        part = functools.partial
        out = [[self.swap_wait, self.ring_start]]
        out += [[part(self.ring_step, step)] for step in range(1, self.p.far(self.order[2]) + 1)]
        out[-1].append(part(self.direct_start, 1))
        return out + [[self.row_sum, part(self.direct_start, 0)]]

    def drain(self):
        n = self.p.size[self.order[2]] - 1
        if n:
            wait_bytes(self.block(2, pl.ds(0, n)), self.send_sem.at[self.u, 2])
        self.direct_wait(1, self.send_sem, 1)
        self.direct_wait(0, self.send_sem, 0)


def enter(p):
    barrier = pltpu.get_barrier_semaphore()
    group = p.grid[2] * p.grid[3]
    peers = [p.base + lax.rem(p.m + k, group) for k in range(1, group)]
    for d in ("y", "z"):
        peers += [p.dev(d, p.wrap(p.pos[d] + k, d)) for k in range(1, p.size[d])]
    for peer in peers:
        pl.semaphore_signal(barrier, inc=1, device_id=(peer,), device_id_type=pl.DeviceIdType.MESH)
    pl.semaphore_wait(barrier, len(peers))


def lanes(ref, j):
    return ref.at[:, :, pl.ds(pl.multiple_of(j * LANES, LANES), LANES)]


class Shuffle:
    def __init__(self, place, one, two, sems, k0):
        self.p, self.one, self.two = place, one, two
        self.sem = lambda k: sems.at[k0 + k]
        self.group = place.grid[2] * place.grid[3]
        self.half = self.group // 2
        self.low = (place.m // self.half) * self.half
        self.mine = place.m - self.low

    def to_tiles_start(self, src1, src2):
        p = self.p
        for k in range(1, self.group):
            j = lax.rem(p.m + k, self.group)
            start_copy(lanes(src1, j), self.one.at[p.m], self.sem(0), self.sem(1), p.base + j)
        for k in range(1, self.half):
            j = lax.rem(self.mine + k, self.half)
            start_copy(lanes(src2, j), self.two.at[self.mine], self.sem(2), self.sem(3), p.base + self.low + j)

    def to_tiles_own(self, src1, src2):
        p = self.p
        pltpu.make_async_copy(lanes(src1, p.m), self.one.at[p.m], self.sem(1)).start()
        pltpu.make_async_copy(lanes(src2, self.mine), self.two.at[self.mine], self.sem(3)).start()

    def drain_sends(self):
        wait_bytes(self.one.at[pl.ds(0, self.group - 1)], self.sem(0))
        wait_bytes(self.two.at[pl.ds(0, self.half - 1)], self.sem(2))

    def to_tiles_finish(self, tiles):
        wait_bytes(self.one, self.sem(1))
        wait_bytes(self.two, self.sem(3))
        for l in range(self.one.shape[1]):
            for m in range(self.group):
                tiles[2 * l, 2 * m:2 * m + 2, :] = self.one[m, l]
            for m in range(self.half):
                tiles[2 * l + 1, 4 * m:4 * m + 4, :] = self.two[m, l]

    def put_rows(self, u, tile):
        if u % 2 == 0:
            for m in range(self.group):
                self.one[m, u // 2] = tile[2 * m:2 * m + 2, :]
        else:
            for m in range(self.half):
                self.two[m, u // 2] = tile[4 * m:4 * m + 4, :]

    def to_rows_start(self, dst1, dst2):
        p = self.p
        pltpu.make_async_copy(self.one.at[p.m], lanes(dst1, p.m), self.sem(1)).start()
        pltpu.make_async_copy(self.two.at[self.mine], lanes(dst2, self.mine), self.sem(3)).start()
        for k in range(1, self.group):
            j = lax.rem(p.m + k, self.group)
            start_copy(self.one.at[j], lanes(dst1, p.m), self.sem(0), self.sem(1), p.base + j)
        for k in range(1, self.half):
            j = lax.rem(self.mine + k, self.half)
            start_copy(self.two.at[j], lanes(dst2, self.mine), self.sem(2), self.sem(3), p.base + self.low + j)

    def to_rows_finish(self):
        wait_bytes(self.one, self.sem(1))
        wait_bytes(self.two, self.sem(3))
        self.drain_sends()


def w_one_of(wbuf, l):
    nz, ny, nx, nc = wbuf.shape[1:5]
    cols = [wbuf[2 * l, :, :, m // nc, m % nc].reshape(nz * ny * 16, LANES) for m in range(nx * nc)]
    return jnp.concatenate(cols, axis=1)


def w_two_of(wbuf, l):
    nz, ny, nx, nc = wbuf.shape[1:5]
    half = nx * nc // 2
    cols = []
    for b in range(half):
        pair = [wbuf[2 * l + 1, :, :, (r * half + b) // nc, b % nc].reshape(nz * ny, 1, 16, LANES) for r in range(2)]
        cols.append(jnp.concatenate(pair, axis=1).reshape(nz * ny * 32, LANES))
    return jnp.concatenate(cols, axis=1)


def contract(a, b, da, db):
    return lax.dot_general(a, b, (((da,), (db,)), ((), ())), preferred_element_type=F32)


def gelu_and_slope(u):
    u2 = u * u
    t = jnp.tanh(GELU_SCALE * (u + GELU_CUBE * (u * u2)))
    half = 0.5 * (1.0 + t)
    slope = half + (0.5 * u) * (1.0 - t * t) * (GELU_SCALE + (3.0 * GELU_CUBE * GELU_SCALE) * u2)
    return u * half, slope


def gelu(u):
    return u * (0.5 * (1.0 + jnp.tanh(GELU_SCALE * (u + GELU_CUBE * (u * u * u)))))


def step_kernel(grid, batch_scale, w1, w2, m1, m2, x0, y0, x1, y1, nw1, nw2, nm1, nm2, loss, hlast, spill,
                wbuf, slope, act, hid, h, dlow, g, part, ring_ab, ring_c, rows, tiles3,
                wone, wtwo, mone, mtwo, wrow1, wrow2, wt, mt, lossbuf,
                gsend, grecv, rsend, rrecv, shuf, local):
    p = Place(grid)
    layers = w1.shape[0]
    units = 2 * layers
    nz, ny, nx, nc = grid
    tok, d_model = h.shape
    d_ff = hid.shape[2]

    def load(src, dst, k):
        return pltpu.make_async_copy(src, dst, local.at[k])

    loads = {"x0": load(x0, act.at[0], 0), "y0": load(y0, dlow, 1),
             "x1": load(x1, act.at[layers - 1], 2), "y1": load(y1, act.at[layers - 2], 3)}
    stage = [load(w1, wrow1, 2), load(w2, wrow2, 3)]
    wshuf = Shuffle(p, wone, wtwo, shuf, 0)
    mshuf = Shuffle(p, mone, mtwo, shuf, 4)
    for c in stage:
        c.start()
    wshuf.to_tiles_own(w1, w2)
    mshuf.to_tiles_own(m1, m2)
    loads["x0"].start()
    loads["y0"].start()
    enter(p)
    for c in stage:
        c.wait()
    wshuf.to_tiles_start(wrow1, wrow2)
    mshuf.to_tiles_start(m1, m2)

    def own_tile(u):
        wbuf[u, p.z, p.y, p.x, p.c] = wt[u].astype(BF16)

    wshuf.to_tiles_finish(wt)
    for u in range(units):
        own_tile(u)
    loads["x0"].wait()
    h[...] = act[0].astype(F32)

    def spill_copy(l):
        return load(slope.at[lax.rem(l, 2)], spill.at[l], 4 + l)

    def unspill_copy(l):
        return load(spill.at[l], slope.at[l % 2], 4 + l)

    def forward_one(l):
        @pl.when(jnp.logical_and(l >= 2, l < SPILLED + 2))
        def _():
            spill_copy(l - 2).wait()

        a = h[...].astype(BF16)
        act[l] = a
        z, s = gelu_and_slope(jnp.dot(a, w_one_of(wbuf, l), preferred_element_type=F32))
        z = z.astype(BF16)
        slope[lax.rem(l, 2)] = s
        hid[l] = z
        h[...] += jnp.dot(z, w_two_of(wbuf, l), preferred_element_type=F32)

        @pl.when(l < SPILLED)
        def _():
            spill_copy(l).start()

    def loss_slope():
        loads["y0"].wait()
        d = (h[...] - dlow[...].astype(F32)) * batch_scale
        h[...] = d
        dlow[...] = d.astype(BF16)

    gather_args = lambda u: (p, wbuf, u, ORDERS[u % 3], gsend, grecv)
    slots = gradient_slots()
    first = [Gather(*gather_args(u)) for u in range(units)]
    again = [Gather(*gather_args(u)) for u in range(units)]
    red = []
    for u in range(units):
        ring = (ring_c, u // 3) if u % 3 == 2 else (ring_ab, 2 * (u // 3) + u % 3)
        red.append(Reduce(p, g, slots[u], part, ring, rows, tiles3, u, ORDERS[u % 3], rsend, rrecv))

    def grad_two(l):
        slot = red[2 * l + 1].gslot
        half = nx * nc // 2
        v = contract(hid[l], dlow[...], 0, 0).astype(BF16).reshape(nz, ny, 2, 16, d_model)
        for b in range(half):
            for r in range(2):
                g[slot, :, :, (r * half + b) // nc, b % nc] = v[:, :, r, :, LANES * b:LANES * b + LANES]

    def back_hidden(l):
        if l + 2 < layers:
            unspill_copy(l).wait()
        q = contract(dlow[...], w_two_of(wbuf, l), 1, 1)
        v = (slope[l % 2] * q).astype(BF16)
        hid[l] = v
        if l:
            d = h[...] + contract(v, w_one_of(wbuf, l), 1, 1)
            h[...] = d
            dlow[...] = d.astype(BF16)
        red[2 * l + 1].swap_start()
        if l >= 2:
            unspill_copy(l - 2).start()

    def grad_one(l):
        slot = red[2 * l].gslot
        v = contract(act[l], hid[l], 0, 0).astype(BF16).reshape(nz, ny, 16, d_ff)
        for m in range(nx * nc):
            g[slot, :, :, m // nc, m % nc] = v[:, :, :, LANES * m:LANES * m + LANES]
        red[2 * l].swap_start()
        if l == layers - 1:
            loads["x1"].start()
        if l == layers - 2:
            loads["y1"].start()

    def update(u):
        total = red[u].tile_sum()
        mom = MOMENTUM * mt[u] + total
        w = wt[u] - LEARN_RATE * mom
        wbuf[u, p.z, p.y, p.x, p.c] = w.astype(BF16)
        wt[u] = w
        mt[u] = mom
        again[u].direct_start(0)

    def moments_ready():
        mshuf.to_tiles_finish(mt)
        mshuf.drain_sends()
        wshuf.drain_sends()

    def second_start():
        loads["x1"].wait()
        h[...] = act[layers - 1].astype(F32)

    def forward_two(l):
        z = gelu(jnp.dot(h[...].astype(BF16), w_one_of(wbuf, l), preferred_element_type=F32)).astype(BF16)
        v = h[...] + jnp.dot(z, w_two_of(wbuf, l), preferred_element_type=F32)
        h[...] = v
        return v

    def forward_last():
        loads["y1"].wait()
        e = forward_two(layers - 1) - act[layers - 2].astype(F32)
        e = e * e
        s = e[:, :LANES]
        for k in range(1, d_model // LANES):
            s = s + e[:, LANES * k:LANES * k + LANES]
        lossbuf[...] = jnp.sum(s.T, axis=0, keepdims=True) * (1.0 / (2 * d_model))

    def new_rows():
        for u in range(units):
            wshuf.put_rows(u, wt[u])
            mshuf.put_rows(u, mt[u])
        wshuf.to_rows_start(nw1, nw2)
        mshuf.to_rows_start(nm1, nm2)

    work = {}
    for u in range(units):
        for k, ev in enumerate(first[u].events()):
            work["a", u, k] = ev
        for k, ev in enumerate(red[u].events()):
            work["r", u, k] = ev
        work["u", u, 0] = [functools.partial(update, u)]
        for k, ev in enumerate(again[u].events()[1:]):
            work["b", u, k] = ev
        work["d", u, 0] = [first[u].drain]
    for l in range(layers):
        work["g", l, 0] = [functools.partial(grad_two, l)]
        work["g", l, 1] = [functools.partial(back_hidden, l)]
        work["g", l, 2] = [functools.partial(grad_one, l)]
    work["s", layers - 1, 0] = [forward_last]
    work["l", 0, 0] = [loss_slope]
    work["m", 0, 0] = [moments_ready]
    work["h", 0, 0] = [second_start]
    work["n", 0, 0] = [new_rows]

    def do(names):
        for name in names:
            for f in work.pop(name):
                f()

    def layer_loop(tag, n, body):
        first = ORDER.index((tag, 0, 0))
        do(ORDER[done[0]:first])
        ends = [ORDER.index((tag, l, 0)) for l in range(n)]

        def step(l, _):
            for k in range(1, n):
                names = ORDER[ends[k - 1] + 1:ends[k]]
                if names:
                    pl.when(l == k)(functools.partial(do, names))
            body(l)
            return 0

        lax.fori_loop(0, n, step, 0)
        done[0] = ends[-1] + 1

    done = [0]
    layer_loop("f", layers, forward_one)

    def forward_step(l):
        forward_two(l)

    layer_loop("s", layers - 1, forward_step)
    do(ORDER[done[0]:])
    assert not work
    out = [load(h, hlast, 0), load(lossbuf, loss, 1)]
    for c in out:
        c.start()
    for u in range(units):
        again[u].drain()
        red[u].drain()
    wshuf.to_rows_finish()
    mshuf.to_rows_finish()
    for c in out:
        c.wait()


def gradient_slots():
    free, held = list(range(G_SLOTS)), {}
    for tag, n, k in ORDER:
        if tag == "g" and k != 1:
            held[2 * n + (k == 0)] = free.pop(0)
        if tag == "r" and k == 0:
            free.append(held[n])
    return held


def make_step(grid, layers, tok, d_model, d_ff, n_dev):
    nz, ny, nx, nc = grid
    units = 2 * layers
    group = nx * nc
    hbm = pl.BlockSpec(memory_space=pl.ANY)
    sds = jax.ShapeDtypeStruct
    tile = (16, LANES)
    dma = pltpu.SemaphoreType.DMA
    thirds = (units + 2) // 3
    outs = (sds((layers, 2, d_ff), F32), sds((layers, 4, d_model), F32), sds((layers, 2, d_ff), F32), sds((layers, 4, d_model), F32),
            sds((1, tok), F32), sds((tok, d_model), F32), sds((SPILLED, tok, d_ff), F32))
    shuffled = [pltpu.VMEM((group, layers, 2, LANES), F32), pltpu.VMEM((group // 2, layers, 4, LANES), F32)]
    scratch = [
        pltpu.VMEM((units, *grid, *tile), BF16),
        pltpu.VMEM((2, tok, d_ff), F32),
        pltpu.VMEM((layers, tok, d_model), BF16),
        pltpu.VMEM((layers, tok, d_ff), BF16),
        pltpu.VMEM((tok, d_model), F32),
        pltpu.VMEM((tok, d_model), BF16),
        pltpu.VMEM((G_SLOTS, *grid, *tile), BF16),
        pltpu.VMEM((units, nz, ny, nx, *tile), BF16),
        pltpu.VMEM((2 * thirds, nx - 1, nz, ny, *tile), BF16),
        pltpu.VMEM((thirds, nz - 1, ny, nx, *tile), BF16),
        pltpu.VMEM((units, max(ny, nx) - 1, max(nz, nx), *tile), BF16),
        pltpu.VMEM((units, max(nz, nx) - 1, *tile), BF16),
        *shuffled, *shuffled,
        pltpu.VMEM((layers, 2, d_ff), F32), pltpu.VMEM((layers, 4, d_model), F32),
        pltpu.VMEM((units, *tile), F32), pltpu.VMEM((units, *tile), F32),
        pltpu.VMEM((1, tok), F32),
        dma((units, 4)), dma((units, 10)), dma((units, 4)), dma((units, 10)), dma((8,)), dma((4 + SPILLED,)),
    ]
    return pl.pallas_call(
        functools.partial(step_kernel, grid, 1.0 / (n_dev * tok * d_model)),
        out_shape=outs, in_specs=[hbm] * 8, out_specs=[hbm] * 7, scratch_shapes=scratch,
        compiler_params=pltpu.CompilerParams(collective_id=0, has_side_effects=True, vmem_limit_bytes=67043328),
        name="train_step")


def hand_over(*refs):
    n = len(refs) // 2
    for src, dst in zip(refs[:n], refs[n:]):
        if len(dst.shape) < len(src.shape):
            dst[...] = src[0, :]
        else:
            dst[...] = src[...]


def solution(mesh):
    n_dev = mesh.shape["data"]
    w_spec = P(None, "data", None)
    row_spec = P("data", None)

    def device_step(w_one, w_two, mom_one, mom_two, x_zero, y_zero, x_one, y_one):
        tok, d_model = x_zero.shape
        step = make_step(GRID, w_one.shape[0], tok, d_model, w_one.shape[2], n_dev)
        made = step(w_one, w_two, mom_one, mom_two, x_zero, y_zero, x_one, y_one)[:6]
        outs = [jax.ShapeDtypeStruct(v.shape, v.dtype) for v in made]
        outs[4] = jax.ShapeDtypeStruct((tok,), F32)
        vmem = pl.BlockSpec(memory_space=pltpu.VMEM)
        return pl.pallas_call(hand_over, out_shape=tuple(outs), in_specs=[vmem] * 6, out_specs=[vmem] * 6, name="hand_over")(*made)

    return jax.shard_map(device_step, mesh=mesh, in_specs=(w_spec, w_spec, w_spec, w_spec, row_spec, row_spec, row_spec, row_spec),
                         out_specs=(w_spec, w_spec, w_spec, w_spec, P("data"), row_spec), check_vma=False)
```

```python
import functools
import jax
import jax.numpy as jnp
from jax import lax
from jax.experimental import pallas as pl
from jax.experimental.pallas import tpu as pltpu
from jax.sharding import PartitionSpec as P

LEARN_RATE = 0.1
MOMENTUM = 0.9
F32, BF16 = jnp.float32, jnp.bfloat16
GRID = (8, 4, 4, 2)
ORDERS = (("z", "x", "y"), ("z", "y", "x"), ("x", "y", "z"), ("y", "x", "z"))
COLOURS = (0, 1, 2, 0, 1, 3, 0, 1, 2, 0, 1, 3)
GELU_SCALE = 0.7978845608028654
GELU_CUBE = 0.044715
G_SLOTS = 6
LANES = 128
SPILLED = 4

ORDER = (
    ("a", 11, 0), ("a", 10, 0), ("a", 3, 0), ("a", 2, 0), ("a", 1, 0), ("a", 4, 0), ("a", 8, 0), ("a", 0, 0), ("a", 5, 0), ("m", 0, 0), ("a", 6, 0),
    ("a", 7, 0), ("a", 11, 1), ("a", 2, 1), ("a", 5, 1), ("a", 8, 1), ("a", 9, 0), ("a", 10, 1), ("a", 3, 1), ("a", 1, 1), ("a", 11, 2), ("a", 2, 2),
    ("a", 4, 1), ("a", 5, 2), ("a", 8, 2), ("a", 0, 1), ("a", 6, 1), ("a", 7, 1), ("a", 3, 2), ("a", 9, 1), ("a", 11, 3), ("a", 1, 2), ("a", 2, 3),
    ("a", 4, 2), ("a", 0, 2), ("a", 5, 3), ("a", 6, 2), ("a", 8, 3), ("a", 3, 3), ("a", 7, 2), ("a", 11, 4), ("a", 2, 4), ("a", 0, 3), ("a", 1, 3),
    ("a", 5, 4), ("a", 4, 3), ("a", 8, 4), ("a", 6, 3), ("a", 11, 5), ("a", 3, 4), ("a", 7, 3), ("a", 2, 5), ("a", 9, 2), ("a", 0, 4), ("a", 3, 5),
    ("a", 1, 4), ("a", 10, 2), ("a", 5, 5), ("a", 6, 4), ("a", 4, 4), ("a", 0, 5), ("a", 1, 5), ("f", 0, 0), ("a", 2, 6), ("a", 11, 6), ("a", 6, 5),
    ("a", 4, 5), ("a", 8, 5), ("m", 0, 1), ("a", 5, 6), ("a", 7, 4), ("a", 9, 3), ("a", 2, 7), ("f", 1, 0), ("a", 11, 7), ("a", 10, 3), ("a", 5, 7),
    ("f", 2, 0), ("a", 7, 5), ("a", 9, 4), ("a", 8, 6), ("f", 3, 0), ("a", 10, 4), ("a", 9, 5), ("a", 8, 7), ("f", 4, 0), ("a", 10, 5), ("d", 0, 0),
    ("f", 5, 0), ("l", 0, 0), ("g", 5, 0), ("g", 5, 1), ("g", 4, 0), ("g", 4, 1), ("g", 4, 2), ("r", 11, 0), ("g", 3, 0), ("g", 3, 1), ("r", 8, 0),
    ("g", 3, 2), ("r", 11, 1), ("r", 9, 0), ("g", 5, 2), ("r", 7, 0), ("g", 2, 0), ("r", 6, 0), ("g", 2, 1), ("r", 8, 1), ("r", 10, 0), ("r", 11, 2),
    ("g", 1, 0), ("r", 9, 1), ("g", 1, 1), ("r", 5, 0), ("r", 7, 1), ("g", 1, 2), ("r", 8, 2), ("r", 6, 1), ("g", 0, 0), ("r", 3, 0), ("r", 10, 1),
    ("r", 11, 3), ("g", 0, 1), ("h", 0, 0), ("r", 2, 0), ("r", 9, 2), ("r", 5, 1), ("g", 0, 2), ("r", 7, 2), ("g", 2, 2), ("r", 8, 3), ("r", 11, 4),
    ("r", 1, 0), ("r", 10, 2), ("r", 6, 2), ("r", 0, 0), ("r", 2, 1), ("r", 3, 1), ("r", 4, 0), ("r", 9, 3), ("r", 5, 2), ("r", 7, 3), ("r", 11, 5),
    ("r", 10, 3), ("r", 8, 4), ("r", 2, 2), ("r", 1, 1), ("r", 0, 1), ("r", 5, 3), ("r", 6, 3), ("r", 3, 2), ("u", 9, 0), ("r", 4, 1), ("u", 11, 0),
    ("r", 2, 3), ("u", 7, 0), ("r", 0, 2), ("u", 10, 0), ("r", 1, 2), ("r", 8, 5), ("r", 5, 4), ("r", 2, 4), ("b", 11, 0), ("r", 3, 3), ("u", 6, 0),
    ("b", 9, 0), ("r", 4, 2), ("r", 1, 3), ("b", 7, 0), ("r", 0, 3), ("u", 8, 0), ("r", 2, 5), ("r", 5, 5), ("b", 11, 1), ("b", 10, 0), ("u", 3, 0),
    ("b", 9, 1), ("r", 4, 3), ("b", 6, 0), ("u", 2, 0), ("b", 7, 1), ("u", 5, 0), ("u", 1, 0), ("b", 11, 2), ("b", 8, 0), ("u", 0, 0), ("b", 10, 1),
    ("b", 9, 2), ("b", 2, 0), ("u", 4, 0), ("n", 0, 0), ("b", 5, 0), ("b", 11, 3), ("b", 6, 1), ("b", 3, 0), ("b", 8, 1), ("b", 7, 2), ("b", 9, 3),
    ("b", 1, 0), ("b", 0, 0), ("b", 2, 1), ("b", 9, 4), ("b", 11, 4), ("b", 4, 0), ("b", 5, 1), ("b", 10, 2), ("b", 3, 1), ("b", 8, 2), ("b", 7, 3),
    ("b", 2, 2), ("b", 1, 1), ("b", 11, 5), ("b", 7, 4), ("b", 0, 1), ("b", 10, 3), ("b", 5, 2), ("b", 4, 1), ("b", 11, 6), ("b", 10, 4), ("b", 8, 3),
    ("b", 3, 2), ("b", 2, 3), ("b", 6, 2), ("b", 5, 3), ("b", 1, 2), ("b", 0, 2), ("b", 8, 4), ("b", 3, 3), ("b", 4, 2), ("b", 2, 4), ("b", 6, 3),
    ("b", 3, 4), ("b", 1, 3), ("b", 5, 4), ("b", 0, 3), ("b", 6, 4), ("b", 8, 5), ("b", 1, 4), ("b", 2, 5), ("b", 4, 3), ("b", 0, 4), ("s", 0, 0),
    ("b", 8, 6), ("b", 5, 5), ("b", 2, 6), ("s", 1, 0), ("b", 5, 6), ("b", 4, 4), ("s", 2, 0), ("s", 3, 0), ("s", 4, 0), ("s", 5, 0),
)


def start_copy(src, dst, send_sem, recv_sem, dev):
    pltpu.make_async_remote_copy(src_ref=src, dst_ref=dst, send_sem=send_sem, recv_sem=recv_sem,
                                 device_id=(dev,), device_id_type=pl.DeviceIdType.MESH).start()


def wait_bytes(ref, sem):
    pltpu.make_async_copy(ref, ref, sem).wait()


class Place:
    def __init__(self, grid):
        self.grid = grid
        nz, ny, nx, nc = grid
        me = lax.axis_index("data")
        self.me = me
        self.c = lax.rem(me, nc)
        self.x = lax.rem(me // nc, nx)
        self.y = lax.rem(me // (nc * nx), ny)
        self.z = me // (nc * nx * ny)
        self.sign = 1 - 2 * self.c
        self.size = {"z": nz, "y": ny, "x": nx}
        self.pos = {"z": self.z, "y": self.y, "x": self.x}
        self.stride = {"z": ny * nx * nc, "y": nx * nc, "x": nc}
        self.sib = me + 1 - 2 * self.c
        self.m = lax.rem(me, nc * nx)
        self.base = me - self.m

    def wrap(self, v, d):
        n = self.size[d]
        return lax.rem(v + 2 * n, n)

    def dev(self, d, v):
        return self.me + (v - self.pos[d]) * self.stride[d]

    def far(self, d):
        return self.size[d] // 2

    def near(self, d):
        return (self.size[d] - 1) // 2


def block_of(buf, lead, place, done, d, v, tail=()):
    idx = []
    for k in ("z", "y", "x"):
        if k in done:
            idx.append(slice(None))
        elif k == d:
            idx.append(v)
        else:
            idx.append(place.pos[k])
    return buf.at[(*lead, *idx, *tail)]


def ring_sem(place, d, way, step):
    return step - 1 if way == 1 else place.far(d) + step - 1


class Sems:
    def __init__(self, place, colours, send, recv, per_unit):
        self.send, self.recv = send, recv
        self.kind = [int(ORDERS[c][2] == "z") for c in colours]
        self.base, n = [], 0
        for c in colours:
            self.base.append(n)
            n += self.count(place.grid, c)
        self.swaps = per_unit

    @staticmethod
    def count(grid, c):
        return 3 + grid["zyx".index(ORDERS[c][2])] - 1

    def r(self, u, k):
        return self.recv.at[self.base[u] + k]

    def s(self, u, stage):
        if stage == 3:
            return self.send.at[6 + (u if self.swaps else 0)]
        return self.send.at[2 * stage + self.kind[u]]


class Gather:
    def __init__(self, place, buf, u, order, sems):
        self.p, self.buf, self.u, self.order, self.sems = place, buf, u, order, sems

    def block(self, stage, v):
        return block_of(self.buf, (self.u,), self.p, self.order[:stage], self.order[stage], v, (self.p.c,))

    def many(self, stage):
        return self.block(stage, pl.ds(0, self.p.size[self.order[stage]] - 1))

    def direct_start(self, stage):
        p, d = self.p, self.order[stage]
        own = self.block(stage, p.pos[d])
        for k in range(1, p.size[d]):
            start_copy(own, own, self.sems.s(self.u, stage), self.sems.r(self.u, stage), p.dev(d, p.wrap(p.pos[d] + k, d)))

    def direct_wait(self, stage):
        if self.p.size[self.order[stage]] > 1:
            wait_bytes(self.many(stage), self.sems.r(self.u, stage))

    def ring_send(self, way, step):
        p, d = self.p, self.order[2]
        s = p.sign * way
        ref = self.block(2, p.wrap(p.pos[d] - (step - 1) * s, d))
        start_copy(ref, ref, self.sems.s(self.u, 2), self.sems.r(self.u, 3 + ring_sem(p, d, way, step)), p.dev(d, p.wrap(p.pos[d] + s, d)))

    def ways(self):
        d = self.order[2]
        return ((1, self.p.far(d)), (-1, self.p.near(d)))

    def ring_start(self):
        for way, n in self.ways():
            if n:
                self.ring_send(way, 1)
        self.swap_start(0)

    def ring_step(self, step):
        p, d = self.p, self.order[2]
        for way, n in self.ways():
            if step <= n:
                ref = self.block(2, p.wrap(p.pos[d] - step * p.sign * way, d))
                wait_bytes(ref, self.sems.r(self.u, 3 + ring_sem(p, d, way, step)))
                if step < n:
                    self.ring_send(way, step + 1)
                self.swap_start(step * way)

    def swap_ref(self, c):
        return self.buf.at[self.u, :, :, :, c]

    def swap_start(self, k):
        d = self.order[2]
        ref = self.block(2, self.p.wrap(self.p.pos[d] - k * self.p.sign, d))
        start_copy(ref, ref, self.sems.s(self.u, 3), self.sems.r(self.u, 2), self.p.sib)

    def swap_wait(self):
        wait_bytes(self.swap_ref(1 - self.p.c), self.sems.r(self.u, 2))

    def events(self):
        part = functools.partial
        out = [[part(self.direct_start, 0)],
               [part(self.direct_wait, 0), part(self.direct_start, 1)],
               [part(self.direct_wait, 1), self.ring_start]]
        out += [[part(self.ring_step, step)] for step in range(1, self.p.far(self.order[2]) + 1)]
        return out + [[self.swap_wait]]


def drain_gather(place, buf, sems):
    nz, ny, nx, nc = place.grid
    heavy = sum(sems.kind)
    light = len(sems.kind) - heavy
    sent = (buf.at[0:light, 0:nz - 1, 0, 0, 0], buf.at[0:heavy, 0, 0, 0:nx - 1, 0],
            buf.at[0:light, :, 0:nx - 1, 0, 0], buf.at[0:heavy, 0, 0:nx - 1, :, 0],
            buf.at[0:light, :, 0:ny - 1, :, 0], buf.at[0:heavy, 0:nz - 1, :, :, 0], buf.at[:, :, :, :, 0])
    for k, ref in enumerate(sent):
        wait_bytes(ref, sems.send.at[k])


def add_into(dst, *srcs):
    total = dst[...].astype(F32)
    for s in srcs:
        total = total + s[...].astype(F32)
    dst[...] = total.astype(BF16)


class Reduce:
    def __init__(self, place, g, gslot, part, ring, rows, tiles, u, order, sems):
        self.p, self.g, self.gslot, self.part, self.u, self.order, self.sems = place, g, gslot, part, u, order, sems
        self.ring = ring
        n0 = place.size[order[0]]
        self.rows = lambda k: rows.at[k, pl.ds(0, n0)]
        self.tiles = lambda k: tiles.at[k]

    def block(self, stage, v):
        return block_of(self.part, (self.u,), self.p, self.order[:stage], self.order[stage], v)

    def swap_start(self):
        start_copy(self.g.at[self.gslot, :, :, :, 1 - self.p.c], self.part.at[self.u],
                   self.sems.s(self.u, 3), self.sems.r(self.u, 2), self.p.sib)

    def swap_wait(self):
        wait_bytes(self.part.at[self.u], self.sems.r(self.u, 2))
        p = self.p

        def add(k, _):
            add_into(self.part.at[self.u, k], self.g.at[self.gslot, k, :, :, p.c])
            return 0

        lax.fori_loop(0, p.size["z"], add, 0)
        wait_bytes(self.part.at[self.u], self.sems.s(self.u, 3))

    def ways(self):
        d = self.order[2]
        return ((1, self.p.far(d)), (-1, self.p.near(d)))

    def ring_send(self, way, step, n):
        p, d = self.p, self.order[2]
        s = p.sign * way
        k = ring_sem(p, d, way, step)
        src = self.block(2, p.wrap(p.pos[d] + n * s, d)) if step == 1 else self.ring(k - 1)
        start_copy(src, self.ring(k), self.sems.s(self.u, 2), self.sems.r(self.u, 3 + k), p.dev(d, p.wrap(p.pos[d] + s, d)))

    def ring_start(self):
        for way, n in self.ways():
            if n:
                self.ring_send(way, 1, n)

    def ring_step(self, step):
        p, d = self.p, self.order[2]
        for way, n in self.ways():
            if step <= n:
                k = ring_sem(p, d, way, step)
                wait_bytes(self.ring(k), self.sems.r(self.u, 3 + k))
                if step < n:
                    add_into(self.ring(k), self.block(2, p.wrap(p.pos[d] + (n - step) * p.sign * way, d)))
                    self.ring_send(way, step + 1, n)
        if step == p.far(d):
            add_into(self.block(2, p.pos[d]), *[self.ring(ring_sem(p, d, way, n)) for way, n in self.ways() if n])

    def direct_start(self, stage):
        p, d = self.p, self.order[stage]
        land = self.rows if stage == 1 else self.tiles
        for k in range(1, p.size[d]):
            v = p.wrap(p.pos[d] + k, d)
            start_copy(self.block(stage, v), land(k - 1), self.sems.s(self.u, stage), self.sems.r(self.u, stage), p.dev(d, v))

    def direct_wait(self, stage):
        n = self.p.size[self.order[stage]]
        if n > 1:
            wait_bytes((self.rows if stage == 1 else self.tiles)(pl.ds(0, n - 1)), self.sems.r(self.u, stage))

    def row_sum(self):
        self.direct_wait(1)
        n = self.p.size[self.order[1]]
        if n > 1:
            add_into(self.block(1, self.p.pos[self.order[1]]), *[self.rows(k) for k in range(n - 1)])

    def tile_sum(self):
        self.direct_wait(0)
        total = self.block(0, self.p.pos[self.order[0]])[...].astype(F32)
        for k in range(self.p.size[self.order[0]] - 1):
            total = total + self.tiles(k)[...].astype(F32)
        return total.astype(BF16).astype(F32)

    def events(self):
        part = functools.partial
        out = [[self.swap_wait, self.ring_start]]
        out += [[part(self.ring_step, step)] for step in range(1, self.p.far(self.order[2]) + 1)]
        out[-1].append(part(self.direct_start, 1))
        return out + [[self.row_sum, part(self.direct_start, 0)]]


def drain_reduce(place, ring_ab, ring_c, rows, tiles, sems):
    nz, ny, nx, nc = place.grid
    heavy = sum(sems.kind)
    light = len(sems.kind) - heavy
    sent = (tiles.at[0:light, 0:nz - 1], tiles.at[0:heavy, 0:nx - 1], rows.at[0:light, :, 0:nz], rows.at[0:heavy, :, 0:nx], ring_ab, ring_c)
    for k, ref in enumerate(sent):
        wait_bytes(ref, sems.send.at[k])


def enter(p):
    barrier = pltpu.get_barrier_semaphore()
    group = p.grid[2] * p.grid[3]
    peers = [p.base + lax.rem(p.m + k, group) for k in range(1, group)]
    for d in ("y", "z"):
        peers += [p.dev(d, p.wrap(p.pos[d] + k, d)) for k in range(1, p.size[d])]
    for peer in peers:
        pl.semaphore_signal(barrier, inc=1, device_id=(peer,), device_id_type=pl.DeviceIdType.MESH)
    pl.semaphore_wait(barrier, len(peers))


def lanes(ref, j):
    return ref.at[:, :, pl.ds(pl.multiple_of(j * LANES, LANES), LANES)]


class Shuffle:
    def __init__(self, place, one, two, sems, k0):
        self.p, self.one, self.two = place, one, two
        self.sem = lambda k: sems.at[k0 + k]
        self.group = place.grid[2] * place.grid[3]
        self.half = self.group // 2
        self.low = (place.m // self.half) * self.half
        self.mine = place.m - self.low

    def to_tiles_start(self, src1, src2):
        p = self.p
        for k in range(1, self.group):
            j = lax.rem(p.m + k, self.group)
            start_copy(lanes(src1, j), self.one.at[p.m], self.sem(0), self.sem(1), p.base + j)
        for k in range(1, self.half):
            j = lax.rem(self.mine + k, self.half)
            start_copy(lanes(src2, j), self.two.at[self.mine], self.sem(2), self.sem(3), p.base + self.low + j)

    def to_tiles_own(self, src1, src2):
        p = self.p
        pltpu.make_async_copy(lanes(src1, p.m), self.one.at[p.m], self.sem(1)).start()
        pltpu.make_async_copy(lanes(src2, self.mine), self.two.at[self.mine], self.sem(3)).start()

    def drain_sends(self):
        wait_bytes(self.one.at[pl.ds(0, self.group - 1)], self.sem(0))
        wait_bytes(self.two.at[pl.ds(0, self.half - 1)], self.sem(2))

    def to_tiles_finish(self, tiles):
        wait_bytes(self.one, self.sem(1))
        wait_bytes(self.two, self.sem(3))
        for l in range(self.one.shape[1]):
            for m in range(self.group):
                tiles[2 * l, 2 * m:2 * m + 2, :] = self.one[m, l]
            for m in range(self.half):
                tiles[2 * l + 1, 4 * m:4 * m + 4, :] = self.two[m, l]

    def put_rows(self, u, tile):
        if u % 2 == 0:
            for m in range(self.group):
                self.one[m, u // 2] = tile[2 * m:2 * m + 2, :]
        else:
            for m in range(self.half):
                self.two[m, u // 2] = tile[4 * m:4 * m + 4, :]

    def to_rows_start(self, dst1, dst2):
        p = self.p
        pltpu.make_async_copy(self.one.at[p.m], lanes(dst1, p.m), self.sem(1)).start()
        pltpu.make_async_copy(self.two.at[self.mine], lanes(dst2, self.mine), self.sem(3)).start()
        for k in range(1, self.group):
            j = lax.rem(p.m + k, self.group)
            start_copy(self.one.at[j], lanes(dst1, p.m), self.sem(0), self.sem(1), p.base + j)
        for k in range(1, self.half):
            j = lax.rem(self.mine + k, self.half)
            start_copy(self.two.at[j], lanes(dst2, self.mine), self.sem(2), self.sem(3), p.base + self.low + j)

    def to_rows_finish(self):
        wait_bytes(self.one, self.sem(1))
        wait_bytes(self.two, self.sem(3))
        self.drain_sends()


def w_one_of(wbuf, l):
    nz, ny, nx, nc = wbuf.shape[1:5]
    cols = [wbuf[2 * l, :, :, m // nc, m % nc].reshape(nz * ny * 16, LANES) for m in range(nx * nc)]
    return jnp.concatenate(cols, axis=1)


def w_two_of(wbuf, l):
    nz, ny, nx, nc = wbuf.shape[1:5]
    half = nx * nc // 2
    cols = []
    for b in range(half):
        pair = [wbuf[2 * l + 1, :, :, (r * half + b) // nc, b % nc].reshape(nz * ny, 1, 16, LANES) for r in range(2)]
        cols.append(jnp.concatenate(pair, axis=1).reshape(nz * ny * 32, LANES))
    return jnp.concatenate(cols, axis=1)


def contract(a, b, da, db):
    return lax.dot_general(a, b, (((da,), (db,)), ((), ())), preferred_element_type=F32)


def gelu_parts(u):
    w = GELU_SCALE + (GELU_SCALE * GELU_CUBE) * (u * u)
    gate = 0.5 + 0.5 * jnp.tanh(u * w)
    return u * gate, gate, w


def gelu(u):
    return gelu_parts(u)[0]


def gelu_and_slope(u):
    z, gate, w = gelu_parts(u)
    return z, gate + (z - z * gate) * (6.0 * w - 4.0 * GELU_SCALE)


def step_kernel(grid, batch_scale, w1, w2, m1, m2, x0, y0, x1, y1, nw1, nw2, nm1, nm2, loss, hlast, spill,
                wbuf, slope, act, hid, h, dlow, g, part, ring_ab, ring_c, rows, tiles3,
                wone, wtwo, mone, mtwo, wrow1, wrow2, wt, mt, lossbuf,
                gsend, grecv, rsend, rrecv, shuf, local):
    p = Place(grid)
    layers = w1.shape[0]
    units = 2 * layers
    nz, ny, nx, nc = grid
    tok, d_model = h.shape
    d_ff = hid.shape[2]

    def load(src, dst, k):
        return pltpu.make_async_copy(src, dst, local.at[k])

    loads = {"x0": load(x0, act.at[0], 0), "y0": load(y0, dlow, 1),
             "x1": load(x1, act.at[layers - 1], 2), "y1": load(y1, act.at[layers - 2], 3)}
    stage = [load(w1, wrow1, 2), load(w2, wrow2, 3)]
    wshuf = Shuffle(p, wone, wtwo, shuf, 0)
    mshuf = Shuffle(p, mone, mtwo, shuf, 4)
    for c in stage:
        c.start()
    wshuf.to_tiles_own(w1, w2)
    mshuf.to_tiles_own(m1, m2)
    loads["x0"].start()
    loads["y0"].start()
    enter(p)
    for c in stage:
        c.wait()
    wshuf.to_tiles_start(wrow1, wrow2)

    def own_tile(u):
        wbuf[u, p.z, p.y, p.x, p.c] = wt[u].astype(BF16)

    wshuf.to_tiles_finish(wt)
    for u in range(units):
        own_tile(u)
    loads["x0"].wait()
    h[...] = act[0].astype(F32)

    def spill_copy(l):
        return load(slope.at[lax.rem(l, 2)], spill.at[l], 4 + l)

    def unspill_copy(l):
        return load(spill.at[l], slope.at[l % 2], 4 + l)

    def forward_one(l):
        @pl.when(jnp.logical_and(l >= 2, l < SPILLED + 2))
        def _():
            spill_copy(l - 2).wait()

        a = h[...].astype(BF16)
        act[l] = a
        z, s = gelu_and_slope(jnp.dot(a, w_one_of(wbuf, l), preferred_element_type=F32))
        z = z.astype(BF16)
        slope[lax.rem(l, 2)] = s
        hid[l] = z
        h[...] += jnp.dot(z, w_two_of(wbuf, l), preferred_element_type=F32)

        @pl.when(l < SPILLED)
        def _():
            spill_copy(l).start()

    def loss_slope():
        loads["y0"].wait()
        d = (h[...] - dlow[...].astype(F32)) * batch_scale
        h[...] = d
        dlow[...] = d.astype(BF16)

    gsems = Sems(p, COLOURS, gsend, grecv, False)
    rsems = Sems(p, COLOURS, rsend, rrecv, True)
    slots = gradient_slots()
    first = [Gather(p, wbuf, u, ORDERS[COLOURS[u]], gsems) for u in range(units)]
    again = [Gather(p, wbuf, u, ORDERS[COLOURS[u]], gsems) for u in range(units)]
    red = []
    for u in range(units):
        n = sum(k == rsems.kind[u] for k in rsems.kind[:u])
        ring = functools.partial(lambda buf, n, k: buf.at[n, k], ring_c if rsems.kind[u] else ring_ab, n)
        red.append(Reduce(p, g, slots[u], part, ring, rows.at[u], tiles3.at[u], u, ORDERS[COLOURS[u]], rsems))

    def grad_two(l):
        slot = red[2 * l + 1].gslot
        half = nx * nc // 2
        v = contract(hid[l], dlow[...], 0, 0).astype(BF16).reshape(nz, ny, 2, 16, d_model)
        for b in range(half):
            for r in range(2):
                g[slot, :, :, (r * half + b) // nc, b % nc] = v[:, :, r, :, LANES * b:LANES * b + LANES]

    def back_hidden(l):
        if l + 2 < layers:
            unspill_copy(l).wait()
        q = contract(dlow[...], w_two_of(wbuf, l), 1, 1)
        v = (slope[l % 2] * q).astype(BF16)
        hid[l] = v
        if l:
            d = h[...] + contract(v, w_one_of(wbuf, l), 1, 1)
            h[...] = d
            dlow[...] = d.astype(BF16)
        red[2 * l + 1].swap_start()
        if l >= 2:
            unspill_copy(l - 2).start()

    def grad_one(l):
        slot = red[2 * l].gslot
        v = contract(act[l], hid[l], 0, 0).astype(BF16).reshape(nz, ny, 16, d_ff)
        for m in range(nx * nc):
            g[slot, :, :, m // nc, m % nc] = v[:, :, :, LANES * m:LANES * m + LANES]
        red[2 * l].swap_start()
        if l == layers - 1:
            loads["x1"].start()
        if l == layers - 2:
            loads["y1"].start()

    def update(u):
        total = red[u].tile_sum()
        mom = MOMENTUM * mt[u] + total
        w = wt[u] - LEARN_RATE * mom
        wbuf[u, p.z, p.y, p.x, p.c] = w.astype(BF16)
        wt[u] = w
        mt[u] = mom
        again[u].direct_start(0)

    def moments_start():
        mshuf.to_tiles_start(m1, m2)

    def moments_ready():
        mshuf.to_tiles_finish(mt)
        mshuf.drain_sends()
        wshuf.drain_sends()

    def second_start():
        loads["x1"].wait()
        h[...] = act[layers - 1].astype(F32)

    def forward_two(l):
        z = gelu(jnp.dot(h[...].astype(BF16), w_one_of(wbuf, l), preferred_element_type=F32)).astype(BF16)
        v = h[...] + jnp.dot(z, w_two_of(wbuf, l), preferred_element_type=F32)
        h[...] = v
        return v

    def forward_last():
        loads["y1"].wait()
        e = forward_two(layers - 1) - act[layers - 2].astype(F32)
        e = e * e
        s = e[:, :LANES]
        for k in range(1, d_model // LANES):
            s = s + e[:, LANES * k:LANES * k + LANES]
        lossbuf[...] = jnp.sum(s.T, axis=0, keepdims=True) * (1.0 / (2 * d_model))

    def new_rows():
        for u in range(units):
            wshuf.put_rows(u, wt[u])
            mshuf.put_rows(u, mt[u])
        wshuf.to_rows_start(nw1, nw2)
        mshuf.to_rows_start(nm1, nm2)

    work = {}
    for u in range(units):
        for k, ev in enumerate(first[u].events()):
            work["a", u, k] = ev
        for k, ev in enumerate(red[u].events()):
            work["r", u, k] = ev
        work["u", u, 0] = [functools.partial(update, u)]
        for k, ev in enumerate(again[u].events()[1:]):
            work["b", u, k] = ev
    for l in range(layers):
        work["g", l, 0] = [functools.partial(grad_two, l)]
        work["g", l, 1] = [functools.partial(back_hidden, l)]
        work["g", l, 2] = [functools.partial(grad_one, l)]
    work["s", layers - 1, 0] = [forward_last]
    work["d", 0, 0] = [functools.partial(drain_gather, p, wbuf, gsems)]
    work["l", 0, 0] = [loss_slope]
    work["m", 0, 0] = [moments_start]
    work["m", 0, 1] = [moments_ready]
    work["h", 0, 0] = [second_start]
    work["n", 0, 0] = [new_rows]

    def do(names):
        for name in names:
            for f in work.pop(name):
                f()

    def layer_loop(tag, n, body):
        first = ORDER.index((tag, 0, 0))
        do(ORDER[done[0]:first])
        ends = [ORDER.index((tag, l, 0)) for l in range(n)]

        def step(l, _):
            for k in range(1, n):
                names = ORDER[ends[k - 1] + 1:ends[k]]
                if names:
                    pl.when(l == k)(functools.partial(do, names))
            body(l)
            return 0

        lax.fori_loop(0, n, step, 0)
        done[0] = ends[-1] + 1

    done = [0]
    layer_loop("f", layers, forward_one)

    def forward_step(l):
        forward_two(l)

    layer_loop("s", layers - 1, forward_step)
    do(ORDER[done[0]:])
    assert not work
    out = [load(h, hlast, 0), load(lossbuf, loss, 1)]
    for c in out:
        c.start()
    drain_gather(p, wbuf, gsems)
    drain_reduce(p, ring_ab, ring_c, rows, tiles3, rsems)
    wshuf.to_rows_finish()
    mshuf.to_rows_finish()
    for c in out:
        c.wait()


def gradient_slots():
    free, held = list(range(G_SLOTS)), {}
    for tag, n, k in ORDER:
        if tag == "g" and k != 1:
            held[2 * n + (k == 0)] = free.pop(0)
        if tag == "r" and k == 0:
            free.append(held[n])
    return held


def make_step(grid, layers, tok, d_model, d_ff, n_dev):
    nz, ny, nx, nc = grid
    units = 2 * layers
    group = nx * nc
    hbm = pl.BlockSpec(memory_space=pl.ANY)
    sds = jax.ShapeDtypeStruct
    tile = (16, LANES)
    dma = pltpu.SemaphoreType.DMA
    heavy = sum(ORDERS[c][2] == "z" for c in COLOURS)
    recvs = sum(Sems.count(grid, c) for c in COLOURS)
    outs = (sds((layers, 2, d_ff), F32), sds((layers, 4, d_model), F32), sds((layers, 2, d_ff), F32), sds((layers, 4, d_model), F32),
            sds((1, tok), F32), sds((tok, d_model), F32), sds((SPILLED, tok, d_ff), F32))
    shuffled = [pltpu.VMEM((group, layers, 2, LANES), F32), pltpu.VMEM((group // 2, layers, 4, LANES), F32)]
    scratch = [
        pltpu.VMEM((units, *grid, *tile), BF16),
        pltpu.VMEM((2, tok, d_ff), F32),
        pltpu.VMEM((layers, tok, d_model), BF16),
        pltpu.VMEM((layers, tok, d_ff), BF16),
        pltpu.VMEM((tok, d_model), F32),
        pltpu.VMEM((tok, d_model), BF16),
        pltpu.VMEM((G_SLOTS, *grid, *tile), BF16),
        pltpu.VMEM((units, nz, ny, nx, *tile), BF16),
        pltpu.VMEM((units - heavy, nx - 1, nz, ny, *tile), BF16),
        pltpu.VMEM((heavy, nz - 1, ny, nx, *tile), BF16),
        pltpu.VMEM((units, max(ny, nx) - 1, max(nz, nx), *tile), BF16),
        pltpu.VMEM((units, max(nz, nx) - 1, *tile), BF16),
        *shuffled, *shuffled,
        pltpu.VMEM((layers, 2, d_ff), F32), pltpu.VMEM((layers, 4, d_model), F32),
        pltpu.VMEM((units, *tile), F32), pltpu.VMEM((units, *tile), F32),
        pltpu.VMEM((1, tok), F32),
        dma((7,)), dma((recvs,)), dma((6 + units,)), dma((recvs,)), dma((8,)), dma((4 + SPILLED,)),
    ]
    return pl.pallas_call(
        functools.partial(step_kernel, grid, 1.0 / (n_dev * tok * d_model)),
        out_shape=outs, in_specs=[hbm] * 8, out_specs=[hbm] * 7, scratch_shapes=scratch,
        compiler_params=pltpu.CompilerParams(collective_id=0, has_side_effects=True, vmem_limit_bytes=67043328),
        name="train_step")


def hand_over(*refs):
    n = len(refs) // 2
    for src, dst in zip(refs[:n], refs[n:]):
        if len(dst.shape) < len(src.shape):
            dst[...] = src[0, :]
        else:
            dst[...] = src[...]


def solution(mesh):
    n_dev = mesh.shape["data"]
    w_spec = P(None, "data", None)
    row_spec = P("data", None)

    def device_step(w_one, w_two, mom_one, mom_two, x_zero, y_zero, x_one, y_one):
        tok, d_model = x_zero.shape
        step = make_step(GRID, w_one.shape[0], tok, d_model, w_one.shape[2], n_dev)
        made = step(w_one, w_two, mom_one, mom_two, x_zero, y_zero, x_one, y_one)[:6]
        outs = [jax.ShapeDtypeStruct(v.shape, v.dtype) for v in made]
        outs[4] = jax.ShapeDtypeStruct((tok,), F32)
        vmem = pl.BlockSpec(memory_space=pltpu.VMEM)
        return pl.pallas_call(hand_over, out_shape=tuple(outs), in_specs=[vmem] * 6, out_specs=[vmem] * 6, name="hand_over")(*made)

    return jax.shard_map(device_step, mesh=mesh, in_specs=(w_spec, w_spec, w_spec, w_spec, row_spec, row_spec, row_spec, row_spec),
                         out_specs=(w_spec, w_spec, w_spec, w_spec, P("data"), row_spec), check_vma=False)
```

```python
import functools
import jax
import jax.numpy as jnp
from jax import lax
from jax.experimental import pallas as pl
from jax.experimental.pallas import tpu as pltpu
from jax.sharding import PartitionSpec as P

LEARN_RATE = 0.1
MOMENTUM = 0.9
F32, BF16 = jnp.float32, jnp.bfloat16
GRID = (8, 4, 4, 2)
ORDERS = (("z", "x", "y"), ("z", "y", "x"), ("x", "y", "z"), ("y", "x", "z"))
COLOURS = (0, 1, 2, 0, 1, 3, 0, 1, 2, 0, 1, 3)
GELU_SCALE = 0.7978845608028654
GELU_CUBE = 0.044715
G_SLOTS = 5
LANES = 128
SPILLED = 4
LATER = (2, 3)

ORDER = (
    ("a", 3, 0), ("a", 1, 0), ("a", 0, 0), ("a", 6, 0), ("a", 10, 0), ("a", 4, 0), ("a", 8, 0), ("a", 2, 0), ("m", 0, 0), ("a", 11, 0), ("a", 7, 0),
    ("a", 5, 0), ("a", 8, 1), ("a", 9, 0), ("a", 11, 1), ("a", 2, 1), ("a", 5, 1), ("a", 3, 1), ("a", 1, 1), ("a", 0, 1), ("a", 6, 1), ("a", 8, 2),
    ("a", 11, 2), ("a", 10, 1), ("a", 2, 2), ("a", 4, 1), ("a", 5, 2), ("a", 7, 1), ("a", 9, 1), ("a", 8, 3), ("a", 1, 2), ("a", 3, 2), ("a", 8, 4),
    ("a", 0, 2), ("a", 6, 2), ("a", 10, 2), ("a", 11, 3), ("a", 2, 3), ("a", 2, 4), ("a", 4, 2), ("a", 5, 3), ("a", 1, 3), ("a", 5, 4), ("a", 7, 2),
    ("a", 8, 5), ("a", 1, 4), ("a", 8, 6), ("a", 11, 4), ("a", 2, 5), ("a", 10, 3), ("a", 0, 3), ("a", 2, 6), ("a", 10, 4), ("a", 5, 5), ("a", 0, 4),
    ("a", 5, 6), ("a", 3, 3), ("a", 3, 4), ("a", 4, 3), ("a", 8, 7), ("a", 6, 3), ("a", 8, 8), ("a", 11, 5), ("a", 4, 4), ("a", 11, 6), ("a", 6, 4),
    ("a", 2, 7), ("a", 9, 2), ("a", 1, 5), ("a", 2, 8), ("a", 0, 5), ("a", 5, 7), ("a", 7, 3), ("a", 5, 8), ("a", 1, 6), ("a", 3, 5), ("a", 8, 9),
    ("a", 0, 6), ("f", 0, 0), ("a", 3, 6), ("a", 2, 9), ("a", 8, 10), ("a", 7, 4), ("a", 6, 5), ("m", 0, 1), ("a", 11, 7), ("a", 10, 5), ("a", 9, 3),
    ("a", 11, 8), ("a", 5, 9), ("a", 4, 5), ("a", 2, 10), ("f", 1, 0), ("a", 9, 4), ("a", 4, 6), ("a", 7, 5), ("a", 5, 10), ("f", 2, 0), ("a", 9, 5),
    ("a", 6, 6), ("a", 7, 6), ("f", 3, 0), ("a", 9, 6), ("a", 11, 9), ("a", 10, 6), ("f", 4, 0), ("a", 11, 10), ("d", 0, 0), ("f", 5, 0), ("l", 0, 0),
    ("g", 5, 0), ("g", 5, 1), ("g", 5, 2), ("g", 4, 0), ("g", 4, 1), ("r", 11, 0), ("g", 3, 1), ("g", 3, 2), ("r", 9, 0), ("r", 10, 0), ("r", 11, 1),
    ("g", 4, 2), ("r", 11, 2), ("g", 2, 1), ("g", 2, 0), ("r", 8, 0), ("r", 11, 3), ("r", 6, 0), ("r", 11, 4), ("r", 9, 1), ("g", 2, 2), ("r", 10, 1),
    ("r", 10, 2), ("r", 9, 2), ("g", 1, 0), ("r", 5, 0), ("g", 1, 1), ("r", 8, 1), ("r", 8, 2), ("r", 4, 0), ("r", 6, 1), ("g", 1, 2), ("r", 5, 1),
    ("r", 6, 2), ("r", 11, 5), ("r", 11, 6), ("g", 0, 0), ("r", 5, 2), ("r", 3, 0), ("r", 9, 3), ("g", 0, 1), ("r", 8, 3), ("r", 8, 4), ("r", 2, 0),
    ("r", 4, 1), ("h", 0, 0), ("g", 3, 0), ("r", 5, 3), ("r", 11, 7), ("r", 6, 3), ("r", 4, 2), ("r", 10, 3), ("g", 0, 2), ("r", 5, 4), ("r", 3, 1),
    ("r", 1, 0), ("r", 8, 5), ("r", 7, 0), ("r", 8, 6), ("r", 9, 4), ("r", 3, 2), ("r", 4, 3), ("r", 2, 1), ("r", 0, 0), ("r", 2, 2), ("r", 5, 5),
    ("r", 11, 8), ("r", 10, 4), ("r", 5, 6), ("r", 8, 7), ("r", 6, 4), ("r", 1, 1), ("r", 2, 3), ("r", 1, 2), ("r", 4, 4), ("r", 2, 4), ("r", 0, 1),
    ("r", 3, 3), ("r", 5, 7), ("u", 9, 0), ("r", 7, 1), ("r", 0, 2), ("r", 7, 2), ("r", 2, 5), ("u", 11, 0), ("r", 8, 8), ("u", 10, 0), ("r", 1, 3),
    ("r", 0, 3), ("r", 2, 6), ("u", 6, 0), ("r", 2, 7), ("u", 4, 0), ("b", 11, 0), ("r", 3, 4), ("r", 5, 8), ("b", 9, 0), ("r", 7, 3), ("u", 8, 0),
    ("r", 1, 4), ("b", 10, 0), ("r", 2, 8), ("r", 0, 4), ("b", 6, 0), ("b", 11, 1), ("u", 5, 0), ("b", 4, 0), ("b", 9, 1), ("r", 7, 4), ("u", 3, 0),
    ("u", 2, 0), ("b", 11, 2), ("b", 10, 1), ("u", 1, 0), ("b", 11, 3), ("u", 0, 0), ("b", 5, 0), ("b", 8, 0), ("b", 4, 1), ("b", 6, 1), ("b", 11, 4),
    ("b", 2, 0), ("u", 7, 0), ("n", 0, 0), ("b", 11, 5), ("b", 3, 0), ("b", 9, 2), ("b", 9, 3), ("b", 8, 1), ("b", 11, 6), ("b", 1, 0), ("b", 5, 1),
    ("b", 0, 0), ("b", 4, 2), ("b", 11, 7), ("b", 6, 2), ("b", 6, 3), ("b", 4, 3), ("b", 8, 2), ("b", 7, 0), ("b", 2, 1), ("b", 9, 4), ("b", 11, 8),
    ("b", 10, 2), ("b", 10, 3), ("b", 5, 2), ("b", 3, 1), ("b", 9, 5), ("b", 11, 9), ("b", 5, 3), ("b", 1, 1), ("b", 6, 4), ("b", 0, 1), ("b", 4, 4),
    ("b", 2, 2), ("b", 2, 3), ("b", 6, 5), ("b", 10, 4), ("b", 5, 4), ("b", 4, 5), ("b", 7, 1), ("b", 5, 5), ("b", 3, 2), ("b", 8, 3), ("b", 10, 5),
    ("b", 1, 2), ("b", 2, 4), ("b", 3, 3), ("b", 2, 5), ("b", 1, 3), ("b", 5, 6), ("b", 0, 2), ("b", 5, 7), ("b", 8, 4), ("b", 7, 2), ("b", 8, 5),
    ("b", 0, 3), ("b", 2, 6), ("b", 7, 3), ("b", 2, 7), ("b", 3, 4), ("b", 5, 8), ("b", 1, 4), ("b", 8, 6), ("b", 0, 4), ("b", 3, 5), ("b", 5, 9),
    ("b", 8, 7), ("b", 7, 4), ("b", 1, 5), ("b", 2, 8), ("b", 0, 5), ("s", 0, 0), ("b", 2, 9), ("b", 8, 8), ("b", 7, 5), ("s", 1, 0), ("s", 2, 0),
    ("s", 3, 0), ("b", 8, 9), ("s", 4, 0), ("s", 5, 0),
)


def start_copy(src, dst, send_sem, recv_sem, dev):
    pltpu.make_async_remote_copy(src_ref=src, dst_ref=dst, send_sem=send_sem, recv_sem=recv_sem,
                                 device_id=(dev,), device_id_type=pl.DeviceIdType.MESH).start()


def wait_bytes(ref, sem):
    pltpu.make_async_copy(ref, ref, sem).wait()


class Place:
    def __init__(self, grid):
        self.grid = grid
        nz, ny, nx, nc = grid
        me = lax.axis_index("data")
        self.me = me
        self.c = lax.rem(me, nc)
        self.x = lax.rem(me // nc, nx)
        self.y = lax.rem(me // (nc * nx), ny)
        self.z = me // (nc * nx * ny)
        self.size = {"z": nz, "y": ny, "x": nx}
        self.pos = {"z": self.z, "y": self.y, "x": self.x}
        self.stride = {"z": ny * nx * nc, "y": nx * nc, "x": nc}
        self.sib = me + 1 - 2 * self.c
        self.m = lax.rem(me, nc * nx)
        self.base = me - self.m

    def wrap(self, v, d):
        n = self.size[d]
        return lax.rem(v + 2 * n, n)

    def dev(self, d, v):
        return self.me + (v - self.pos[d]) * self.stride[d]

    def far(self, d):
        return self.size[d] // 2

    def near(self, d):
        return (self.size[d] - 1) // 2


def block_of(buf, lead, place, done, d, v, tail=()):
    idx = []
    for k in ("z", "y", "x"):
        if k in done:
            idx.append(slice(None))
        elif k == d:
            idx.append(v)
        else:
            idx.append(place.pos[k])
    return buf.at[(*lead, *idx, *tail)]


def half_of(buf, lead, place, d, v, h, tail=()):
    cut = "y" if d == "z" else "z"
    n = place.size[cut] // 2
    idx = [v if k == d else pl.ds(h * n, n) if k == cut else slice(None) for k in ("z", "y", "x")]
    return buf.at[(*lead, *idx, *tail)]


def ring_sem(place, d, way, step):
    return step - 1 if way == 1 else place.far(d) + step - 1


def ring_steps(place, d):
    out = []
    for step in range(1, place.far(d) + 1):
        out.append((1, step))
        if step <= place.near(d):
            out.append((-1, step))
    return out


class Sems:
    def __init__(self, place, colours, send, recv, per_unit):
        self.send, self.recv = send, recv
        self.kind = [int(ORDERS[c][2] == "z") for c in colours]
        self.base, n = [], 0
        for c in colours:
            self.base.append(n)
            n += self.count(place.grid, c)
        self.swaps = per_unit

    @staticmethod
    def count(grid, c):
        return 3 + grid["zyx".index(ORDERS[c][2])] - 1

    def r(self, u, k):
        return self.recv.at[self.base[u] + k]

    def s(self, u, stage):
        if stage == 3:
            return self.send.at[6 + (u if self.swaps else 0)]
        return self.send.at[2 * stage + self.kind[u]]


class Gather:
    def __init__(self, place, buf, u, order, sems):
        self.p, self.buf, self.u, self.order, self.sems = place, buf, u, order, sems

    def block(self, stage, v):
        return block_of(self.buf, (self.u,), self.p, self.order[:stage], self.order[stage], v, (self.p.c,))

    def many(self, stage):
        return self.block(stage, pl.ds(0, self.p.size[self.order[stage]] - 1))

    def direct_start(self, stage):
        p, d = self.p, self.order[stage]
        own = self.block(stage, p.pos[d])
        for k in range(1, p.size[d]):
            start_copy(own, own, self.sems.s(self.u, stage), self.sems.r(self.u, stage), p.dev(d, p.wrap(p.pos[d] + k, d)))

    def direct_wait(self, stage):
        if self.p.size[self.order[stage]] > 1:
            wait_bytes(self.many(stage), self.sems.r(self.u, stage))

    def ring_send(self, way, step):
        p, d = self.p, self.order[2]
        for h in range(2):
            s = way * (1 - 2 * h)
            ref = half_of(self.buf, (self.u,), p, d, p.wrap(p.pos[d] - (step - 1) * s, d), h, (p.c,))
            start_copy(ref, ref, self.sems.s(self.u, 2), self.sems.r(self.u, 3 + ring_sem(p, d, way, step)), p.dev(d, p.wrap(p.pos[d] + s, d)))

    def ring_start(self):
        d = self.order[2]
        for way, n in ((1, self.p.far(d)), (-1, self.p.near(d))):
            if n:
                self.ring_send(way, 1)
        self.swap_start(0)

    def ring_step(self, way, step):
        p, d = self.p, self.order[2]
        n = p.far(d) if way == 1 else p.near(d)
        wait_bytes(self.block(2, 0), self.sems.r(self.u, 3 + ring_sem(p, d, way, step)))
        if step < n:
            self.ring_send(way, step + 1)
        if way == -1:
            self.swap_start(step)
            self.swap_start(-step)
        elif step > p.near(d):
            self.swap_start(step)

    def swap_ref(self, c):
        return self.buf.at[self.u, :, :, :, c]

    def swap_start(self, k):
        d = self.order[2]
        ref = self.block(2, self.p.wrap(self.p.pos[d] - k, d))
        start_copy(ref, ref, self.sems.s(self.u, 3), self.sems.r(self.u, 2), self.p.sib)

    def swap_wait(self):
        wait_bytes(self.swap_ref(1 - self.p.c), self.sems.r(self.u, 2))

    def events(self):
        part = functools.partial
        out = [[part(self.direct_start, 0)],
               [part(self.direct_wait, 0), part(self.direct_start, 1)],
               [part(self.direct_wait, 1), self.ring_start]]
        out += [[part(self.ring_step, way, step)] for way, step in ring_steps(self.p, self.order[2])]
        return out + [[self.swap_wait]]


def drain_gather(place, buf, sems):
    nz, ny, nx, nc = place.grid
    heavy = sum(sems.kind)
    light = len(sems.kind) - heavy
    sent = (buf.at[0:light, 0:nz - 1, 0, 0, 0], buf.at[0:heavy, 0, 0, 0:nx - 1, 0],
            buf.at[0:light, :, 0:nx - 1, 0, 0], buf.at[0:heavy, 0, 0:nx - 1, :, 0],
            buf.at[0:light, :, 0:ny - 1, :, 0], buf.at[0:heavy, 0:nz - 1, :, :, 0], buf.at[:, :, :, :, 0])
    for k, ref in enumerate(sent):
        wait_bytes(ref, sems.send.at[k])


def add_into(dst, *srcs):
    total = dst[...].astype(F32)
    for s in srcs:
        total = total + s[...].astype(F32)
    dst[...] = total.astype(BF16)


class Reduce:
    def __init__(self, place, g, gslot, part, ring, rows, tiles, u, order, sems):
        self.p, self.g, self.gslot, self.part, self.u, self.order, self.sems = place, g, gslot, part, u, order, sems
        self.ring = ring
        n0 = place.size[order[0]]
        self.rows = lambda k: rows.at[k, pl.ds(0, n0)]
        self.tiles = lambda k: tiles.at[k]

    def block(self, stage, v):
        return block_of(self.part, (self.u,), self.p, self.order[:stage], self.order[stage], v)

    def swap_start(self):
        start_copy(self.g.at[self.gslot, :, :, :, 1 - self.p.c], self.part.at[self.u],
                   self.sems.s(self.u, 3), self.sems.r(self.u, 2), self.p.sib)

    def swap_wait(self):
        wait_bytes(self.part.at[self.u], self.sems.r(self.u, 2))
        p = self.p

        def add(k, _):
            add_into(self.part.at[self.u, k], self.g.at[self.gslot, k, :, :, p.c])
            return 0

        lax.fori_loop(0, p.size["z"], add, 0)
        wait_bytes(self.part.at[self.u], self.sems.s(self.u, 3))

    def count(self, way):
        d = self.order[2]
        return self.p.far(d) if way == 1 else self.p.near(d)

    def half(self, k, h):
        ref = self.ring(k)
        n = ref.shape[0] // 2
        return ref.at[pl.ds(h * n, n)]

    def own_half(self, way, ahead, h):
        p, d = self.p, self.order[2]
        return half_of(self.part, (self.u,), p, d, p.wrap(p.pos[d] + ahead * way * (1 - 2 * h), d), h)

    def ring_send(self, way, step):
        p, d = self.p, self.order[2]
        k = ring_sem(p, d, way, step)
        for h in range(2):
            src = self.own_half(way, self.count(way), h) if step == 1 else self.half(k - 1, h)
            start_copy(src, self.half(k, h), self.sems.s(self.u, 2), self.sems.r(self.u, 3 + k),
                       p.dev(d, p.wrap(p.pos[d] + way * (1 - 2 * h), d)))

    def ring_start(self):
        for way in (1, -1):
            if self.count(way):
                self.ring_send(way, 1)

    def ring_step(self, way, step):
        p, d = self.p, self.order[2]
        n = self.count(way)
        k = ring_sem(p, d, way, step)
        wait_bytes(self.ring(k), self.sems.r(self.u, 3 + k))
        if step < n:
            for h in range(2):
                add_into(self.half(k, h), self.own_half(way, n - step, h))
            self.ring_send(way, step + 1)
        if way == 1 and step == n:
            add_into(self.block(2, p.pos[d]), *[self.ring(ring_sem(p, d, w, self.count(w))) for w in (1, -1) if self.count(w)])

    def direct_start(self, stage):
        p, d = self.p, self.order[stage]
        land = self.rows if stage == 1 else self.tiles
        for k in range(1, p.size[d]):
            v = p.wrap(p.pos[d] + k, d)
            start_copy(self.block(stage, v), land(k - 1), self.sems.s(self.u, stage), self.sems.r(self.u, stage), p.dev(d, v))

    def direct_wait(self, stage):
        n = self.p.size[self.order[stage]]
        if n > 1:
            wait_bytes((self.rows if stage == 1 else self.tiles)(pl.ds(0, n - 1)), self.sems.r(self.u, stage))

    def row_sum(self):
        self.direct_wait(1)
        n = self.p.size[self.order[1]]
        if n > 1:
            add_into(self.block(1, self.p.pos[self.order[1]]), *[self.rows(k) for k in range(n - 1)])

    def tile_sum(self):
        self.direct_wait(0)
        total = self.block(0, self.p.pos[self.order[0]])[...].astype(F32)
        for k in range(self.p.size[self.order[0]] - 1):
            total = total + self.tiles(k)[...].astype(F32)
        return total.astype(BF16).astype(F32)

    def events(self):
        part = functools.partial
        out = [[self.swap_wait, self.ring_start]]
        out += [[part(self.ring_step, way, step)] for way, step in ring_steps(self.p, self.order[2])]
        out[-1].append(part(self.direct_start, 1))
        return out + [[self.row_sum, part(self.direct_start, 0)]]


def drain_reduce(place, ring_ab, ring_c, rows, tiles, sems):
    nz, ny, nx, nc = place.grid
    heavy = sum(sems.kind)
    light = len(sems.kind) - heavy
    sent = (tiles.at[0:light, 0:nz - 1], tiles.at[0:heavy, 0:nx - 1], rows.at[0:light, :, 0:nz], rows.at[0:heavy, :, 0:nx], ring_ab, ring_c)
    for k, ref in enumerate(sent):
        wait_bytes(ref, sems.send.at[k])


def enter(p):
    barrier = pltpu.get_barrier_semaphore()
    group = p.grid[2] * p.grid[3]
    peers = [p.base + lax.rem(p.m + k, group) for k in range(1, group)]
    for d in ("y", "z"):
        peers += [p.dev(d, p.wrap(p.pos[d] + k, d)) for k in range(1, p.size[d])]
    for peer in peers:
        pl.semaphore_signal(barrier, inc=1, device_id=(peer,), device_id_type=pl.DeviceIdType.MESH)
    pl.semaphore_wait(barrier, len(peers))


def lanes(ref, j):
    return ref.at[:, :, pl.ds(pl.multiple_of(j * LANES, LANES), LANES)]


class Shuffle:
    def __init__(self, place, one, two, sems, k0):
        self.p, self.one, self.two = place, one, two
        self.sem = lambda k: sems.at[k0 + k]
        self.group = place.grid[2] * place.grid[3]
        self.half = self.group // 2
        self.low = (place.m // self.half) * self.half
        self.mine = place.m - self.low

    def to_tiles_start(self, src1, src2):
        p = self.p
        for k in range(1, self.group):
            j = lax.rem(p.m + k, self.group)
            start_copy(lanes(src1, j), self.one.at[p.m], self.sem(0), self.sem(1), p.base + j)
        for k in range(1, self.half):
            j = lax.rem(self.mine + k, self.half)
            start_copy(lanes(src2, j), self.two.at[self.mine], self.sem(2), self.sem(3), p.base + self.low + j)

    def to_tiles_own(self, src1, src2):
        p = self.p
        pltpu.make_async_copy(lanes(src1, p.m), self.one.at[p.m], self.sem(1)).start()
        pltpu.make_async_copy(lanes(src2, self.mine), self.two.at[self.mine], self.sem(3)).start()

    def drain_sends(self):
        wait_bytes(self.one.at[pl.ds(0, self.group - 1)], self.sem(0))
        wait_bytes(self.two.at[pl.ds(0, self.half - 1)], self.sem(2))

    def to_tiles_finish(self, tiles):
        wait_bytes(self.one, self.sem(1))
        wait_bytes(self.two, self.sem(3))
        for l in range(self.one.shape[1]):
            for m in range(self.group):
                tiles[2 * l, 2 * m:2 * m + 2, :] = self.one[m, l]
            for m in range(self.half):
                tiles[2 * l + 1, 4 * m:4 * m + 4, :] = self.two[m, l]

    def put_rows(self, u, tile):
        if u % 2 == 0:
            for m in range(self.group):
                self.one[m, u // 2] = tile[2 * m:2 * m + 2, :]
        else:
            for m in range(self.half):
                self.two[m, u // 2] = tile[4 * m:4 * m + 4, :]

    def to_rows_start(self, dst1, dst2):
        p = self.p
        pltpu.make_async_copy(self.one.at[p.m], lanes(dst1, p.m), self.sem(1)).start()
        pltpu.make_async_copy(self.two.at[self.mine], lanes(dst2, self.mine), self.sem(3)).start()
        for k in range(1, self.group):
            j = lax.rem(p.m + k, self.group)
            start_copy(self.one.at[j], lanes(dst1, p.m), self.sem(0), self.sem(1), p.base + j)
        for k in range(1, self.half):
            j = lax.rem(self.mine + k, self.half)
            start_copy(self.two.at[j], lanes(dst2, self.mine), self.sem(2), self.sem(3), p.base + self.low + j)

    def to_rows_finish(self):
        wait_bytes(self.one, self.sem(1))
        wait_bytes(self.two, self.sem(3))
        self.drain_sends()


def w_one_of(wbuf, l):
    nz, ny, nx, nc = wbuf.shape[1:5]
    cols = [wbuf[2 * l, :, :, m // nc, m % nc].reshape(nz * ny * 16, LANES) for m in range(nx * nc)]
    return jnp.concatenate(cols, axis=1)


def w_two_of(wbuf, l):
    nz, ny, nx, nc = wbuf.shape[1:5]
    half = nx * nc // 2
    cols = []
    for b in range(half):
        pair = [wbuf[2 * l + 1, :, :, (r * half + b) // nc, b % nc].reshape(nz * ny, 1, 16, LANES) for r in range(2)]
        cols.append(jnp.concatenate(pair, axis=1).reshape(nz * ny * 32, LANES))
    return jnp.concatenate(cols, axis=1)


def contract(a, b, da, db):
    return lax.dot_general(a, b, (((da,), (db,)), ((), ())), preferred_element_type=F32)


def gelu_parts(u):
    w = GELU_SCALE + (GELU_SCALE * GELU_CUBE) * (u * u)
    gate = 0.5 + 0.5 * jnp.tanh(u * w)
    return u * gate, gate, w


def gelu(u):
    return gelu_parts(u)[0]


def gelu_and_slope(u):
    z, gate, w = gelu_parts(u)
    return z, gate + (z - z * gate) * (6.0 * w - 4.0 * GELU_SCALE)


def step_kernel(grid, batch_scale, w1, w2, m1, m2, x0, y0, x1, y1, nw1, nw2, nm1, nm2, loss, hlast, spill,
                wbuf, slope, act, hid, h, dlow, g, part, ring_ab, ring_c, rows, tiles3,
                wone, wtwo, mone, mtwo, wrow1, wrow2, wt, mt, lossbuf,
                gsend, grecv, rsend, rrecv, shuf, local):
    p = Place(grid)
    layers = w1.shape[0]
    units = 2 * layers
    nz, ny, nx, nc = grid
    tok, d_model = h.shape
    d_ff = hid.shape[2]

    def load(src, dst, k):
        return pltpu.make_async_copy(src, dst, local.at[k])

    loads = {"x0": load(x0, act.at[0], 0), "y0": load(y0, dlow.at[0], 1),
             "x1": load(x1, act.at[layers - 1], 2), "y1": load(y1, act.at[layers - 2], 3)}
    stage = [load(w1, wrow1, 2), load(w2, wrow2, 3)]
    wshuf = Shuffle(p, wone, wtwo, shuf, 0)
    mshuf = Shuffle(p, mone, mtwo, shuf, 4)
    for c in stage:
        c.start()
    wshuf.to_tiles_own(w1, w2)
    mshuf.to_tiles_own(m1, m2)
    loads["x0"].start()
    loads["y0"].start()
    enter(p)
    for c in stage:
        c.wait()
    wshuf.to_tiles_start(wrow1, wrow2)

    def own_tile(u):
        wbuf[u, p.z, p.y, p.x, p.c] = wt[u].astype(BF16)

    wshuf.to_tiles_finish(wt)
    for u in range(units):
        own_tile(u)
    loads["x0"].wait()
    h[...] = act[0].astype(F32)

    def spill_copy(l):
        return load(slope.at[lax.rem(l, 2)], spill.at[l], 4 + l)

    def unspill_copy(l):
        return load(spill.at[l], slope.at[l % 2], 4 + l)

    def forward_one(l):
        @pl.when(jnp.logical_and(l >= 2, l < SPILLED + 2))
        def _():
            spill_copy(l - 2).wait()

        a = h[...].astype(BF16)
        act[l] = a
        z, s = gelu_and_slope(jnp.dot(a, w_one_of(wbuf, l), preferred_element_type=F32))
        z = z.astype(BF16)
        slope[lax.rem(l, 2)] = s
        hid[l] = z
        h[...] += jnp.dot(z, w_two_of(wbuf, l), preferred_element_type=F32)

        @pl.when(l < SPILLED)
        def _():
            spill_copy(l).start()

    def loss_slope():
        loads["y0"].wait()
        d = (h[...] - dlow[0].astype(F32)) * batch_scale
        h[...] = d
        dlow[0] = d.astype(BF16)

    gsems = Sems(p, COLOURS, gsend, grecv, False)
    rsems = Sems(p, COLOURS, rsend, rrecv, True)
    slots = gradient_slots()
    first = [Gather(p, wbuf, u, ORDERS[COLOURS[u]], gsems) for u in range(units)]
    again = [Gather(p, wbuf, u, ORDERS[COLOURS[u]], gsems) for u in range(units)]
    red = []
    for u in range(units):
        n = sum(k == rsems.kind[u] for k in rsems.kind[:u])
        ring = functools.partial(lambda buf, n, k: buf.at[n, k], ring_c if rsems.kind[u] else ring_ab, n)
        red.append(Reduce(p, g, slots[u], part, ring, rows.at[u], tiles3.at[u], u, ORDERS[COLOURS[u]], rsems))

    def slope_of(l):
        return dlow.at[1 + LATER.index(l) if l in LATER else 0]

    def hidden_slope_of(l):
        return hid.at[l + len(LATER) if l in LATER else l]

    def grad_two(l):
        slot = red[2 * l + 1].gslot
        half = nx * nc // 2
        v = contract(hid[l], slope_of(l)[...], 0, 0).astype(BF16).reshape(nz, ny, 2, 16, d_model)
        for b in range(half):
            for r in range(2):
                g[slot, :, :, (r * half + b) // nc, b % nc] = v[:, :, r, :, LANES * b:LANES * b + LANES]
        if l in LATER:
            red[2 * l + 1].swap_start()

    def back_hidden(l):
        if l + 2 < layers:
            unspill_copy(l).wait()
        q = contract(slope_of(l)[...], w_two_of(wbuf, l), 1, 1)
        v = (slope[l % 2] * q).astype(BF16)
        hidden_slope_of(l)[...] = v
        if l:
            d = h[...] + contract(v, w_one_of(wbuf, l), 1, 1)
            h[...] = d
            slope_of(l - 1)[...] = d.astype(BF16)
        if l not in LATER:
            red[2 * l + 1].swap_start()
        if l >= 2:
            unspill_copy(l - 2).start()

    def grad_one(l):
        slot = red[2 * l].gslot
        v = contract(act[l], hidden_slope_of(l)[...], 0, 0).astype(BF16).reshape(nz, ny, 16, d_ff)
        for m in range(nx * nc):
            g[slot, :, :, m // nc, m % nc] = v[:, :, :, LANES * m:LANES * m + LANES]
        red[2 * l].swap_start()
        if l == layers - 1:
            loads["x1"].start()
        if l == layers - 2:
            loads["y1"].start()

    def update(u):
        total = red[u].tile_sum()
        mom = MOMENTUM * mt[u] + total
        w = wt[u] - LEARN_RATE * mom
        wbuf[u, p.z, p.y, p.x, p.c] = w.astype(BF16)
        wt[u] = w
        mt[u] = mom
        again[u].direct_start(0)

    def moments_start():
        mshuf.to_tiles_start(m1, m2)

    def moments_ready():
        mshuf.to_tiles_finish(mt)
        mshuf.drain_sends()
        wshuf.drain_sends()

    def second_start():
        loads["x1"].wait()
        h[...] = act[layers - 1].astype(F32)

    def forward_two(l):
        z = gelu(jnp.dot(h[...].astype(BF16), w_one_of(wbuf, l), preferred_element_type=F32)).astype(BF16)
        v = h[...] + jnp.dot(z, w_two_of(wbuf, l), preferred_element_type=F32)
        h[...] = v
        return v

    def forward_last():
        loads["y1"].wait()
        e = forward_two(layers - 1) - act[layers - 2].astype(F32)
        e = e * e
        s = e[:, :LANES]
        for k in range(1, d_model // LANES):
            s = s + e[:, LANES * k:LANES * k + LANES]
        lossbuf[...] = jnp.sum(s.T, axis=0, keepdims=True) * (1.0 / (2 * d_model))

    def new_rows():
        for u in range(units):
            wshuf.put_rows(u, wt[u])
            mshuf.put_rows(u, mt[u])
        wshuf.to_rows_start(nw1, nw2)
        mshuf.to_rows_start(nm1, nm2)

    work = {}
    for u in range(units):
        for k, ev in enumerate(first[u].events()):
            work["a", u, k] = ev
        for k, ev in enumerate(red[u].events()):
            work["r", u, k] = ev
        work["u", u, 0] = [functools.partial(update, u)]
        for k, ev in enumerate(again[u].events()[1:]):
            work["b", u, k] = ev
    for l in range(layers):
        work["g", l, 0] = [functools.partial(grad_two, l)]
        work["g", l, 1] = [functools.partial(back_hidden, l)]
        work["g", l, 2] = [functools.partial(grad_one, l)]
    work["s", layers - 1, 0] = [forward_last]
    work["d", 0, 0] = [functools.partial(drain_gather, p, wbuf, gsems)]
    work["l", 0, 0] = [loss_slope]
    work["m", 0, 0] = [moments_start]
    work["m", 0, 1] = [moments_ready]
    work["h", 0, 0] = [second_start]
    work["n", 0, 0] = [new_rows]

    def do(names):
        for name in names:
            for f in work.pop(name):
                f()

    def layer_loop(tag, n, body):
        first = ORDER.index((tag, 0, 0))
        do(ORDER[done[0]:first])
        ends = [ORDER.index((tag, l, 0)) for l in range(n)]

        def step(l, _):
            for k in range(1, n):
                names = ORDER[ends[k - 1] + 1:ends[k]]
                if names:
                    pl.when(l == k)(functools.partial(do, names))
            body(l)
            return 0

        lax.fori_loop(0, n, step, 0)
        done[0] = ends[-1] + 1

    done = [0]
    layer_loop("f", layers, forward_one)

    def forward_step(l):
        forward_two(l)

    layer_loop("s", layers - 1, forward_step)
    do(ORDER[done[0]:])
    assert not work
    out = [load(h, hlast, 0), load(lossbuf, loss, 1)]
    for c in out:
        c.start()
    drain_gather(p, wbuf, gsems)
    drain_reduce(p, ring_ab, ring_c, rows, tiles3, rsems)
    wshuf.to_rows_finish()
    mshuf.to_rows_finish()
    for c in out:
        c.wait()


def gradient_slots():
    free, held = list(range(G_SLOTS)), {}
    for tag, n, k in ORDER:
        if tag == "g" and k != 1:
            held[2 * n + (k == 0)] = free.pop(0)
        if tag == "r" and k == 0:
            free.append(held[n])
    return held


def make_step(grid, layers, tok, d_model, d_ff, n_dev):
    nz, ny, nx, nc = grid
    units = 2 * layers
    group = nx * nc
    hbm = pl.BlockSpec(memory_space=pl.ANY)
    sds = jax.ShapeDtypeStruct
    tile = (16, LANES)
    dma = pltpu.SemaphoreType.DMA
    heavy = sum(ORDERS[c][2] == "z" for c in COLOURS)
    recvs = sum(Sems.count(grid, c) for c in COLOURS)
    outs = (sds((layers, 2, d_ff), F32), sds((layers, 4, d_model), F32), sds((layers, 2, d_ff), F32), sds((layers, 4, d_model), F32),
            sds((1, tok), F32), sds((tok, d_model), F32), sds((SPILLED, tok, d_ff), F32))
    shuffled = [pltpu.VMEM((group, layers, 2, LANES), F32), pltpu.VMEM((group // 2, layers, 4, LANES), F32)]
    scratch = [
        pltpu.VMEM((units, *grid, *tile), BF16),
        pltpu.VMEM((2, tok, d_ff), F32),
        pltpu.VMEM((layers, tok, d_model), BF16),
        pltpu.VMEM((layers, tok, d_ff), BF16),
        pltpu.VMEM((tok, d_model), F32),
        pltpu.VMEM((len(LATER) + 1, tok, d_model), BF16),
        pltpu.VMEM((G_SLOTS, *grid, *tile), BF16),
        pltpu.VMEM((units, nz, ny, nx, *tile), BF16),
        pltpu.VMEM((units - heavy, nx - 1, nz, ny, *tile), BF16),
        pltpu.VMEM((heavy, nz - 1, ny, nx, *tile), BF16),
        pltpu.VMEM((units, max(ny, nx) - 1, max(nz, nx), *tile), BF16),
        pltpu.VMEM((units, max(nz, nx) - 1, *tile), BF16),
        *shuffled, *shuffled,
        pltpu.VMEM((layers, 2, d_ff), F32), pltpu.VMEM((layers, 4, d_model), F32),
        pltpu.VMEM((units, *tile), F32), pltpu.VMEM((units, *tile), F32),
        pltpu.VMEM((1, tok), F32),
        dma((7,)), dma((recvs,)), dma((6 + units,)), dma((recvs,)), dma((8,)), dma((4 + SPILLED,)),
    ]
    return pl.pallas_call(
        functools.partial(step_kernel, grid, 1.0 / (n_dev * tok * d_model)),
        out_shape=outs, in_specs=[hbm] * 8, out_specs=[hbm] * 7, scratch_shapes=scratch,
        compiler_params=pltpu.CompilerParams(collective_id=0, has_side_effects=True, vmem_limit_bytes=67043328),
        name="train_step")


def hand_over(*refs):
    n = len(refs) // 2
    for src, dst in zip(refs[:n], refs[n:]):
        if len(dst.shape) < len(src.shape):
            dst[...] = src[0, :]
        else:
            dst[...] = src[...]


def solution(mesh):
    n_dev = mesh.shape["data"]
    w_spec = P(None, "data", None)
    row_spec = P("data", None)

    def device_step(w_one, w_two, mom_one, mom_two, x_zero, y_zero, x_one, y_one):
        tok, d_model = x_zero.shape
        step = make_step(GRID, w_one.shape[0], tok, d_model, w_one.shape[2], n_dev)
        made = step(w_one, w_two, mom_one, mom_two, x_zero, y_zero, x_one, y_one)[:6]
        outs = [jax.ShapeDtypeStruct(v.shape, v.dtype) for v in made]
        outs[4] = jax.ShapeDtypeStruct((tok,), F32)
        vmem = pl.BlockSpec(memory_space=pltpu.VMEM)
        return pl.pallas_call(hand_over, out_shape=tuple(outs), in_specs=[vmem] * 6, out_specs=[vmem] * 6, name="hand_over")(*made)

    return jax.shard_map(device_step, mesh=mesh, in_specs=(w_spec, w_spec, w_spec, w_spec, row_spec, row_spec, row_spec, row_spec),
                         out_specs=(w_spec, w_spec, w_spec, w_spec, P("data"), row_spec), check_vma=False)
```

```python
import functools
import jax
import jax.numpy as jnp
from jax import lax
from jax.experimental import pallas as pl
from jax.experimental.pallas import tpu as pltpu
from jax.sharding import PartitionSpec as P

LEARN_RATE = 0.1
MOMENTUM = 0.9
F32, BF16 = jnp.float32, jnp.bfloat16
GRID = (8, 4, 4, 2)
ORDERS = (("z", "x", "y"), ("z", "y", "x"), ("x", "y", "z"), ("y", "x", "z"))
COLOURS = (0, 1, 0, 1, 2, 3, 0, 1, 2, 0, 1, 3)
GELU_SCALE = 0.7978845608028654
GELU_CUBE = 0.044715
G_SLOTS = 5
LANES = 128
SPILLED = 4
LATER = (2, 3)

ORDER = (
    ("a", 0, 0), ("a", 4, 0), ("a", 5, 0), ("a", 1, 0), ("a", 3, 0), ("m", 0, 0), ("a", 2, 0), ("a", 11, 0), ("a", 8, 0), ("a", 9, 0), ("a", 7, 0),
    ("a", 6, 0), ("a", 4, 1), ("a", 10, 0), ("a", 5, 1), ("a", 8, 1), ("a", 11, 1), ("a", 0, 1), ("a", 1, 1), ("a", 3, 1), ("a", 2, 1), ("a", 4, 2),
    ("a", 5, 2), ("a", 9, 1), ("a", 8, 2), ("a", 11, 2), ("a", 7, 1), ("a", 6, 1), ("a", 10, 1), ("a", 0, 2), ("a", 4, 3), ("a", 1, 2), ("a", 4, 4),
    ("a", 5, 3), ("a", 3, 2), ("a", 2, 2), ("a", 5, 4), ("a", 8, 3), ("a", 8, 4), ("a", 11, 3), ("a", 1, 3), ("a", 11, 4), ("a", 0, 3), ("a", 4, 5),
    ("a", 0, 4), ("a", 1, 4), ("a", 4, 6), ("a", 5, 5), ("a", 7, 2), ("a", 6, 2), ("a", 3, 3), ("a", 2, 3), ("a", 5, 6), ("a", 8, 5), ("a", 3, 4),
    ("a", 2, 4), ("a", 8, 6), ("a", 11, 5), ("a", 1, 5), ("a", 11, 6), ("a", 0, 5), ("a", 9, 2), ("a", 4, 7), ("a", 10, 2), ("a", 1, 6), ("a", 4, 8),
    ("a", 0, 6), ("f", 0, 0), ("a", 5, 7), ("a", 5, 8), ("m", 0, 1), ("a", 3, 5), ("a", 7, 3), ("a", 2, 5), ("a", 6, 3), ("a", 8, 7), ("a", 8, 8),
    ("a", 7, 4), ("a", 11, 7), ("a", 6, 4), ("a", 9, 3), ("a", 10, 3), ("a", 3, 6), ("a", 11, 8), ("a", 2, 6), ("f", 1, 0), ("a", 5, 9), ("a", 4, 9),
    ("a", 8, 9), ("a", 10, 4), ("a", 6, 5), ("a", 11, 9), ("a", 7, 5), ("a", 5, 10), ("a", 9, 4), ("a", 4, 10), ("f", 2, 0), ("a", 6, 6), ("a", 7, 6),
    ("a", 9, 5), ("a", 11, 10), ("f", 3, 0), ("a", 9, 6), ("a", 10, 5), ("a", 8, 10), ("f", 4, 0), ("a", 10, 6), ("f", 5, 0), ("d", 0, 0),
    ("l", 0, 0), ("g", 5, 0), ("g", 5, 1), ("g", 4, 0), ("g", 5, 2), ("g", 4, 1), ("g", 3, 1), ("g", 3, 2), ("g", 3, 0), ("r", 9, 0), ("r", 11, 0),
    ("r", 10, 0), ("g", 4, 2), ("g", 2, 1), ("r", 7, 0), ("r", 11, 1), ("r", 6, 0), ("g", 2, 2), ("r", 11, 2), ("r", 9, 1), ("r", 10, 1), ("g", 2, 0),
    ("r", 9, 2), ("r", 10, 2), ("r", 8, 0), ("g", 1, 0), ("r", 4, 0), ("r", 11, 3), ("g", 1, 1), ("r", 7, 1), ("r", 7, 2), ("r", 6, 1), ("r", 6, 2),
    ("r", 11, 4), ("r", 5, 0), ("g", 0, 0), ("r", 4, 1), ("r", 9, 3), ("r", 10, 3), ("g", 0, 1), ("r", 3, 0), ("h", 0, 0), ("r", 4, 2), ("g", 0, 2),
    ("r", 7, 3), ("r", 11, 5), ("r", 11, 6), ("r", 5, 1), ("r", 8, 1), ("g", 1, 2), ("r", 5, 2), ("r", 6, 3), ("r", 4, 3), ("r", 9, 4), ("r", 0, 0),
    ("r", 4, 4), ("r", 10, 4), ("r", 1, 0), ("r", 3, 1), ("r", 5, 3), ("r", 2, 0), ("r", 3, 2), ("r", 11, 7), ("r", 7, 4), ("r", 5, 4), ("r", 4, 5),
    ("r", 0, 1), ("r", 1, 1), ("r", 6, 4), ("r", 4, 6), ("r", 0, 2), ("r", 8, 2), ("r", 1, 2), ("r", 5, 5), ("r", 2, 1), ("r", 8, 3), ("u", 9, 0),
    ("r", 3, 3), ("r", 5, 6), ("r", 2, 2), ("u", 10, 0), ("r", 4, 7), ("r", 11, 8), ("r", 0, 3), ("r", 1, 3), ("u", 7, 0), ("r", 8, 4), ("r", 5, 7),
    ("r", 2, 3), ("r", 8, 5), ("u", 6, 0), ("r", 3, 4), ("r", 4, 8), ("u", 11, 0), ("r", 8, 6), ("r", 0, 4), ("b", 9, 0), ("r", 8, 7), ("r", 5, 8),
    ("r", 1, 4), ("b", 10, 0), ("r", 2, 4), ("b", 7, 0), ("u", 4, 0), ("b", 11, 0), ("b", 6, 0), ("u", 3, 0), ("r", 8, 8), ("u", 5, 0), ("b", 9, 1),
    ("u", 0, 0), ("b", 10, 1), ("u", 1, 0), ("b", 11, 1), ("u", 2, 0), ("b", 4, 0), ("b", 5, 0), ("b", 6, 1), ("u", 8, 0), ("n", 0, 0), ("b", 7, 1),
    ("b", 3, 0), ("b", 11, 2), ("b", 11, 3), ("b", 0, 0), ("b", 9, 2), ("b", 9, 3), ("b", 4, 1), ("b", 5, 1), ("b", 1, 0), ("b", 8, 0), ("b", 10, 2),
    ("b", 10, 3), ("b", 2, 0), ("b", 11, 4), ("b", 6, 2), ("b", 6, 3), ("b", 4, 2), ("b", 4, 3), ("b", 3, 1), ("b", 5, 2), ("b", 9, 4), ("b", 0, 1),
    ("b", 5, 3), ("b", 10, 4), ("b", 9, 5), ("b", 11, 5), ("b", 11, 6), ("b", 1, 1), ("b", 10, 5), ("b", 4, 4), ("b", 8, 1), ("b", 2, 1), ("b", 6, 4),
    ("b", 5, 4), ("b", 3, 2), ("b", 5, 5), ("b", 11, 7), ("b", 6, 5), ("b", 3, 3), ("b", 0, 2), ("b", 11, 8), ("b", 0, 3), ("b", 1, 2), ("b", 4, 5),
    ("b", 8, 2), ("b", 11, 9), ("b", 8, 3), ("b", 2, 2), ("b", 1, 3), ("b", 7, 2), ("b", 5, 6), ("b", 7, 3), ("b", 5, 7), ("b", 2, 3), ("b", 3, 4),
    ("b", 4, 6), ("b", 4, 7), ("b", 0, 4), ("b", 1, 4), ("b", 8, 4), ("b", 3, 5), ("b", 8, 5), ("b", 2, 4), ("b", 0, 5), ("b", 7, 4), ("b", 1, 5),
    ("s", 0, 0), ("b", 2, 5), ("b", 4, 8), ("b", 7, 5), ("b", 8, 6), ("b", 5, 8), ("s", 1, 0), ("b", 4, 9), ("b", 8, 7), ("b", 5, 9), ("s", 2, 0),
    ("b", 8, 8), ("s", 3, 0), ("b", 8, 9), ("s", 4, 0), ("s", 5, 0),
)


def start_copy(src, dst, send_sem, recv_sem, dev):
    pltpu.make_async_remote_copy(src_ref=src, dst_ref=dst, send_sem=send_sem, recv_sem=recv_sem,
                                 device_id=(dev,), device_id_type=pl.DeviceIdType.MESH).start()


def wait_bytes(ref, sem):
    pltpu.make_async_copy(ref, ref, sem).wait()


class Place:
    def __init__(self, grid):
        self.grid = grid
        nz, ny, nx, nc = grid
        me = lax.axis_index("data")
        self.me = me
        self.c = lax.rem(me, nc)
        self.x = lax.rem(me // nc, nx)
        self.y = lax.rem(me // (nc * nx), ny)
        self.z = me // (nc * nx * ny)
        self.size = {"z": nz, "y": ny, "x": nx}
        self.pos = {"z": self.z, "y": self.y, "x": self.x}
        self.stride = {"z": ny * nx * nc, "y": nx * nc, "x": nc}
        self.sib = me + 1 - 2 * self.c
        self.m = lax.rem(me, nc * nx)
        self.base = me - self.m

    def wrap(self, v, d):
        n = self.size[d]
        return lax.rem(v + 2 * n, n)

    def dev(self, d, v):
        return self.me + (v - self.pos[d]) * self.stride[d]

    def far(self, d):
        return self.size[d] // 2

    def near(self, d):
        return (self.size[d] - 1) // 2


def block_of(buf, lead, place, done, d, v, tail=()):
    idx = []
    for k in ("z", "y", "x"):
        if k in done:
            idx.append(slice(None))
        elif k == d:
            idx.append(v)
        else:
            idx.append(place.pos[k])
    return buf.at[(*lead, *idx, *tail)]


def half_of(buf, lead, place, d, v, h, tail=()):
    cut = "y" if d == "z" else "z"
    n = place.size[cut] // 2
    idx = [v if k == d else pl.ds(h * n, n) if k == cut else slice(None) for k in ("z", "y", "x")]
    return buf.at[(*lead, *idx, *tail)]


def ring_sem(place, d, way, step):
    return step - 1 if way == 1 else place.far(d) + step - 1


def ring_steps(place, d):
    out = []
    for step in range(1, place.far(d) + 1):
        out.append((1, step))
        if step <= place.near(d):
            out.append((-1, step))
    return out


class Sems:
    def __init__(self, place, colours, send, recv, per_unit):
        self.send, self.recv = send, recv
        self.kind = [int(ORDERS[c][2] == "z") for c in colours]
        self.base, n = [], 0
        for c in colours:
            self.base.append(n)
            n += self.count(place.grid, c)
        self.swaps = per_unit

    @staticmethod
    def count(grid, c):
        return 3 + grid["zyx".index(ORDERS[c][2])] - 1

    def r(self, u, k):
        return self.recv.at[self.base[u] + k]

    def s(self, u, stage):
        if stage == 3:
            return self.send.at[6 + (u if self.swaps else 0)]
        return self.send.at[2 * stage + self.kind[u]]


class Gather:
    def __init__(self, place, buf, u, order, sems):
        self.p, self.buf, self.u, self.order, self.sems = place, buf, u, order, sems

    def block(self, stage, v):
        return block_of(self.buf, (self.u,), self.p, self.order[:stage], self.order[stage], v, (self.p.c,))

    def many(self, stage):
        return self.block(stage, pl.ds(0, self.p.size[self.order[stage]] - 1))

    def direct_start(self, stage):
        p, d = self.p, self.order[stage]
        own = self.block(stage, p.pos[d])
        for k in range(1, p.size[d]):
            start_copy(own, own, self.sems.s(self.u, stage), self.sems.r(self.u, stage), p.dev(d, p.wrap(p.pos[d] + k, d)))

    def direct_wait(self, stage):
        if self.p.size[self.order[stage]] > 1:
            wait_bytes(self.many(stage), self.sems.r(self.u, stage))

    def ring_send(self, way, step):
        p, d = self.p, self.order[2]
        for h in range(2):
            s = way * (1 - 2 * h)
            ref = half_of(self.buf, (self.u,), p, d, p.wrap(p.pos[d] - (step - 1) * s, d), h, (p.c,))
            start_copy(ref, ref, self.sems.s(self.u, 2), self.sems.r(self.u, 3 + ring_sem(p, d, way, step)), p.dev(d, p.wrap(p.pos[d] + s, d)))

    def ring_start(self):
        d = self.order[2]
        for way, n in ((1, self.p.far(d)), (-1, self.p.near(d))):
            if n:
                self.ring_send(way, 1)
        self.swap_start(0)

    def ring_step(self, way, step):
        p, d = self.p, self.order[2]
        n = p.far(d) if way == 1 else p.near(d)
        wait_bytes(self.block(2, 0), self.sems.r(self.u, 3 + ring_sem(p, d, way, step)))
        if step < n:
            self.ring_send(way, step + 1)
        if way == -1:
            self.swap_start(step)
            self.swap_start(-step)
        elif step > p.near(d):
            self.swap_start(step)

    def swap_ref(self, c):
        return self.buf.at[self.u, :, :, :, c]

    def swap_start(self, k):
        d = self.order[2]
        ref = self.block(2, self.p.wrap(self.p.pos[d] - k, d))
        start_copy(ref, ref, self.sems.s(self.u, 3), self.sems.r(self.u, 2), self.p.sib)

    def swap_wait(self):
        wait_bytes(self.swap_ref(1 - self.p.c), self.sems.r(self.u, 2))

    def events(self):
        part = functools.partial
        out = [[part(self.direct_start, 0)],
               [part(self.direct_wait, 0), part(self.direct_start, 1)],
               [part(self.direct_wait, 1), self.ring_start]]
        out += [[part(self.ring_step, way, step)] for way, step in ring_steps(self.p, self.order[2])]
        return out + [[self.swap_wait]]


def drain_gather(place, buf, sems):
    nz, ny, nx, nc = place.grid
    heavy = sum(sems.kind)
    light = len(sems.kind) - heavy
    sent = (buf.at[0:light, 0:nz - 1, 0, 0, 0], buf.at[0:heavy, 0, 0, 0:nx - 1, 0],
            buf.at[0:light, :, 0:nx - 1, 0, 0], buf.at[0:heavy, 0, 0:nx - 1, :, 0],
            buf.at[0:light, :, 0:ny - 1, :, 0], buf.at[0:heavy, 0:nz - 1, :, :, 0], buf.at[:, :, :, :, 0])
    for k, ref in enumerate(sent):
        wait_bytes(ref, sems.send.at[k])


def add_into(dst, *srcs):
    total = dst[...].astype(F32)
    for s in srcs:
        total = total + s[...].astype(F32)
    dst[...] = total.astype(BF16)


class Reduce:
    def __init__(self, place, g, gslot, part, ring, rows, tiles, u, order, sems):
        self.p, self.g, self.gslot, self.part, self.u, self.order, self.sems = place, g, gslot, part, u, order, sems
        self.ring = ring
        n0 = place.size[order[0]]
        self.rows = lambda k: rows.at[k, pl.ds(0, n0)]
        self.tiles = lambda k: tiles.at[k]

    def block(self, stage, v):
        return block_of(self.part, (self.u,), self.p, self.order[:stage], self.order[stage], v)

    def swap_start(self):
        start_copy(self.g.at[self.gslot, :, :, :, 1 - self.p.c], self.part.at[self.u],
                   self.sems.s(self.u, 3), self.sems.r(self.u, 2), self.p.sib)

    def swap_wait(self):
        wait_bytes(self.part.at[self.u], self.sems.r(self.u, 2))
        p = self.p

        def add(k, _):
            add_into(self.part.at[self.u, k], self.g.at[self.gslot, k, :, :, p.c])
            return 0

        lax.fori_loop(0, p.size["z"], add, 0)
        wait_bytes(self.part.at[self.u], self.sems.s(self.u, 3))

    def count(self, way):
        d = self.order[2]
        return self.p.far(d) if way == 1 else self.p.near(d)

    def half(self, k, h):
        ref = self.ring(k)
        n = ref.shape[0] // 2
        return ref.at[pl.ds(h * n, n)]

    def own_half(self, way, ahead, h):
        p, d = self.p, self.order[2]
        return half_of(self.part, (self.u,), p, d, p.wrap(p.pos[d] + ahead * way * (1 - 2 * h), d), h)

    def ring_send(self, way, step):
        p, d = self.p, self.order[2]
        k = ring_sem(p, d, way, step)
        for h in range(2):
            src = self.own_half(way, self.count(way), h) if step == 1 else self.half(k - 1, h)
            start_copy(src, self.half(k, h), self.sems.s(self.u, 2), self.sems.r(self.u, 3 + k),
                       p.dev(d, p.wrap(p.pos[d] + way * (1 - 2 * h), d)))

    def ring_start(self):
        for way in (1, -1):
            if self.count(way):
                self.ring_send(way, 1)

    def ring_step(self, way, step):
        p, d = self.p, self.order[2]
        n = self.count(way)
        k = ring_sem(p, d, way, step)
        wait_bytes(self.ring(k), self.sems.r(self.u, 3 + k))
        if step < n:
            for h in range(2):
                add_into(self.half(k, h), self.own_half(way, n - step, h))
            self.ring_send(way, step + 1)
        if way == 1 and step == n:
            add_into(self.block(2, p.pos[d]), *[self.ring(ring_sem(p, d, w, self.count(w))) for w in (1, -1) if self.count(w)])

    def direct_start(self, stage):
        p, d = self.p, self.order[stage]
        land = self.rows if stage == 1 else self.tiles
        for k in range(1, p.size[d]):
            v = p.wrap(p.pos[d] + k, d)
            start_copy(self.block(stage, v), land(k - 1), self.sems.s(self.u, stage), self.sems.r(self.u, stage), p.dev(d, v))

    def direct_wait(self, stage):
        n = self.p.size[self.order[stage]]
        if n > 1:
            wait_bytes((self.rows if stage == 1 else self.tiles)(pl.ds(0, n - 1)), self.sems.r(self.u, stage))

    def row_sum(self):
        self.direct_wait(1)
        n = self.p.size[self.order[1]]
        if n > 1:
            add_into(self.block(1, self.p.pos[self.order[1]]), *[self.rows(k) for k in range(n - 1)])

    def tile_sum(self):
        self.direct_wait(0)
        total = self.block(0, self.p.pos[self.order[0]])[...].astype(F32)
        for k in range(self.p.size[self.order[0]] - 1):
            total = total + self.tiles(k)[...].astype(F32)
        return total.astype(BF16).astype(F32)

    def events(self):
        part = functools.partial
        out = [[self.swap_wait, self.ring_start]]
        out += [[part(self.ring_step, way, step)] for way, step in ring_steps(self.p, self.order[2])]
        out[-1].append(part(self.direct_start, 1))
        return out + [[self.row_sum, part(self.direct_start, 0)]]


def drain_reduce(place, ring_ab, ring_c, rows, tiles, sems):
    nz, ny, nx, nc = place.grid
    heavy = sum(sems.kind)
    light = len(sems.kind) - heavy
    sent = (tiles.at[0:light, 0:nz - 1], tiles.at[0:heavy, 0:nx - 1], rows.at[0:light, :, 0:nz], rows.at[0:heavy, :, 0:nx], ring_ab, ring_c)
    for k, ref in enumerate(sent):
        wait_bytes(ref, sems.send.at[k])


def enter(p):
    barrier = pltpu.get_barrier_semaphore()
    group = p.grid[2] * p.grid[3]
    peers = [p.base + lax.rem(p.m + k, group) for k in range(1, group)]
    for d in ("y", "z"):
        peers += [p.dev(d, p.wrap(p.pos[d] + k, d)) for k in range(1, p.size[d])]
    for peer in peers:
        pl.semaphore_signal(barrier, inc=1, device_id=(peer,), device_id_type=pl.DeviceIdType.MESH)
    pl.semaphore_wait(barrier, len(peers))


def lanes(ref, j):
    return ref.at[:, :, pl.ds(pl.multiple_of(j * LANES, LANES), LANES)]


class Shuffle:
    def __init__(self, place, one, two, sems, k0):
        self.p, self.one, self.two = place, one, two
        self.sem = lambda k: sems.at[k0 + k]
        self.group = place.grid[2] * place.grid[3]
        self.half = self.group // 2
        self.low = (place.m // self.half) * self.half
        self.mine = place.m - self.low

    def to_tiles_start(self, src1, src2):
        p = self.p
        for k in range(1, self.group):
            j = lax.rem(p.m + k, self.group)
            start_copy(lanes(src1, j), self.one.at[p.m], self.sem(0), self.sem(1), p.base + j)
        for k in range(1, self.half):
            j = lax.rem(self.mine + k, self.half)
            start_copy(lanes(src2, j), self.two.at[self.mine], self.sem(2), self.sem(3), p.base + self.low + j)

    def to_tiles_own(self, src1, src2):
        p = self.p
        pltpu.make_async_copy(lanes(src1, p.m), self.one.at[p.m], self.sem(1)).start()
        pltpu.make_async_copy(lanes(src2, self.mine), self.two.at[self.mine], self.sem(3)).start()

    def drain_sends(self):
        wait_bytes(self.one.at[pl.ds(0, self.group - 1)], self.sem(0))
        wait_bytes(self.two.at[pl.ds(0, self.half - 1)], self.sem(2))

    def to_tiles_finish(self, tiles):
        wait_bytes(self.one, self.sem(1))
        wait_bytes(self.two, self.sem(3))
        for l in range(self.one.shape[1]):
            for m in range(self.group):
                tiles[2 * l, 2 * m:2 * m + 2, :] = self.one[m, l]
            for m in range(self.half):
                tiles[2 * l + 1, 4 * m:4 * m + 4, :] = self.two[m, l]

    def put_rows(self, u, tile):
        if u % 2 == 0:
            for m in range(self.group):
                self.one[m, u // 2] = tile[2 * m:2 * m + 2, :]
        else:
            for m in range(self.half):
                self.two[m, u // 2] = tile[4 * m:4 * m + 4, :]

    def to_rows_start(self, dst1, dst2):
        p = self.p
        pltpu.make_async_copy(self.one.at[p.m], lanes(dst1, p.m), self.sem(1)).start()
        pltpu.make_async_copy(self.two.at[self.mine], lanes(dst2, self.mine), self.sem(3)).start()
        for k in range(1, self.group):
            j = lax.rem(p.m + k, self.group)
            start_copy(self.one.at[j], lanes(dst1, p.m), self.sem(0), self.sem(1), p.base + j)
        for k in range(1, self.half):
            j = lax.rem(self.mine + k, self.half)
            start_copy(self.two.at[j], lanes(dst2, self.mine), self.sem(2), self.sem(3), p.base + self.low + j)

    def to_rows_finish(self):
        wait_bytes(self.one, self.sem(1))
        wait_bytes(self.two, self.sem(3))
        self.drain_sends()


def w_one_of(wbuf, l):
    nz, ny, nx, nc = wbuf.shape[1:5]
    cols = [wbuf[2 * l, :, :, m // nc, m % nc].reshape(nz * ny * 16, LANES) for m in range(nx * nc)]
    return jnp.concatenate(cols, axis=1)


def w_two_of(wbuf, l):
    nz, ny, nx, nc = wbuf.shape[1:5]
    half = nx * nc // 2
    cols = []
    for b in range(half):
        pair = [wbuf[2 * l + 1, :, :, (r * half + b) // nc, b % nc].reshape(nz * ny, 1, 16, LANES) for r in range(2)]
        cols.append(jnp.concatenate(pair, axis=1).reshape(nz * ny * 32, LANES))
    return jnp.concatenate(cols, axis=1)


def contract(a, b, da, db):
    return lax.dot_general(a, b, (((da,), (db,)), ((), ())), preferred_element_type=F32)


def gelu_parts(u):
    w = GELU_SCALE + (GELU_SCALE * GELU_CUBE) * (u * u)
    gate = 0.5 + 0.5 * jnp.tanh(u * w)
    return u * gate, gate, w


def gelu(u):
    return gelu_parts(u)[0]


def gelu_slope(u):
    z, gate, w = gelu_parts(u)
    return gate + (z - z * gate) * (6.0 * w - 4.0 * GELU_SCALE)


def step_kernel(grid, batch_scale, w1, w2, m1, m2, x0, y0, x1, y1, nw1, nw2, nm1, nm2, loss, hlast, spill,
                wbuf, before, act, hid, h, dlow, g, part, ring_ab, ring_c, rows, tiles3,
                wone, wtwo, mone, mtwo, wrow1, wrow2, wt, mt, lossbuf,
                gsend, grecv, rsend, rrecv, shuf, local):
    p = Place(grid)
    layers = w1.shape[0]
    units = 2 * layers
    nz, ny, nx, nc = grid
    tok, d_model = h.shape
    d_ff = hid.shape[2]

    def load(src, dst, k):
        return pltpu.make_async_copy(src, dst, local.at[k])

    loads = {"x0": load(x0, act.at[0], 0), "y0": load(y0, dlow.at[0], 1),
             "x1": load(x1, act.at[layers - 1], 2), "y1": load(y1, act.at[layers - 2], 3)}
    stage = [load(w1, wrow1, 2), load(w2, wrow2, 3)]
    wshuf = Shuffle(p, wone, wtwo, shuf, 0)
    mshuf = Shuffle(p, mone, mtwo, shuf, 4)
    for c in stage:
        c.start()
    wshuf.to_tiles_own(w1, w2)
    mshuf.to_tiles_own(m1, m2)
    loads["x0"].start()
    loads["y0"].start()
    enter(p)
    for c in stage:
        c.wait()
    wshuf.to_tiles_start(wrow1, wrow2)

    def own_tile(u):
        wbuf[u, p.z, p.y, p.x, p.c] = wt[u].astype(BF16)

    wshuf.to_tiles_finish(wt)
    for u in range(units):
        own_tile(u)
    loads["x0"].wait()
    h[...] = act[0].astype(F32)

    def spill_copy(l):
        return load(before.at[lax.rem(l, 2)], spill.at[l], 4 + l)

    def unspill_copy(l):
        return load(spill.at[l], before.at[l % 2], 4 + l)

    def forward_one(l):
        @pl.when(jnp.logical_and(l >= 2, l < SPILLED + 2))
        def _():
            spill_copy(l - 2).wait()

        a = h[...].astype(BF16)
        act[l] = a
        u = jnp.dot(a, w_one_of(wbuf, l), preferred_element_type=F32)
        before[lax.rem(l, 2)] = u
        z = gelu(u).astype(BF16)
        hid[l] = z
        h[...] += jnp.dot(z, w_two_of(wbuf, l), preferred_element_type=F32)

        @pl.when(l < SPILLED)
        def _():
            spill_copy(l).start()

    def loss_slope():
        loads["y0"].wait()
        d = (h[...] - dlow[0].astype(F32)) * batch_scale
        h[...] = d
        dlow[0] = d.astype(BF16)

    gsems = Sems(p, COLOURS, gsend, grecv, False)
    rsems = Sems(p, COLOURS, rsend, rrecv, True)
    slots = gradient_slots()
    first = [Gather(p, wbuf, u, ORDERS[COLOURS[u]], gsems) for u in range(units)]
    again = [Gather(p, wbuf, u, ORDERS[COLOURS[u]], gsems) for u in range(units)]
    red = []
    for u in range(units):
        n = sum(k == rsems.kind[u] for k in rsems.kind[:u])
        ring = functools.partial(lambda buf, n, k: buf.at[n, k], ring_c if rsems.kind[u] else ring_ab, n)
        red.append(Reduce(p, g, slots[u], part, ring, rows.at[u], tiles3.at[u], u, ORDERS[COLOURS[u]], rsems))

    def slope_of(l):
        return dlow.at[1 + LATER.index(l) if l in LATER else 0]

    def hidden_slope_of(l):
        return hid.at[l + len(LATER) if l in LATER else l]

    def grad_two(l):
        slot = red[2 * l + 1].gslot
        half = nx * nc // 2
        v = contract(hid[l], slope_of(l)[...], 0, 0).astype(BF16).reshape(nz, ny, 2, 16, d_model)
        for b in range(half):
            for r in range(2):
                g[slot, :, :, (r * half + b) // nc, b % nc] = v[:, :, r, :, LANES * b:LANES * b + LANES]
        if l in LATER:
            red[2 * l + 1].swap_start()

    def back_hidden(l):
        if l + 2 < layers:
            unspill_copy(l).wait()
        q = contract(slope_of(l)[...], w_two_of(wbuf, l), 1, 1)
        v = (gelu_slope(before[l % 2]) * q).astype(BF16)
        hidden_slope_of(l)[...] = v
        if l:
            d = h[...] + contract(v, w_one_of(wbuf, l), 1, 1)
            h[...] = d
            slope_of(l - 1)[...] = d.astype(BF16)
        if l not in LATER:
            red[2 * l + 1].swap_start()
        if l >= 2:
            unspill_copy(l - 2).start()

    def grad_one(l):
        slot = red[2 * l].gslot
        v = contract(act[l], hidden_slope_of(l)[...], 0, 0).astype(BF16).reshape(nz, ny, 16, d_ff)
        for m in range(nx * nc):
            g[slot, :, :, m // nc, m % nc] = v[:, :, :, LANES * m:LANES * m + LANES]
        red[2 * l].swap_start()
        if l == layers - 1:
            loads["x1"].start()
        if l == layers - 2:
            loads["y1"].start()

    def update(u):
        total = red[u].tile_sum()
        mom = MOMENTUM * mt[u] + total
        w = wt[u] - LEARN_RATE * mom
        wbuf[u, p.z, p.y, p.x, p.c] = w.astype(BF16)
        wt[u] = w
        mt[u] = mom
        again[u].direct_start(0)

    def moments_start():
        mshuf.to_tiles_start(m1, m2)

    def moments_ready():
        mshuf.to_tiles_finish(mt)
        mshuf.drain_sends()
        wshuf.drain_sends()

    def second_start():
        loads["x1"].wait()
        h[...] = act[layers - 1].astype(F32)

    def forward_two(l):
        z = gelu(jnp.dot(h[...].astype(BF16), w_one_of(wbuf, l), preferred_element_type=F32)).astype(BF16)
        v = h[...] + jnp.dot(z, w_two_of(wbuf, l), preferred_element_type=F32)
        h[...] = v
        return v

    def forward_last():
        loads["y1"].wait()
        e = forward_two(layers - 1) - act[layers - 2].astype(F32)
        e = e * e
        s = e[:, :LANES]
        for k in range(1, d_model // LANES):
            s = s + e[:, LANES * k:LANES * k + LANES]
        lossbuf[...] = jnp.sum(s.T, axis=0, keepdims=True) * (1.0 / (2 * d_model))

    def new_rows():
        for u in range(units):
            wshuf.put_rows(u, wt[u])
            mshuf.put_rows(u, mt[u])
        wshuf.to_rows_start(nw1, nw2)
        mshuf.to_rows_start(nm1, nm2)

    work = {}
    for u in range(units):
        for k, ev in enumerate(first[u].events()):
            work["a", u, k] = ev
        for k, ev in enumerate(red[u].events()):
            work["r", u, k] = ev
        work["u", u, 0] = [functools.partial(update, u)]
        for k, ev in enumerate(again[u].events()[1:]):
            work["b", u, k] = ev
    for l in range(layers):
        work["g", l, 0] = [functools.partial(grad_two, l)]
        work["g", l, 1] = [functools.partial(back_hidden, l)]
        work["g", l, 2] = [functools.partial(grad_one, l)]
    work["s", layers - 1, 0] = [forward_last]
    work["d", 0, 0] = [functools.partial(drain_gather, p, wbuf, gsems)]
    work["l", 0, 0] = [loss_slope]
    work["m", 0, 0] = [moments_start]
    work["m", 0, 1] = [moments_ready]
    work["h", 0, 0] = [second_start]
    work["n", 0, 0] = [new_rows]

    def do(names):
        for name in names:
            for f in work.pop(name):
                f()

    def layer_loop(tag, n, body):
        first = ORDER.index((tag, 0, 0))
        do(ORDER[done[0]:first])
        ends = [ORDER.index((tag, l, 0)) for l in range(n)]

        def step(l, _):
            for k in range(1, n):
                names = ORDER[ends[k - 1] + 1:ends[k]]
                if names:
                    pl.when(l == k)(functools.partial(do, names))
            body(l)
            return 0

        lax.fori_loop(0, n, step, 0)
        done[0] = ends[-1] + 1

    done = [0]
    layer_loop("f", layers, forward_one)

    def forward_step(l):
        forward_two(l)

    layer_loop("s", layers - 1, forward_step)
    do(ORDER[done[0]:])
    assert not work
    out = [load(h, hlast, 0), load(lossbuf, loss, 1)]
    for c in out:
        c.start()
    drain_gather(p, wbuf, gsems)
    drain_reduce(p, ring_ab, ring_c, rows, tiles3, rsems)
    wshuf.to_rows_finish()
    mshuf.to_rows_finish()
    for c in out:
        c.wait()


def gradient_slots():
    free, held = list(range(G_SLOTS)), {}
    for tag, n, k in ORDER:
        if tag == "g" and k != 1:
            held[2 * n + (k == 0)] = free.pop(0)
        if tag == "r" and k == 0:
            free.append(held[n])
    return held


def make_step(grid, layers, tok, d_model, d_ff, n_dev):
    nz, ny, nx, nc = grid
    units = 2 * layers
    group = nx * nc
    hbm = pl.BlockSpec(memory_space=pl.ANY)
    sds = jax.ShapeDtypeStruct
    tile = (16, LANES)
    dma = pltpu.SemaphoreType.DMA
    heavy = sum(ORDERS[c][2] == "z" for c in COLOURS)
    recvs = sum(Sems.count(grid, c) for c in COLOURS)
    outs = (sds((layers, 2, d_ff), F32), sds((layers, 4, d_model), F32), sds((layers, 2, d_ff), F32), sds((layers, 4, d_model), F32),
            sds((1, tok), F32), sds((tok, d_model), F32), sds((SPILLED, tok, d_ff), F32))
    shuffled = [pltpu.VMEM((group, layers, 2, LANES), F32), pltpu.VMEM((group // 2, layers, 4, LANES), F32)]
    scratch = [
        pltpu.VMEM((units, *grid, *tile), BF16),
        pltpu.VMEM((2, tok, d_ff), F32),
        pltpu.VMEM((layers, tok, d_model), BF16),
        pltpu.VMEM((layers, tok, d_ff), BF16),
        pltpu.VMEM((tok, d_model), F32),
        pltpu.VMEM((len(LATER) + 1, tok, d_model), BF16),
        pltpu.VMEM((G_SLOTS, *grid, *tile), BF16),
        pltpu.VMEM((units, nz, ny, nx, *tile), BF16),
        pltpu.VMEM((units - heavy, nx - 1, nz, ny, *tile), BF16),
        pltpu.VMEM((heavy, nz - 1, ny, nx, *tile), BF16),
        pltpu.VMEM((units, max(ny, nx) - 1, max(nz, nx), *tile), BF16),
        pltpu.VMEM((units, max(nz, nx) - 1, *tile), BF16),
        *shuffled, *shuffled,
        pltpu.VMEM((layers, 2, d_ff), F32), pltpu.VMEM((layers, 4, d_model), F32),
        pltpu.VMEM((units, *tile), F32), pltpu.VMEM((units, *tile), F32),
        pltpu.VMEM((1, tok), F32),
        dma((7,)), dma((recvs,)), dma((6 + units,)), dma((recvs,)), dma((8,)), dma((4 + SPILLED,)),
    ]
    return pl.pallas_call(
        functools.partial(step_kernel, grid, 1.0 / (n_dev * tok * d_model)),
        out_shape=outs, in_specs=[hbm] * 8, out_specs=[hbm] * 7, scratch_shapes=scratch,
        compiler_params=pltpu.CompilerParams(collective_id=0, has_side_effects=True, vmem_limit_bytes=67043328),
        name="train_step")


def hand_over(*refs):
    n = len(refs) // 2
    for src, dst in zip(refs[:n], refs[n:]):
        if len(dst.shape) < len(src.shape):
            dst[...] = src[0, :]
        else:
            dst[...] = src[...]


def solution(mesh):
    n_dev = mesh.shape["data"]
    w_spec = P(None, "data", None)
    row_spec = P("data", None)

    def device_step(w_one, w_two, mom_one, mom_two, x_zero, y_zero, x_one, y_one):
        tok, d_model = x_zero.shape
        step = make_step(GRID, w_one.shape[0], tok, d_model, w_one.shape[2], n_dev)
        made = step(w_one, w_two, mom_one, mom_two, x_zero, y_zero, x_one, y_one)[:6]
        outs = [jax.ShapeDtypeStruct(v.shape, v.dtype) for v in made]
        outs[4] = jax.ShapeDtypeStruct((tok,), F32)
        vmem = pl.BlockSpec(memory_space=pltpu.VMEM)
        return pl.pallas_call(hand_over, out_shape=tuple(outs), in_specs=[vmem] * 6, out_specs=[vmem] * 6, name="hand_over")(*made)

    return jax.shard_map(device_step, mesh=mesh, in_specs=(w_spec, w_spec, w_spec, w_spec, row_spec, row_spec, row_spec, row_spec),
                         out_specs=(w_spec, w_spec, w_spec, w_spec, P("data"), row_spec), check_vma=False)
```

```python
import functools
import jax
import jax.numpy as jnp
from jax import lax
from jax.experimental import pallas as pl
from jax.experimental.pallas import tpu as pltpu
from jax.sharding import PartitionSpec as P

LEARN_RATE = 0.1
MOMENTUM = 0.9
F32, BF16 = jnp.float32, jnp.bfloat16
GRID = (8, 4, 4, 2)
ORDERS = (("z", "x", "y"), ("z", "y", "x"), ("x", "y", "z"), ("y", "x", "z"))
COLOURS = (0, 1, 0, 1, 2, 3, 0, 1, 2, 0, 1, 3)
GELU_SCALE = 0.7978845608028654
GELU_CUBE = 0.044715
G_SLOTS = 5
LANES = 128
SPILLED = 4
LATER = (2, 3)

ORDER = (
    ("a", 0, 0), ("a", 4, 0), ("a", 5, 0), ("a", 1, 0), ("a", 3, 0), ("m", 0, 0), ("a", 2, 0), ("a", 11, 0), ("a", 8, 0), ("a", 9, 0), ("a", 7, 0),
    ("a", 6, 0), ("a", 4, 1), ("a", 10, 0), ("a", 5, 1), ("a", 8, 1), ("a", 11, 1), ("a", 0, 1), ("a", 1, 1), ("a", 3, 1), ("a", 2, 1), ("a", 4, 2),
    ("a", 5, 2), ("a", 9, 1), ("a", 8, 2), ("a", 11, 2), ("a", 7, 1), ("a", 6, 1), ("a", 10, 1), ("a", 0, 2), ("a", 4, 3), ("a", 1, 2), ("a", 4, 4),
    ("a", 5, 3), ("a", 3, 2), ("a", 2, 2), ("a", 5, 4), ("a", 8, 3), ("a", 8, 4), ("a", 11, 3), ("a", 1, 3), ("a", 11, 4), ("a", 0, 3), ("a", 4, 5),
    ("a", 0, 4), ("a", 1, 4), ("a", 4, 6), ("a", 5, 5), ("a", 7, 2), ("a", 6, 2), ("a", 3, 3), ("a", 2, 3), ("a", 5, 6), ("a", 8, 5), ("a", 3, 4),
    ("a", 2, 4), ("a", 8, 6), ("a", 11, 5), ("a", 1, 5), ("a", 11, 6), ("a", 0, 5), ("a", 9, 2), ("a", 4, 7), ("a", 10, 2), ("a", 1, 6), ("a", 4, 8),
    ("a", 0, 6), ("f", 0, 0), ("a", 5, 7), ("a", 5, 8), ("m", 0, 1), ("a", 3, 5), ("a", 7, 3), ("a", 2, 5), ("a", 6, 3), ("a", 8, 7), ("a", 8, 8),
    ("a", 7, 4), ("a", 11, 7), ("a", 6, 4), ("a", 9, 3), ("a", 10, 3), ("a", 3, 6), ("a", 11, 8), ("a", 2, 6), ("f", 1, 0), ("a", 5, 9), ("a", 4, 9),
    ("a", 8, 9), ("a", 10, 4), ("a", 6, 5), ("a", 11, 9), ("a", 7, 5), ("a", 5, 10), ("a", 9, 4), ("a", 4, 10), ("f", 2, 0), ("a", 6, 6), ("a", 7, 6),
    ("a", 9, 5), ("a", 11, 10), ("f", 3, 0), ("a", 9, 6), ("a", 10, 5), ("a", 8, 10), ("f", 4, 0), ("a", 10, 6), ("f", 5, 0), ("d", 0, 0),
    ("l", 0, 0), ("g", 5, 0), ("g", 5, 1), ("g", 4, 0), ("g", 5, 2), ("g", 4, 1), ("g", 3, 1), ("g", 3, 2), ("g", 3, 0), ("r", 9, 0), ("r", 11, 0),
    ("r", 10, 0), ("g", 4, 2), ("g", 2, 1), ("r", 7, 0), ("r", 11, 1), ("r", 6, 0), ("g", 2, 2), ("r", 11, 2), ("r", 9, 1), ("r", 10, 1), ("g", 2, 0),
    ("r", 9, 2), ("r", 10, 2), ("r", 8, 0), ("g", 1, 0), ("r", 4, 0), ("r", 11, 3), ("g", 1, 1), ("r", 7, 1), ("r", 7, 2), ("r", 6, 1), ("r", 6, 2),
    ("r", 11, 4), ("r", 5, 0), ("g", 0, 0), ("r", 4, 1), ("r", 9, 3), ("r", 10, 3), ("g", 0, 1), ("r", 3, 0), ("h", 0, 0), ("r", 4, 2), ("g", 0, 2),
    ("r", 7, 3), ("r", 11, 5), ("r", 11, 6), ("r", 5, 1), ("r", 8, 1), ("g", 1, 2), ("r", 5, 2), ("r", 6, 3), ("r", 4, 3), ("r", 9, 4), ("r", 0, 0),
    ("r", 4, 4), ("r", 10, 4), ("r", 1, 0), ("r", 3, 1), ("r", 5, 3), ("r", 2, 0), ("r", 3, 2), ("r", 11, 7), ("r", 7, 4), ("r", 5, 4), ("r", 4, 5),
    ("r", 0, 1), ("r", 1, 1), ("r", 6, 4), ("r", 4, 6), ("r", 0, 2), ("r", 8, 2), ("r", 1, 2), ("r", 5, 5), ("r", 2, 1), ("r", 8, 3), ("u", 9, 0),
    ("r", 3, 3), ("r", 5, 6), ("r", 2, 2), ("u", 10, 0), ("r", 4, 7), ("r", 11, 8), ("r", 0, 3), ("r", 1, 3), ("u", 7, 0), ("r", 8, 4), ("r", 5, 7),
    ("r", 2, 3), ("r", 8, 5), ("u", 6, 0), ("r", 3, 4), ("r", 4, 8), ("u", 11, 0), ("r", 8, 6), ("r", 0, 4), ("b", 9, 0), ("r", 8, 7), ("r", 5, 8),
    ("r", 1, 4), ("b", 10, 0), ("r", 2, 4), ("b", 7, 0), ("u", 4, 0), ("b", 11, 0), ("b", 6, 0), ("u", 3, 0), ("r", 8, 8), ("u", 5, 0), ("b", 9, 1),
    ("u", 0, 0), ("b", 10, 1), ("u", 1, 0), ("b", 11, 1), ("u", 2, 0), ("b", 4, 0), ("b", 5, 0), ("b", 6, 1), ("u", 8, 0), ("n", 0, 0), ("b", 7, 1),
    ("b", 3, 0), ("b", 11, 2), ("b", 11, 3), ("b", 0, 0), ("b", 9, 2), ("b", 9, 3), ("b", 4, 1), ("b", 5, 1), ("b", 1, 0), ("b", 8, 0), ("b", 10, 2),
    ("b", 10, 3), ("b", 2, 0), ("b", 11, 4), ("b", 6, 2), ("b", 6, 3), ("b", 4, 2), ("b", 4, 3), ("b", 3, 1), ("b", 5, 2), ("b", 9, 4), ("b", 0, 1),
    ("b", 5, 3), ("b", 10, 4), ("b", 9, 5), ("b", 11, 5), ("b", 11, 6), ("b", 1, 1), ("b", 10, 5), ("b", 4, 4), ("b", 8, 1), ("b", 2, 1), ("b", 6, 4),
    ("b", 5, 4), ("b", 3, 2), ("b", 5, 5), ("b", 11, 7), ("b", 6, 5), ("b", 3, 3), ("b", 0, 2), ("b", 11, 8), ("b", 0, 3), ("b", 1, 2), ("b", 4, 5),
    ("b", 8, 2), ("b", 11, 9), ("b", 8, 3), ("b", 2, 2), ("b", 1, 3), ("b", 7, 2), ("b", 5, 6), ("b", 7, 3), ("b", 5, 7), ("b", 2, 3), ("b", 3, 4),
    ("b", 4, 6), ("b", 4, 7), ("b", 0, 4), ("b", 1, 4), ("b", 8, 4), ("b", 3, 5), ("b", 8, 5), ("b", 2, 4), ("b", 0, 5), ("b", 7, 4), ("b", 1, 5),
    ("s", 0, 0), ("b", 2, 5), ("b", 4, 8), ("b", 7, 5), ("b", 8, 6), ("b", 5, 8), ("s", 1, 0), ("n", 0, 1), ("b", 4, 9), ("b", 8, 7), ("b", 5, 9), ("s", 2, 0),
    ("b", 8, 8), ("s", 3, 0), ("b", 8, 9), ("s", 4, 0), ("s", 5, 0),
)


def start_copy(src, dst, send_sem, recv_sem, dev):
    pltpu.make_async_remote_copy(src_ref=src, dst_ref=dst, send_sem=send_sem, recv_sem=recv_sem,
                                 device_id=(dev,), device_id_type=pl.DeviceIdType.MESH).start()


def wait_bytes(ref, sem):
    pltpu.make_async_copy(ref, ref, sem).wait()


class Place:
    def __init__(self, grid):
        self.grid = grid
        nz, ny, nx, nc = grid
        me = lax.axis_index("data")
        self.me = me
        self.c = lax.rem(me, nc)
        self.x = lax.rem(me // nc, nx)
        self.y = lax.rem(me // (nc * nx), ny)
        self.z = me // (nc * nx * ny)
        self.size = {"z": nz, "y": ny, "x": nx}
        self.pos = {"z": self.z, "y": self.y, "x": self.x}
        self.stride = {"z": ny * nx * nc, "y": nx * nc, "x": nc}
        self.sib = me + 1 - 2 * self.c
        self.m = lax.rem(me, nc * nx)
        self.base = me - self.m

    def wrap(self, v, d):
        n = self.size[d]
        return lax.rem(v + 2 * n, n)

    def dev(self, d, v):
        return self.me + (v - self.pos[d]) * self.stride[d]

    def far(self, d):
        return self.size[d] // 2

    def near(self, d):
        return (self.size[d] - 1) // 2


def block_of(buf, lead, place, done, d, v, tail=()):
    idx = []
    for k in ("z", "y", "x"):
        if k in done:
            idx.append(slice(None))
        elif k == d:
            idx.append(v)
        else:
            idx.append(place.pos[k])
    return buf.at[(*lead, *idx, *tail)]


def half_of(buf, lead, place, d, v, h, tail=()):
    cut = "y" if d == "z" else "z"
    n = place.size[cut] // 2
    idx = [v if k == d else pl.ds(h * n, n) if k == cut else slice(None) for k in ("z", "y", "x")]
    return buf.at[(*lead, *idx, *tail)]


def ring_sem(place, d, way, step):
    return step - 1 if way == 1 else place.far(d) + step - 1


def ring_steps(place, d):
    out = []
    for step in range(1, place.far(d) + 1):
        out.append((1, step))
        if step <= place.near(d):
            out.append((-1, step))
    return out


class Sems:
    def __init__(self, place, colours, send, recv, per_unit):
        self.send, self.recv = send, recv
        self.kind = [int(ORDERS[c][2] == "z") for c in colours]
        self.base, n = [], 0
        for c in colours:
            self.base.append(n)
            n += self.count(place.grid, c)
        self.swaps = per_unit

    @staticmethod
    def count(grid, c):
        return 3 + grid["zyx".index(ORDERS[c][2])] - 1

    def r(self, u, k):
        return self.recv.at[self.base[u] + k]

    def s(self, u, stage):
        if stage == 3:
            return self.send.at[6 + (u if self.swaps else 0)]
        return self.send.at[2 * stage + self.kind[u]]


class Gather:
    def __init__(self, place, buf, u, order, sems):
        self.p, self.buf, self.u, self.order, self.sems = place, buf, u, order, sems

    def block(self, stage, v):
        return block_of(self.buf, (self.u,), self.p, self.order[:stage], self.order[stage], v, (self.p.c,))

    def many(self, stage):
        return self.block(stage, pl.ds(0, self.p.size[self.order[stage]] - 1))

    def direct_start(self, stage):
        p, d = self.p, self.order[stage]
        own = self.block(stage, p.pos[d])
        for k in range(1, p.size[d]):
            start_copy(own, own, self.sems.s(self.u, stage), self.sems.r(self.u, stage), p.dev(d, p.wrap(p.pos[d] + k, d)))

    def direct_wait(self, stage):
        if self.p.size[self.order[stage]] > 1:
            wait_bytes(self.many(stage), self.sems.r(self.u, stage))

    def ring_send(self, way, step):
        p, d = self.p, self.order[2]
        for h in range(2):
            s = way * (1 - 2 * h)
            ref = half_of(self.buf, (self.u,), p, d, p.wrap(p.pos[d] - (step - 1) * s, d), h, (p.c,))
            start_copy(ref, ref, self.sems.s(self.u, 2), self.sems.r(self.u, 3 + ring_sem(p, d, way, step)), p.dev(d, p.wrap(p.pos[d] + s, d)))

    def ring_start(self):
        d = self.order[2]
        for way, n in ((1, self.p.far(d)), (-1, self.p.near(d))):
            if n:
                self.ring_send(way, 1)
        self.swap_start(0)

    def ring_step(self, way, step):
        p, d = self.p, self.order[2]
        n = p.far(d) if way == 1 else p.near(d)
        wait_bytes(self.block(2, 0), self.sems.r(self.u, 3 + ring_sem(p, d, way, step)))
        if step < n:
            self.ring_send(way, step + 1)
        if way == -1:
            self.swap_start(step)
            self.swap_start(-step)
        elif step > p.near(d):
            self.swap_start(step)

    def swap_ref(self, c):
        return self.buf.at[self.u, :, :, :, c]

    def swap_start(self, k):
        d = self.order[2]
        ref = self.block(2, self.p.wrap(self.p.pos[d] - k, d))
        start_copy(ref, ref, self.sems.s(self.u, 3), self.sems.r(self.u, 2), self.p.sib)

    def swap_wait(self):
        wait_bytes(self.swap_ref(1 - self.p.c), self.sems.r(self.u, 2))

    def events(self):
        part = functools.partial
        out = [[part(self.direct_start, 0)],
               [part(self.direct_wait, 0), part(self.direct_start, 1)],
               [part(self.direct_wait, 1), self.ring_start]]
        out += [[part(self.ring_step, way, step)] for way, step in ring_steps(self.p, self.order[2])]
        return out + [[self.swap_wait]]


def drain_gather(place, buf, sems):
    nz, ny, nx, nc = place.grid
    heavy = sum(sems.kind)
    light = len(sems.kind) - heavy
    sent = (buf.at[0:light, 0:nz - 1, 0, 0, 0], buf.at[0:heavy, 0, 0, 0:nx - 1, 0],
            buf.at[0:light, :, 0:nx - 1, 0, 0], buf.at[0:heavy, 0, 0:nx - 1, :, 0],
            buf.at[0:light, :, 0:ny - 1, :, 0], buf.at[0:heavy, 0:nz - 1, :, :, 0], buf.at[:, :, :, :, 0])
    for k, ref in enumerate(sent):
        wait_bytes(ref, sems.send.at[k])


def add_into(dst, *srcs):
    total = dst[...].astype(F32)
    for s in srcs:
        total = total + s[...].astype(F32)
    dst[...] = total.astype(BF16)


class Reduce:
    def __init__(self, place, g, gslot, part, ring, rows, tiles, u, order, sems):
        self.p, self.g, self.gslot, self.part, self.u, self.order, self.sems = place, g, gslot, part, u, order, sems
        self.ring = ring
        n0 = place.size[order[0]]
        self.rows = lambda k: rows.at[k, pl.ds(0, n0)]
        self.tiles = lambda k: tiles.at[k]

    def block(self, stage, v):
        return block_of(self.part, (self.u,), self.p, self.order[:stage], self.order[stage], v)

    def swap_start(self):
        start_copy(self.g.at[self.gslot, :, :, :, 1 - self.p.c], self.part.at[self.u],
                   self.sems.s(self.u, 3), self.sems.r(self.u, 2), self.p.sib)

    def swap_wait(self):
        wait_bytes(self.part.at[self.u], self.sems.r(self.u, 2))
        p = self.p

        def add(k, _):
            add_into(self.part.at[self.u, k], self.g.at[self.gslot, k, :, :, p.c])
            return 0

        lax.fori_loop(0, p.size["z"], add, 0)
        wait_bytes(self.part.at[self.u], self.sems.s(self.u, 3))

    def count(self, way):
        d = self.order[2]
        return self.p.far(d) if way == 1 else self.p.near(d)

    def half(self, k, h):
        ref = self.ring(k)
        n = ref.shape[0] // 2
        return ref.at[pl.ds(h * n, n)]

    def own_half(self, way, ahead, h):
        p, d = self.p, self.order[2]
        return half_of(self.part, (self.u,), p, d, p.wrap(p.pos[d] + ahead * way * (1 - 2 * h), d), h)

    def ring_send(self, way, step):
        p, d = self.p, self.order[2]
        k = ring_sem(p, d, way, step)
        for h in range(2):
            src = self.own_half(way, self.count(way), h) if step == 1 else self.half(k - 1, h)
            start_copy(src, self.half(k, h), self.sems.s(self.u, 2), self.sems.r(self.u, 3 + k),
                       p.dev(d, p.wrap(p.pos[d] + way * (1 - 2 * h), d)))

    def ring_start(self):
        for way in (1, -1):
            if self.count(way):
                self.ring_send(way, 1)

    def ring_step(self, way, step):
        p, d = self.p, self.order[2]
        n = self.count(way)
        k = ring_sem(p, d, way, step)
        wait_bytes(self.ring(k), self.sems.r(self.u, 3 + k))
        if step < n:
            for h in range(2):
                add_into(self.half(k, h), self.own_half(way, n - step, h))
            self.ring_send(way, step + 1)
        if way == 1 and step == n:
            add_into(self.block(2, p.pos[d]), *[self.ring(ring_sem(p, d, w, self.count(w))) for w in (1, -1) if self.count(w)])

    def direct_start(self, stage):
        p, d = self.p, self.order[stage]
        land = self.rows if stage == 1 else self.tiles
        for k in range(1, p.size[d]):
            v = p.wrap(p.pos[d] + k, d)
            start_copy(self.block(stage, v), land(k - 1), self.sems.s(self.u, stage), self.sems.r(self.u, stage), p.dev(d, v))

    def direct_wait(self, stage):
        n = self.p.size[self.order[stage]]
        if n > 1:
            wait_bytes((self.rows if stage == 1 else self.tiles)(pl.ds(0, n - 1)), self.sems.r(self.u, stage))

    def row_sum(self):
        self.direct_wait(1)
        n = self.p.size[self.order[1]]
        if n > 1:
            add_into(self.block(1, self.p.pos[self.order[1]]), *[self.rows(k) for k in range(n - 1)])

    def tile_sum(self):
        self.direct_wait(0)
        total = self.block(0, self.p.pos[self.order[0]])[...].astype(F32)
        for k in range(self.p.size[self.order[0]] - 1):
            total = total + self.tiles(k)[...].astype(F32)
        return total.astype(BF16).astype(F32)

    def events(self):
        part = functools.partial
        out = [[self.swap_wait, self.ring_start]]
        out += [[part(self.ring_step, way, step)] for way, step in ring_steps(self.p, self.order[2])]
        out[-1].append(part(self.direct_start, 1))
        return out + [[self.row_sum, part(self.direct_start, 0)]]


def drain_reduce(place, ring_ab, ring_c, rows, tiles, sems):
    nz, ny, nx, nc = place.grid
    heavy = sum(sems.kind)
    light = len(sems.kind) - heavy
    sent = (tiles.at[0:light, 0:nz - 1], tiles.at[0:heavy, 0:nx - 1], rows.at[0:light, :, 0:nz], rows.at[0:heavy, :, 0:nx], ring_ab, ring_c)
    for k, ref in enumerate(sent):
        wait_bytes(ref, sems.send.at[k])


def enter(p):
    barrier = pltpu.get_barrier_semaphore()
    group = p.grid[2] * p.grid[3]
    peers = [p.base + lax.rem(p.m + k, group) for k in range(1, group)]
    for d in ("y", "z"):
        peers += [p.dev(d, p.wrap(p.pos[d] + k, d)) for k in range(1, p.size[d])]
    for peer in peers:
        pl.semaphore_signal(barrier, inc=1, device_id=(peer,), device_id_type=pl.DeviceIdType.MESH)
    pl.semaphore_wait(barrier, len(peers))


def lanes(ref, j):
    return ref.at[:, :, pl.ds(pl.multiple_of(j * LANES, LANES), LANES)]


class Shuffle:
    def __init__(self, place, one, two, sems, k0):
        self.p, self.one, self.two = place, one, two
        self.sem = lambda k: sems.at[k0 + k]
        self.group = place.grid[2] * place.grid[3]
        self.half = self.group // 2
        self.low = (place.m // self.half) * self.half
        self.mine = place.m - self.low

    def to_tiles_start(self, src1, src2):
        p = self.p
        for k in range(1, self.group):
            j = lax.rem(p.m + k, self.group)
            start_copy(lanes(src1, j), self.one.at[p.m], self.sem(0), self.sem(1), p.base + j)
        for k in range(1, self.half):
            j = lax.rem(self.mine + k, self.half)
            start_copy(lanes(src2, j), self.two.at[self.mine], self.sem(2), self.sem(3), p.base + self.low + j)

    def to_tiles_own(self, src1, src2):
        p = self.p
        pltpu.make_async_copy(lanes(src1, p.m), self.one.at[p.m], self.sem(1)).start()
        pltpu.make_async_copy(lanes(src2, self.mine), self.two.at[self.mine], self.sem(3)).start()

    def drain_sends(self):
        wait_bytes(self.one.at[pl.ds(0, self.group - 1)], self.sem(0))
        wait_bytes(self.two.at[pl.ds(0, self.half - 1)], self.sem(2))

    def to_tiles_finish(self, tiles):
        wait_bytes(self.one, self.sem(1))
        wait_bytes(self.two, self.sem(3))
        for l in range(self.one.shape[1]):
            for m in range(self.group):
                tiles[2 * l, 2 * m:2 * m + 2, :] = self.one[m, l]
            for m in range(self.half):
                tiles[2 * l + 1, 4 * m:4 * m + 4, :] = self.two[m, l]

    def put_rows(self, u, tile):
        if u % 2 == 0:
            for m in range(self.group):
                self.one[m, u // 2] = tile[2 * m:2 * m + 2, :]
        else:
            for m in range(self.half):
                self.two[m, u // 2] = tile[4 * m:4 * m + 4, :]

    def to_rows_start(self, dst1, dst2):
        p = self.p
        pltpu.make_async_copy(self.one.at[p.m], lanes(dst1, p.m), self.sem(1)).start()
        pltpu.make_async_copy(self.two.at[self.mine], lanes(dst2, self.mine), self.sem(3)).start()
        for k in range(1, self.group):
            j = lax.rem(p.m + k, self.group)
            start_copy(self.one.at[j], lanes(dst1, p.m), self.sem(0), self.sem(1), p.base + j)
        for k in range(1, self.half):
            j = lax.rem(self.mine + k, self.half)
            start_copy(self.two.at[j], lanes(dst2, self.mine), self.sem(2), self.sem(3), p.base + self.low + j)

    def to_rows_finish(self):
        wait_bytes(self.one, self.sem(1))
        wait_bytes(self.two, self.sem(3))
        self.drain_sends()


def w_one_of(wbuf, l):
    nz, ny, nx, nc = wbuf.shape[1:5]
    cols = [wbuf[2 * l, :, :, m // nc, m % nc].reshape(nz * ny * 16, LANES) for m in range(nx * nc)]
    return jnp.concatenate(cols, axis=1)


def w_two_of(wbuf, l):
    nz, ny, nx, nc = wbuf.shape[1:5]
    half = nx * nc // 2
    cols = []
    for b in range(half):
        pair = [wbuf[2 * l + 1, :, :, (r * half + b) // nc, b % nc].reshape(nz * ny, 1, 16, LANES) for r in range(2)]
        cols.append(jnp.concatenate(pair, axis=1).reshape(nz * ny * 32, LANES))
    return jnp.concatenate(cols, axis=1)


def contract(a, b, da, db):
    return lax.dot_general(a, b, (((da,), (db,)), ((), ())), preferred_element_type=F32)


def gelu_parts(u):
    w = GELU_SCALE + (GELU_SCALE * GELU_CUBE) * (u * u)
    gate = 0.5 + 0.5 * jnp.tanh(u * w)
    return u * gate, gate, w


def gelu(u):
    return gelu_parts(u)[0]


def gelu_slope(u):
    z, gate, w = gelu_parts(u)
    return gate + (z - z * gate) * (6.0 * w - 4.0 * GELU_SCALE)


def step_kernel(grid, batch_scale, w1, w2, m1, m2, x0, y0, x1, y1, nw1, nw2, nm1, nm2, loss, hlast, spill,
                wbuf, before, act, hid, h, dlow, g, part, ring_ab, ring_c, rows, tiles3,
                wone, wtwo, mone, mtwo, wrow1, wrow2, wt, mt, lossbuf,
                gsend, grecv, rsend, rrecv, shuf, local):
    p = Place(grid)
    layers = w1.shape[0]
    units = 2 * layers
    nz, ny, nx, nc = grid
    tok, d_model = h.shape
    d_ff = hid.shape[2]

    def load(src, dst, k):
        return pltpu.make_async_copy(src, dst, local.at[k])

    loads = {"x0": load(x0, act.at[0], 0), "y0": load(y0, dlow.at[0], 1),
             "x1": load(x1, act.at[layers - 1], 2), "y1": load(y1, act.at[layers - 2], 3)}
    stage = [load(w1, wrow1, 2), load(w2, wrow2, 3)]
    wshuf = Shuffle(p, wone, wtwo, shuf, 0)
    mshuf = Shuffle(p, mone, mtwo, shuf, 4)
    for c in stage:
        c.start()
    wshuf.to_tiles_own(w1, w2)
    mshuf.to_tiles_own(m1, m2)
    loads["x0"].start()
    loads["y0"].start()
    enter(p)
    for c in stage:
        c.wait()
    wshuf.to_tiles_start(wrow1, wrow2)

    def own_tile(u):
        wbuf[u, p.z, p.y, p.x, p.c] = wt[u].astype(BF16)

    wshuf.to_tiles_finish(wt)
    for u in range(units):
        own_tile(u)
    loads["x0"].wait()
    h[...] = act[0].astype(F32)

    def spill_copy(l):
        return load(before.at[lax.rem(l, 2)], spill.at[l], 4 + l)

    def unspill_copy(l):
        return load(spill.at[l], before.at[l % 2], 4 + l)

    def forward_one(l):
        @pl.when(jnp.logical_and(l >= 2, l < SPILLED + 2))
        def _():
            spill_copy(l - 2).wait()

        a = h[...].astype(BF16)
        act[l] = a
        u = jnp.dot(a, w_one_of(wbuf, l), preferred_element_type=F32)
        before[lax.rem(l, 2)] = u
        z = gelu(u).astype(BF16)
        hid[l] = z
        h[...] += jnp.dot(z, w_two_of(wbuf, l), preferred_element_type=F32)

        @pl.when(l < SPILLED)
        def _():
            spill_copy(l).start()

    def loss_slope():
        loads["y0"].wait()
        d = (h[...] - dlow[0].astype(F32)) * batch_scale
        h[...] = d
        dlow[0] = d.astype(BF16)

    gsems = Sems(p, COLOURS, gsend, grecv, False)
    rsems = Sems(p, COLOURS, rsend, rrecv, True)
    slots = gradient_slots()
    first = [Gather(p, wbuf, u, ORDERS[COLOURS[u]], gsems) for u in range(units)]
    again = [Gather(p, wbuf, u, ORDERS[COLOURS[u]], gsems) for u in range(units)]
    red = []
    for u in range(units):
        n = sum(k == rsems.kind[u] for k in rsems.kind[:u])
        ring = functools.partial(lambda buf, n, k: buf.at[n, k], ring_c if rsems.kind[u] else ring_ab, n)
        red.append(Reduce(p, g, slots[u], part, ring, rows.at[u], tiles3.at[u], u, ORDERS[COLOURS[u]], rsems))

    def slope_of(l):
        return dlow.at[1 + LATER.index(l) if l in LATER else 0]

    def hidden_slope_of(l):
        return hid.at[l + len(LATER) if l in LATER else l]

    def grad_two(l):
        slot = red[2 * l + 1].gslot
        half = nx * nc // 2
        v = contract(hid[l], slope_of(l)[...], 0, 0).astype(BF16).reshape(nz, ny, 2, 16, d_model)
        for b in range(half):
            for r in range(2):
                g[slot, :, :, (r * half + b) // nc, b % nc] = v[:, :, r, :, LANES * b:LANES * b + LANES]
        if l in LATER:
            red[2 * l + 1].swap_start()

    def back_hidden(l):
        if l + 2 < layers:
            unspill_copy(l).wait()
        q = contract(slope_of(l)[...], w_two_of(wbuf, l), 1, 1)
        v = (gelu_slope(before[l % 2]) * q).astype(BF16)
        hidden_slope_of(l)[...] = v
        if l:
            d = h[...] + contract(v, w_one_of(wbuf, l), 1, 1)
            h[...] = d
            slope_of(l - 1)[...] = d.astype(BF16)
        if l not in LATER:
            red[2 * l + 1].swap_start()
        if l >= 2:
            unspill_copy(l - 2).start()

    def grad_one(l):
        slot = red[2 * l].gslot
        v = contract(act[l], hidden_slope_of(l)[...], 0, 0).astype(BF16).reshape(nz, ny, 16, d_ff)
        for m in range(nx * nc):
            g[slot, :, :, m // nc, m % nc] = v[:, :, :, LANES * m:LANES * m + LANES]
        red[2 * l].swap_start()
        if l == layers - 1:
            loads["x1"].start()
        if l == layers - 2:
            loads["y1"].start()

    def update(u):
        total = red[u].tile_sum()
        mom = MOMENTUM * mt[u] + total
        w = wt[u] - LEARN_RATE * mom
        wbuf[u, p.z, p.y, p.x, p.c] = w.astype(BF16)
        wt[u] = w
        mt[u] = mom
        again[u].direct_start(0)

    def moments_start():
        mshuf.to_tiles_start(m1, m2)

    def moments_ready():
        mshuf.to_tiles_finish(mt)
        mshuf.drain_sends()
        wshuf.drain_sends()

    def second_start():
        loads["x1"].wait()
        h[...] = act[layers - 1].astype(F32)

    def forward_two(l):
        z = gelu(jnp.dot(h[...].astype(BF16), w_one_of(wbuf, l), preferred_element_type=F32)).astype(BF16)
        v = h[...] + jnp.dot(z, w_two_of(wbuf, l), preferred_element_type=F32)
        h[...] = v
        return v

    def forward_last():
        loads["y1"].wait()
        e = forward_two(layers - 1) - act[layers - 2].astype(F32)
        e = e * e
        s = e[:, :LANES]
        for k in range(1, d_model // LANES):
            s = s + e[:, LANES * k:LANES * k + LANES]
        lossbuf[...] = jnp.sum(s.T, axis=0, keepdims=True) * (1.0 / (2 * d_model))

    def new_rows():
        for u in range(units):
            wshuf.put_rows(u, wt[u])
            mshuf.put_rows(u, mt[u])

    def send_rows():
        wshuf.to_rows_start(nw1, nw2)
        mshuf.to_rows_start(nm1, nm2)

    work = {}
    for u in range(units):
        for k, ev in enumerate(first[u].events()):
            work["a", u, k] = ev
        for k, ev in enumerate(red[u].events()):
            work["r", u, k] = ev
        work["u", u, 0] = [functools.partial(update, u)]
        for k, ev in enumerate(again[u].events()[1:]):
            work["b", u, k] = ev
    for l in range(layers):
        work["g", l, 0] = [functools.partial(grad_two, l)]
        work["g", l, 1] = [functools.partial(back_hidden, l)]
        work["g", l, 2] = [functools.partial(grad_one, l)]
    work["s", layers - 1, 0] = [forward_last]
    work["d", 0, 0] = [functools.partial(drain_gather, p, wbuf, gsems)]
    work["l", 0, 0] = [loss_slope]
    work["m", 0, 0] = [moments_start]
    work["m", 0, 1] = [moments_ready]
    work["h", 0, 0] = [second_start]
    work["n", 0, 0] = [new_rows]
    work["n", 0, 1] = [send_rows]

    def do(names):
        for name in names:
            for f in work.pop(name):
                f()

    def layer_loop(tag, n, body):
        first = ORDER.index((tag, 0, 0))
        do(ORDER[done[0]:first])
        ends = [ORDER.index((tag, l, 0)) for l in range(n)]

        def step(l, _):
            for k in range(1, n):
                names = ORDER[ends[k - 1] + 1:ends[k]]
                if names:
                    pl.when(l == k)(functools.partial(do, names))
            body(l)
            return 0

        lax.fori_loop(0, n, step, 0)
        done[0] = ends[-1] + 1

    done = [0]
    layer_loop("f", layers, forward_one)

    def forward_step(l):
        forward_two(l)

    layer_loop("s", layers - 1, forward_step)
    do(ORDER[done[0]:])
    assert not work
    out = [load(h, hlast, 0), load(lossbuf, loss, 1)]
    for c in out:
        c.start()
    drain_gather(p, wbuf, gsems)
    drain_reduce(p, ring_ab, ring_c, rows, tiles3, rsems)
    wshuf.to_rows_finish()
    mshuf.to_rows_finish()
    for c in out:
        c.wait()


def gradient_slots():
    free, held = list(range(G_SLOTS)), {}
    for tag, n, k in ORDER:
        if tag == "g" and k != 1:
            held[2 * n + (k == 0)] = free.pop(0)
        if tag == "r" and k == 0:
            free.append(held[n])
    return held


def make_step(grid, layers, tok, d_model, d_ff, n_dev):
    nz, ny, nx, nc = grid
    units = 2 * layers
    group = nx * nc
    hbm = pl.BlockSpec(memory_space=pl.ANY)
    sds = jax.ShapeDtypeStruct
    tile = (16, LANES)
    dma = pltpu.SemaphoreType.DMA
    heavy = sum(ORDERS[c][2] == "z" for c in COLOURS)
    recvs = sum(Sems.count(grid, c) for c in COLOURS)
    outs = (sds((layers, 2, d_ff), F32), sds((layers, 4, d_model), F32), sds((layers, 2, d_ff), F32), sds((layers, 4, d_model), F32),
            sds((1, tok), F32), sds((tok, d_model), F32), sds((SPILLED, tok, d_ff), F32))
    shuffled = [pltpu.VMEM((group, layers, 2, LANES), F32), pltpu.VMEM((group // 2, layers, 4, LANES), F32)]
    scratch = [
        pltpu.VMEM((units, *grid, *tile), BF16),
        pltpu.VMEM((2, tok, d_ff), F32),
        pltpu.VMEM((layers, tok, d_model), BF16),
        pltpu.VMEM((layers, tok, d_ff), BF16),
        pltpu.VMEM((tok, d_model), F32),
        pltpu.VMEM((len(LATER) + 1, tok, d_model), BF16),
        pltpu.VMEM((G_SLOTS, *grid, *tile), BF16),
        pltpu.VMEM((units, nz, ny, nx, *tile), BF16),
        pltpu.VMEM((units - heavy, nx - 1, nz, ny, *tile), BF16),
        pltpu.VMEM((heavy, nz - 1, ny, nx, *tile), BF16),
        pltpu.VMEM((units, max(ny, nx) - 1, max(nz, nx), *tile), BF16),
        pltpu.VMEM((units, max(nz, nx) - 1, *tile), BF16),
        *shuffled, *shuffled,
        pltpu.VMEM((layers, 2, d_ff), F32), pltpu.VMEM((layers, 4, d_model), F32),
        pltpu.VMEM((units, *tile), F32), pltpu.VMEM((units, *tile), F32),
        pltpu.VMEM((1, tok), F32),
        dma((7,)), dma((recvs,)), dma((6 + units,)), dma((recvs,)), dma((8,)), dma((4 + SPILLED,)),
    ]
    return pl.pallas_call(
        functools.partial(step_kernel, grid, 1.0 / (n_dev * tok * d_model)),
        out_shape=outs, in_specs=[hbm] * 8, out_specs=[hbm] * 7, scratch_shapes=scratch,
        compiler_params=pltpu.CompilerParams(collective_id=0, has_side_effects=True, vmem_limit_bytes=67043328),
        name="train_step")


def hand_over(*refs):
    n = len(refs) // 2
    for src, dst in zip(refs[:n], refs[n:]):
        if len(dst.shape) < len(src.shape):
            dst[...] = src[0, :]
        else:
            dst[...] = src[...]


def solution(mesh):
    n_dev = mesh.shape["data"]
    w_spec = P(None, "data", None)
    row_spec = P("data", None)

    def device_step(w_one, w_two, mom_one, mom_two, x_zero, y_zero, x_one, y_one):
        tok, d_model = x_zero.shape
        step = make_step(GRID, w_one.shape[0], tok, d_model, w_one.shape[2], n_dev)
        made = step(w_one, w_two, mom_one, mom_two, x_zero, y_zero, x_one, y_one)[:6]
        outs = [jax.ShapeDtypeStruct(v.shape, v.dtype) for v in made]
        outs[4] = jax.ShapeDtypeStruct((tok,), F32)
        vmem = pl.BlockSpec(memory_space=pltpu.VMEM)
        return pl.pallas_call(hand_over, out_shape=tuple(outs), in_specs=[vmem] * 6, out_specs=[vmem] * 6, name="hand_over")(*made)

    return jax.shard_map(device_step, mesh=mesh, in_specs=(w_spec, w_spec, w_spec, w_spec, row_spec, row_spec, row_spec, row_spec),
                         out_specs=(w_spec, w_spec, w_spec, w_spec, P("data"), row_spec), check_vma=False)
```

```python
import functools
import jax
import jax.numpy as jnp
from jax import lax
from jax.experimental import pallas as pl
from jax.experimental.pallas import tpu as pltpu
from jax.sharding import PartitionSpec as P

LEARN_RATE = 0.1
MOMENTUM = 0.9
F32, BF16 = jnp.float32, jnp.bfloat16
GRID = (8, 4, 4, 2)
ORDERS = (("z", "x", "y"), ("z", "y", "x"), ("x", "y", "z"), ("y", "x", "z"))
COLOURS = (0, 1, 0, 1, 2, 3, 0, 1, 2, 0, 1, 3)
GELU_SCALE = 0.7978845608028654
GELU_CUBE = 0.044715
G_SLOTS = 5
LANES = 128
SPILLED = 4
LATER = (2, 3)

ORDER = (
    ("a", 5, 0), ("a", 1, 0), ("a", 4, 0), ("a", 8, 0), ("a", 0, 0), ("m", 0, 0), ("a", 11, 0), ("a", 2, 0), ("a", 3, 0), ("a", 7, 0), ("a", 6, 0),
    ("a", 5, 1), ("a", 4, 1), ("a", 11, 1), ("a", 8, 1), ("a", 10, 0), ("a", 9, 0), ("a", 1, 1), ("a", 0, 1), ("a", 2, 1), ("a", 3, 1), ("a", 5, 2),
    ("a", 4, 2), ("a", 7, 1), ("a", 11, 2), ("a", 6, 1), ("a", 10, 1), ("a", 9, 1), ("a", 1, 2), ("a", 8, 2), ("a", 5, 3), ("a", 0, 2), ("a", 5, 4),
    ("a", 4, 3), ("a", 3, 2), ("a", 2, 2), ("a", 4, 4), ("a", 11, 3), ("a", 11, 4), ("a", 1, 3), ("a", 0, 3), ("a", 5, 5), ("a", 0, 4), ("a", 8, 3),
    ("a", 1, 4), ("a", 5, 6), ("a", 4, 5), ("a", 7, 2), ("a", 2, 3), ("a", 3, 3), ("a", 4, 6), ("a", 6, 2), ("a", 11, 5), ("a", 2, 4), ("a", 3, 4),
    ("a", 11, 6), ("a", 5, 7), ("a", 0, 5), ("a", 1, 5), ("a", 8, 4), ("a", 5, 8), ("a", 8, 5), ("a", 2, 5), ("a", 7, 3), ("a", 0, 6), ("a", 4, 7),
    ("a", 9, 2), ("a", 1, 6), ("f", 0, 0), ("a", 10, 2), ("m", 0, 1), ("a", 7, 4), ("a", 2, 6), ("a", 11, 7), ("a", 11, 8), ("a", 6, 3), ("a", 3, 5),
    ("a", 5, 9), ("a", 4, 8), ("a", 8, 6), ("a", 6, 4), ("a", 8, 7), ("a", 9, 3), ("a", 7, 5), ("a", 3, 6), ("f", 1, 0), ("a", 10, 3), ("a", 5, 10),
    ("a", 4, 9), ("a", 7, 6), ("a", 11, 9), ("a", 9, 4), ("a", 8, 8), ("a", 6, 5), ("a", 8, 9), ("a", 10, 4), ("a", 4, 10), ("f", 2, 0), ("a", 8, 10),
    ("a", 9, 5), ("a", 11, 10), ("a", 6, 6), ("f", 3, 0), ("a", 10, 5), ("a", 9, 6), ("f", 4, 0), ("a", 10, 6), ("f", 5, 0), ("d", 0, 0), ("l", 0, 0),
    ("g", 5, 0), ("g", 5, 1), ("g", 4, 0), ("g", 4, 1), ("g", 4, 2), ("r", 11, 0), ("g", 5, 2), ("r", 9, 0), ("g", 3, 1), ("g", 3, 0), ("r", 11, 1),
    ("r", 11, 2), ("r", 10, 0), ("g", 3, 2), ("r", 9, 1), ("r", 8, 0), ("g", 2, 1), ("r", 9, 2), ("r", 7, 0), ("g", 2, 2), ("r", 10, 1), ("r", 6, 0),
    ("r", 8, 1), ("g", 2, 0), ("r", 9, 3), ("r", 10, 2), ("r", 8, 2), ("g", 1, 0), ("r", 4, 0), ("r", 11, 3), ("r", 11, 4), ("g", 1, 1), ("r", 7, 1),
    ("r", 7, 2), ("r", 8, 3), ("r", 6, 1), ("r", 5, 0), ("g", 1, 2), ("r", 4, 1), ("r", 10, 3), ("r", 6, 2), ("r", 8, 4), ("g", 0, 0), ("r", 4, 2),
    ("r", 3, 0), ("r", 11, 5), ("g", 0, 1), ("r", 9, 4), ("r", 7, 3), ("h", 0, 0), ("r", 11, 6), ("r", 6, 3), ("r", 5, 1), ("r", 8, 5), ("r", 2, 0),
    ("g", 0, 2), ("r", 4, 3), ("r", 5, 2), ("r", 1, 0), ("r", 10, 4), ("r", 8, 6), ("r", 3, 1), ("r", 4, 4), ("r", 0, 0), ("r", 3, 2), ("r", 11, 7),
    ("r", 5, 3), ("r", 7, 4), ("r", 2, 1), ("r", 8, 7), ("r", 6, 4), ("r", 4, 5), ("r", 1, 1), ("u", 9, 0), ("r", 2, 2), ("r", 5, 4), ("r", 1, 2),
    ("r", 0, 1), ("r", 4, 6), ("r", 5, 5), ("r", 3, 3), ("r", 0, 2), ("u", 10, 0), ("r", 2, 3), ("r", 11, 8), ("r", 4, 7), ("r", 1, 3), ("u", 7, 0),
    ("r", 5, 6), ("r", 8, 8), ("u", 6, 0), ("r", 0, 3), ("r", 5, 7), ("b", 9, 0), ("r", 3, 4), ("u", 11, 0), ("r", 2, 4), ("r", 4, 8), ("b", 10, 0),
    ("u", 8, 0), ("r", 1, 4), ("r", 0, 4), ("b", 7, 0), ("r", 5, 8), ("b", 6, 0), ("b", 9, 1), ("b", 11, 0), ("u", 4, 0), ("b", 8, 0), ("u", 3, 0),
    ("b", 10, 1), ("u", 2, 0), ("b", 7, 1), ("u", 5, 0), ("u", 1, 0), ("b", 6, 1), ("u", 0, 0), ("n", 0, 0), ("b", 4, 0), ("b", 11, 1), ("b", 10, 2),
    ("b", 10, 3), ("b", 3, 0), ("b", 8, 1), ("b", 5, 0), ("b", 6, 2), ("b", 7, 2), ("b", 11, 2), ("b", 6, 3), ("b", 1, 0), ("b", 7, 3), ("b", 11, 3),
    ("b", 0, 0), ("b", 8, 2), ("b", 4, 1), ("b", 10, 4), ("b", 8, 3), ("b", 9, 2), ("b", 9, 3), ("b", 2, 0), ("b", 3, 1), ("b", 10, 5), ("b", 5, 1),
    ("b", 6, 4), ("b", 7, 4), ("b", 8, 4), ("b", 6, 5), ("b", 7, 5), ("b", 4, 2), ("b", 1, 1), ("b", 0, 1), ("b", 4, 3), ("b", 9, 4), ("b", 8, 5),
    ("b", 5, 2), ("b", 9, 5), ("b", 3, 2), ("b", 5, 3), ("b", 2, 1), ("b", 8, 6), ("b", 3, 3), ("b", 4, 4), ("b", 4, 5), ("b", 0, 2), ("b", 1, 2),
    ("b", 8, 7), ("b", 0, 3), ("b", 5, 4), ("b", 1, 3), ("b", 5, 5), ("b", 2, 2), ("b", 8, 8), ("b", 11, 4), ("b", 3, 4), ("b", 4, 6), ("b", 2, 3),
    ("b", 8, 9), ("b", 4, 7), ("b", 1, 4), ("b", 3, 5), ("b", 5, 6), ("b", 0, 4), ("b", 5, 7), ("b", 11, 5), ("b", 1, 5), ("b", 11, 6), ("b", 2, 4),
    ("b", 0, 5), ("s", 0, 0), ("b", 5, 8), ("b", 4, 8), ("b", 2, 5), ("s", 1, 0), ("n", 0, 1), ("b", 5, 9), ("b", 4, 9), ("b", 11, 7), ("s", 2, 0), ("b", 11, 8),
    ("s", 3, 0), ("s", 4, 0), ("b", 11, 9), ("s", 5, 0),
)


def start_copy(src, dst, send_sem, recv_sem, dev):
    pltpu.make_async_remote_copy(src_ref=src, dst_ref=dst, send_sem=send_sem, recv_sem=recv_sem,
                                 device_id=(dev,), device_id_type=pl.DeviceIdType.MESH).start()


def wait_bytes(ref, sem):
    pltpu.make_async_copy(ref, ref, sem).wait()


class Place:
    def __init__(self, grid):
        self.grid = grid
        nz, ny, nx, nc = grid
        me = lax.axis_index("data")
        self.me = me
        self.c = lax.rem(me, nc)
        self.x = lax.rem(me // nc, nx)
        self.y = lax.rem(me // (nc * nx), ny)
        self.z = me // (nc * nx * ny)
        self.size = {"z": nz, "y": ny, "x": nx}
        self.pos = {"z": self.z, "y": self.y, "x": self.x}
        self.stride = {"z": ny * nx * nc, "y": nx * nc, "x": nc}
        self.sib = me + 1 - 2 * self.c
        self.m = lax.rem(me, nc * nx)
        self.base = me - self.m

    def wrap(self, v, d):
        n = self.size[d]
        return lax.rem(v + 2 * n, n)

    def dev(self, d, v):
        return self.me + (v - self.pos[d]) * self.stride[d]

    def far(self, d):
        return self.size[d] // 2

    def near(self, d):
        return (self.size[d] - 1) // 2


def block_of(buf, lead, place, done, d, v, tail=()):
    idx = []
    for k in ("z", "y", "x"):
        if k in done:
            idx.append(slice(None))
        elif k == d:
            idx.append(v)
        else:
            idx.append(place.pos[k])
    return buf.at[(*lead, *idx, *tail)]


def half_of(buf, lead, place, d, v, h, tail=()):
    cut = "y" if d == "z" else "z"
    n = place.size[cut] // 2
    idx = [v if k == d else pl.ds(h * n, n) if k == cut else slice(None) for k in ("z", "y", "x")]
    return buf.at[(*lead, *idx, *tail)]


def ring_sem(place, d, way, step):
    return step - 1 if way == 1 else place.far(d) + step - 1


def ring_steps(place, d):
    out = []
    for step in range(1, place.far(d) + 1):
        out.append((1, step))
        if step <= place.near(d):
            out.append((-1, step))
    return out


class Sems:
    def __init__(self, place, colours, send, recv, per_unit):
        self.send, self.recv = send, recv
        self.kind = [int(ORDERS[c][2] == "z") for c in colours]
        self.base, n = [], 0
        for c in colours:
            self.base.append(n)
            n += self.count(place.grid, c)
        self.swaps = per_unit

    @staticmethod
    def count(grid, c):
        return 3 + grid["zyx".index(ORDERS[c][2])] - 1

    def r(self, u, k):
        return self.recv.at[self.base[u] + k]

    def s(self, u, stage):
        if stage == 3:
            return self.send.at[6 + (u if self.swaps else 0)]
        return self.send.at[2 * stage + self.kind[u]]


class Gather:
    def __init__(self, place, buf, u, order, sems):
        self.p, self.buf, self.u, self.order, self.sems = place, buf, u, order, sems

    def block(self, stage, v):
        return block_of(self.buf, (self.u,), self.p, self.order[:stage], self.order[stage], v, (self.p.c,))

    def many(self, stage):
        return self.block(stage, pl.ds(0, self.p.size[self.order[stage]] - 1))

    def direct_start(self, stage):
        p, d = self.p, self.order[stage]
        own = self.block(stage, p.pos[d])
        for k in range(1, p.size[d]):
            start_copy(own, own, self.sems.s(self.u, stage), self.sems.r(self.u, stage), p.dev(d, p.wrap(p.pos[d] + k, d)))

    def direct_wait(self, stage):
        if self.p.size[self.order[stage]] > 1:
            wait_bytes(self.many(stage), self.sems.r(self.u, stage))

    def ring_send(self, way, step):
        p, d = self.p, self.order[2]
        for h in range(2):
            s = way * (1 - 2 * h)
            ref = half_of(self.buf, (self.u,), p, d, p.wrap(p.pos[d] - (step - 1) * s, d), h, (p.c,))
            start_copy(ref, ref, self.sems.s(self.u, 2), self.sems.r(self.u, 3 + ring_sem(p, d, way, step)), p.dev(d, p.wrap(p.pos[d] + s, d)))

    def ring_start(self):
        d = self.order[2]
        for way, n in ((1, self.p.far(d)), (-1, self.p.near(d))):
            if n:
                self.ring_send(way, 1)
        self.swap_start(0)

    def ring_step(self, way, step):
        p, d = self.p, self.order[2]
        n = p.far(d) if way == 1 else p.near(d)
        wait_bytes(self.block(2, 0), self.sems.r(self.u, 3 + ring_sem(p, d, way, step)))
        if step < n:
            self.ring_send(way, step + 1)
        if way == -1:
            self.swap_start(step)
            self.swap_start(-step)
        elif step > p.near(d):
            self.swap_start(step)

    def swap_ref(self, c):
        return self.buf.at[self.u, :, :, :, c]

    def swap_start(self, k):
        d = self.order[2]
        ref = self.block(2, self.p.wrap(self.p.pos[d] - k, d))
        start_copy(ref, ref, self.sems.s(self.u, 3), self.sems.r(self.u, 2), self.p.sib)

    def swap_wait(self):
        wait_bytes(self.swap_ref(1 - self.p.c), self.sems.r(self.u, 2))

    def events(self):
        part = functools.partial
        out = [[part(self.direct_start, 0)],
               [part(self.direct_wait, 0), part(self.direct_start, 1)],
               [part(self.direct_wait, 1), self.ring_start]]
        out += [[part(self.ring_step, way, step)] for way, step in ring_steps(self.p, self.order[2])]
        return out + [[self.swap_wait]]


def drain_gather(place, buf, sems):
    nz, ny, nx, nc = place.grid
    heavy = sum(sems.kind)
    light = len(sems.kind) - heavy
    sent = (buf.at[0:light, 0:nz - 1, 0, 0, 0], buf.at[0:heavy, 0, 0, 0:nx - 1, 0],
            buf.at[0:light, :, 0:nx - 1, 0, 0], buf.at[0:heavy, 0, 0:nx - 1, :, 0],
            buf.at[0:light, :, 0:ny - 1, :, 0], buf.at[0:heavy, 0:nz - 1, :, :, 0], buf.at[:, :, :, :, 0])
    for k, ref in enumerate(sent):
        wait_bytes(ref, sems.send.at[k])


def add_into(dst, *srcs):
    total = dst[...].astype(F32)
    for s in srcs:
        total = total + s[...].astype(F32)
    dst[...] = total.astype(BF16)


class Reduce:
    def __init__(self, place, g, gslot, part, ring, rows, tiles, u, order, sems):
        self.p, self.g, self.gslot, self.part, self.u, self.order, self.sems = place, g, gslot, part, u, order, sems
        self.ring = ring
        n0 = place.size[order[0]]
        self.rows = lambda k: rows.at[k, pl.ds(0, n0)]
        self.tiles = lambda k: tiles.at[k]

    def block(self, stage, v):
        return block_of(self.part, (self.u,), self.p, self.order[:stage], self.order[stage], v)

    def swap_start(self):
        start_copy(self.g.at[self.gslot, :, :, :, 1 - self.p.c], self.part.at[self.u],
                   self.sems.s(self.u, 3), self.sems.r(self.u, 2), self.p.sib)

    def swap_wait(self):
        wait_bytes(self.part.at[self.u], self.sems.r(self.u, 2))
        p = self.p

        def add(k, _):
            add_into(self.part.at[self.u, k], self.g.at[self.gslot, k, :, :, p.c])
            return 0

        lax.fori_loop(0, p.size["z"], add, 0)
        wait_bytes(self.part.at[self.u], self.sems.s(self.u, 3))

    def count(self, way):
        d = self.order[2]
        return self.p.far(d) if way == 1 else self.p.near(d)

    def half(self, k, h):
        ref = self.ring(k)
        n = ref.shape[0] // 2
        return ref.at[pl.ds(h * n, n)]

    def own_half(self, way, ahead, h):
        p, d = self.p, self.order[2]
        return half_of(self.part, (self.u,), p, d, p.wrap(p.pos[d] + ahead * way * (1 - 2 * h), d), h)

    def ring_send(self, way, step):
        p, d = self.p, self.order[2]
        k = ring_sem(p, d, way, step)
        for h in range(2):
            src = self.own_half(way, self.count(way), h) if step == 1 else self.half(k - 1, h)
            start_copy(src, self.half(k, h), self.sems.s(self.u, 2), self.sems.r(self.u, 3 + k),
                       p.dev(d, p.wrap(p.pos[d] + way * (1 - 2 * h), d)))

    def ring_start(self):
        for way in (1, -1):
            if self.count(way):
                self.ring_send(way, 1)

    def ring_step(self, way, step):
        p, d = self.p, self.order[2]
        n = self.count(way)
        k = ring_sem(p, d, way, step)
        wait_bytes(self.ring(k), self.sems.r(self.u, 3 + k))
        if step < n:
            for h in range(2):
                add_into(self.half(k, h), self.own_half(way, n - step, h))
            self.ring_send(way, step + 1)
        if way == 1 and step == n:
            add_into(self.block(2, p.pos[d]), *[self.ring(ring_sem(p, d, w, self.count(w))) for w in (1, -1) if self.count(w)])

    def direct_start(self, stage):
        p, d = self.p, self.order[stage]
        land = self.rows if stage == 1 else self.tiles
        for k in range(1, p.size[d]):
            v = p.wrap(p.pos[d] + k, d)
            start_copy(self.block(stage, v), land(k - 1), self.sems.s(self.u, stage), self.sems.r(self.u, stage), p.dev(d, v))

    def direct_wait(self, stage):
        n = self.p.size[self.order[stage]]
        if n > 1:
            wait_bytes((self.rows if stage == 1 else self.tiles)(pl.ds(0, n - 1)), self.sems.r(self.u, stage))

    def row_sum(self):
        self.direct_wait(1)
        n = self.p.size[self.order[1]]
        if n > 1:
            add_into(self.block(1, self.p.pos[self.order[1]]), *[self.rows(k) for k in range(n - 1)])

    def tile_sum(self):
        self.direct_wait(0)
        total = self.block(0, self.p.pos[self.order[0]])[...].astype(F32)
        for k in range(self.p.size[self.order[0]] - 1):
            total = total + self.tiles(k)[...].astype(F32)
        return total.astype(BF16).astype(F32)

    def events(self):
        part = functools.partial
        out = [[self.swap_wait, self.ring_start]]
        out += [[part(self.ring_step, way, step)] for way, step in ring_steps(self.p, self.order[2])]
        out[-1].append(part(self.direct_start, 1))
        return out + [[self.row_sum, part(self.direct_start, 0)]]


def drain_reduce(place, ring_ab, ring_c, rows, tiles, sems):
    nz, ny, nx, nc = place.grid
    heavy = sum(sems.kind)
    light = len(sems.kind) - heavy
    sent = (tiles.at[0:light, 0:nz - 1], tiles.at[0:heavy, 0:nx - 1], rows.at[0:light, :, 0:nz], rows.at[0:heavy, :, 0:nx], ring_ab, ring_c)
    for k, ref in enumerate(sent):
        wait_bytes(ref, sems.send.at[k])


def enter(p):
    barrier = pltpu.get_barrier_semaphore()
    group = p.grid[2] * p.grid[3]
    peers = [p.base + lax.rem(p.m + k, group) for k in range(1, group)]
    for d in ("y", "z"):
        peers += [p.dev(d, p.wrap(p.pos[d] + k, d)) for k in range(1, p.size[d])]
    for peer in peers:
        pl.semaphore_signal(barrier, inc=1, device_id=(peer,), device_id_type=pl.DeviceIdType.MESH)
    pl.semaphore_wait(barrier, len(peers))


def lanes(ref, j):
    return ref.at[:, :, pl.ds(pl.multiple_of(j * LANES, LANES), LANES)]


class Shuffle:
    def __init__(self, place, one, two, sems, k0):
        self.p, self.one, self.two = place, one, two
        self.sem = lambda k: sems.at[k0 + k]
        self.group = place.grid[2] * place.grid[3]
        self.half = self.group // 2
        self.low = (place.m // self.half) * self.half
        self.mine = place.m - self.low

    def to_tiles_start(self, src1, src2):
        p = self.p
        for k in range(1, self.group):
            j = lax.rem(p.m + k, self.group)
            start_copy(lanes(src1, j), self.one.at[p.m], self.sem(0), self.sem(1), p.base + j)
        for k in range(1, self.half):
            j = lax.rem(self.mine + k, self.half)
            start_copy(lanes(src2, j), self.two.at[self.mine], self.sem(2), self.sem(3), p.base + self.low + j)

    def to_tiles_own(self, src1, src2):
        p = self.p
        pltpu.make_async_copy(lanes(src1, p.m), self.one.at[p.m], self.sem(1)).start()
        pltpu.make_async_copy(lanes(src2, self.mine), self.two.at[self.mine], self.sem(3)).start()

    def drain_sends(self):
        wait_bytes(self.one.at[pl.ds(0, self.group - 1)], self.sem(0))
        wait_bytes(self.two.at[pl.ds(0, self.half - 1)], self.sem(2))

    def to_tiles_finish(self, tiles):
        wait_bytes(self.one, self.sem(1))
        wait_bytes(self.two, self.sem(3))
        for l in range(self.one.shape[1]):
            for m in range(self.group):
                tiles[2 * l, 2 * m:2 * m + 2, :] = self.one[m, l]
            for m in range(self.half):
                tiles[2 * l + 1, 4 * m:4 * m + 4, :] = self.two[m, l]

    def put_rows(self, u, tile):
        if u % 2 == 0:
            for m in range(self.group):
                self.one[m, u // 2] = tile[2 * m:2 * m + 2, :]
        else:
            for m in range(self.half):
                self.two[m, u // 2] = tile[4 * m:4 * m + 4, :]

    def to_rows_start(self, dst1, dst2):
        p = self.p
        pltpu.make_async_copy(self.one.at[p.m], lanes(dst1, p.m), self.sem(1)).start()
        pltpu.make_async_copy(self.two.at[self.mine], lanes(dst2, self.mine), self.sem(3)).start()
        for k in range(1, self.group):
            j = lax.rem(p.m + k, self.group)
            start_copy(self.one.at[j], lanes(dst1, p.m), self.sem(0), self.sem(1), p.base + j)
        for k in range(1, self.half):
            j = lax.rem(self.mine + k, self.half)
            start_copy(self.two.at[j], lanes(dst2, self.mine), self.sem(2), self.sem(3), p.base + self.low + j)

    def to_rows_finish(self):
        wait_bytes(self.one, self.sem(1))
        wait_bytes(self.two, self.sem(3))
        self.drain_sends()


def w_one_of(wbuf, l):
    nz, ny, nx, nc = wbuf.shape[1:5]
    cols = [wbuf[2 * l, :, :, m // nc, m % nc].reshape(nz * ny * 16, LANES) for m in range(nx * nc)]
    return jnp.concatenate(cols, axis=1)


def w_two_of(wbuf, l):
    nz, ny, nx, nc = wbuf.shape[1:5]
    half = nx * nc // 2
    cols = []
    for b in range(half):
        pair = [wbuf[2 * l + 1, :, :, (r * half + b) // nc, b % nc].reshape(nz * ny, 1, 16, LANES) for r in range(2)]
        cols.append(jnp.concatenate(pair, axis=1).reshape(nz * ny * 32, LANES))
    return jnp.concatenate(cols, axis=1)


def contract(a, b, da, db):
    return lax.dot_general(a, b, (((da,), (db,)), ((), ())), preferred_element_type=F32)


def gelu_parts(u):
    w = GELU_SCALE + (GELU_SCALE * GELU_CUBE) * (u * u)
    gate = 0.5 + 0.5 * jnp.tanh(u * w)
    return u * gate, gate, w


def gelu(u):
    return gelu_parts(u)[0]


def gelu_slope(u):
    z, gate, w = gelu_parts(u)
    return gate + (z - z * gate) * (6.0 * w - 4.0 * GELU_SCALE)


def step_kernel(grid, batch_scale, w1, w2, m1, m2, x0, y0, x1, y1, nw1, nw2, nm1, nm2, loss, hlast, spill,
                wbuf, before, act, hid, h, dlow, g, part, ring_ab, ring_c, rows, tiles3,
                wone, wtwo, mone, mtwo, wrow1, wrow2, wt, mt, lossbuf,
                gsend, grecv, rsend, rrecv, shuf, local):
    p = Place(grid)
    layers = w1.shape[0]
    units = 2 * layers
    nz, ny, nx, nc = grid
    tok, d_model = h.shape
    d_ff = hid.shape[2]

    def load(src, dst, k):
        return pltpu.make_async_copy(src, dst, local.at[k])

    loads = {"x0": load(x0, act.at[0], 0), "y0": load(y0, dlow.at[0], 1),
             "x1": load(x1, act.at[layers - 1], 2), "y1": load(y1, act.at[layers - 2], 3)}
    stage = [load(w1, wrow1, 2), load(w2, wrow2, 3)]
    wshuf = Shuffle(p, wone, wtwo, shuf, 0)
    mshuf = Shuffle(p, mone, mtwo, shuf, 4)
    for c in stage:
        c.start()
    wshuf.to_tiles_own(w1, w2)
    mshuf.to_tiles_own(m1, m2)
    loads["x0"].start()
    loads["y0"].start()
    enter(p)
    for c in stage:
        c.wait()
    wshuf.to_tiles_start(wrow1, wrow2)

    def own_tile(u):
        wbuf[u, p.z, p.y, p.x, p.c] = wt[u].astype(BF16)

    wshuf.to_tiles_finish(wt)
    for u in range(units):
        own_tile(u)
    loads["x0"].wait()
    h[...] = act[0].astype(F32)

    def spill_copy(l):
        return load(before.at[lax.rem(l, 2)], spill.at[l], 4 + l)

    def unspill_copy(l):
        return load(spill.at[l], before.at[l % 2], 4 + l)

    def forward_one(l):
        @pl.when(jnp.logical_and(l >= 2, l < SPILLED + 2))
        def _():
            spill_copy(l - 2).wait()

        a = h[...].astype(BF16)
        act[l] = a
        u = jnp.dot(a, w_one_of(wbuf, l), preferred_element_type=F32)
        before[lax.rem(l, 2)] = u
        z = gelu(u).astype(BF16)
        hid[l] = z
        h[...] += jnp.dot(z, w_two_of(wbuf, l), preferred_element_type=F32)

        @pl.when(l < SPILLED)
        def _():
            spill_copy(l).start()

    def loss_slope():
        loads["y0"].wait()
        d = (h[...] - dlow[0].astype(F32)) * batch_scale
        h[...] = d
        dlow[0] = d.astype(BF16)

    gsems = Sems(p, COLOURS, gsend, grecv, False)
    rsems = Sems(p, COLOURS, rsend, rrecv, True)
    slots = gradient_slots()
    first = [Gather(p, wbuf, u, ORDERS[COLOURS[u]], gsems) for u in range(units)]
    again = [Gather(p, wbuf, u, ORDERS[COLOURS[u]], gsems) for u in range(units)]
    red = []
    for u in range(units):
        n = sum(k == rsems.kind[u] for k in rsems.kind[:u])
        ring = functools.partial(lambda buf, n, k: buf.at[n, k], ring_c if rsems.kind[u] else ring_ab, n)
        red.append(Reduce(p, g, slots[u], part, ring, rows.at[u], tiles3.at[u], u, ORDERS[COLOURS[u]], rsems))

    def slope_of(l):
        return dlow.at[1 + LATER.index(l) if l in LATER else 0]

    def hidden_slope_of(l):
        return hid.at[l + len(LATER) if l in LATER else l]

    def grad_two(l):
        slot = red[2 * l + 1].gslot
        half = nx * nc // 2
        v = contract(hid[l], slope_of(l)[...], 0, 0).astype(BF16).reshape(nz, ny, 2, 16, d_model)
        for b in range(half):
            for r in range(2):
                g[slot, :, :, (r * half + b) // nc, b % nc] = v[:, :, r, :, LANES * b:LANES * b + LANES]
        if l in LATER:
            red[2 * l + 1].swap_start()

    def back_hidden(l):
        if l + 2 < layers:
            unspill_copy(l).wait()
        q = contract(slope_of(l)[...], w_two_of(wbuf, l), 1, 1)
        v = (gelu_slope(before[l % 2]) * q).astype(BF16)
        hidden_slope_of(l)[...] = v
        if l:
            d = h[...] + contract(v, w_one_of(wbuf, l), 1, 1)
            h[...] = d
            slope_of(l - 1)[...] = d.astype(BF16)
        if l not in LATER:
            red[2 * l + 1].swap_start()
        if l >= 2:
            unspill_copy(l - 2).start()

    def grad_one(l):
        slot = red[2 * l].gslot
        v = contract(act[l], hidden_slope_of(l)[...], 0, 0).astype(BF16).reshape(nz, ny, 16, d_ff)
        for m in range(nx * nc):
            g[slot, :, :, m // nc, m % nc] = v[:, :, :, LANES * m:LANES * m + LANES]
        red[2 * l].swap_start()
        if l == layers - 1:
            loads["x1"].start()
        if l == layers - 2:
            loads["y1"].start()

    def update(u):
        total = red[u].tile_sum()
        mom = MOMENTUM * mt[u] + total
        w = wt[u] - LEARN_RATE * mom
        wbuf[u, p.z, p.y, p.x, p.c] = w.astype(BF16)
        wt[u] = w
        mt[u] = mom
        again[u].direct_start(0)

    def moments_start():
        mshuf.to_tiles_start(m1, m2)

    def moments_ready():
        mshuf.to_tiles_finish(mt)
        mshuf.drain_sends()
        wshuf.drain_sends()

    def second_start():
        loads["x1"].wait()
        h[...] = act[layers - 1].astype(F32)

    def forward_two(l):
        z = gelu(jnp.dot(h[...].astype(BF16), w_one_of(wbuf, l), preferred_element_type=F32)).astype(BF16)
        v = h[...] + jnp.dot(z, w_two_of(wbuf, l), preferred_element_type=F32)
        h[...] = v
        return v

    def forward_last():
        loads["y1"].wait()
        e = forward_two(layers - 1) - act[layers - 2].astype(F32)
        e = e * e
        s = e[:, :LANES]
        for k in range(1, d_model // LANES):
            s = s + e[:, LANES * k:LANES * k + LANES]
        lossbuf[...] = jnp.sum(s.T, axis=0, keepdims=True) * (1.0 / (2 * d_model))

    def new_rows():
        for u in range(units):
            wshuf.put_rows(u, wt[u])
            mshuf.put_rows(u, mt[u])

    def send_rows():
        wshuf.to_rows_start(nw1, nw2)
        mshuf.to_rows_start(nm1, nm2)

    work = {}
    for u in range(units):
        for k, ev in enumerate(first[u].events()):
            work["a", u, k] = ev
        for k, ev in enumerate(red[u].events()):
            work["r", u, k] = ev
        work["u", u, 0] = [functools.partial(update, u)]
        for k, ev in enumerate(again[u].events()[1:]):
            work["b", u, k] = ev
    for l in range(layers):
        work["g", l, 0] = [functools.partial(grad_two, l)]
        work["g", l, 1] = [functools.partial(back_hidden, l)]
        work["g", l, 2] = [functools.partial(grad_one, l)]
    work["s", layers - 1, 0] = [forward_last]
    work["d", 0, 0] = [functools.partial(drain_gather, p, wbuf, gsems)]
    work["l", 0, 0] = [loss_slope]
    work["m", 0, 0] = [moments_start]
    work["m", 0, 1] = [moments_ready]
    work["h", 0, 0] = [second_start]
    work["n", 0, 0] = [new_rows]
    work["n", 0, 1] = [send_rows]

    def do(names):
        for name in names:
            for f in work.pop(name):
                f()

    def layer_loop(tag, n, body):
        first = ORDER.index((tag, 0, 0))
        do(ORDER[done[0]:first])
        ends = [ORDER.index((tag, l, 0)) for l in range(n)]

        def step(l, _):
            for k in range(1, n):
                names = ORDER[ends[k - 1] + 1:ends[k]]
                if names:
                    pl.when(l == k)(functools.partial(do, names))
            body(l)
            return 0

        lax.fori_loop(0, n, step, 0)
        done[0] = ends[-1] + 1

    done = [0]
    layer_loop("f", layers, forward_one)

    def forward_step(l):
        forward_two(l)

    layer_loop("s", layers - 1, forward_step)
    do(ORDER[done[0]:])
    assert not work
    out = [load(h, hlast, 0), load(lossbuf, loss, 1)]
    for c in out:
        c.start()
    drain_gather(p, wbuf, gsems)
    drain_reduce(p, ring_ab, ring_c, rows, tiles3, rsems)
    wshuf.to_rows_finish()
    mshuf.to_rows_finish()
    for c in out:
        c.wait()


def gradient_slots():
    free, held = list(range(G_SLOTS)), {}
    for tag, n, k in ORDER:
        if tag == "g" and k != 1:
            held[2 * n + (k == 0)] = free.pop(0)
        if tag == "r" and k == 0:
            free.append(held[n])
    return held


def make_step(grid, layers, tok, d_model, d_ff, n_dev):
    nz, ny, nx, nc = grid
    units = 2 * layers
    group = nx * nc
    hbm = pl.BlockSpec(memory_space=pl.ANY)
    sds = jax.ShapeDtypeStruct
    tile = (16, LANES)
    dma = pltpu.SemaphoreType.DMA
    heavy = sum(ORDERS[c][2] == "z" for c in COLOURS)
    recvs = sum(Sems.count(grid, c) for c in COLOURS)
    outs = (sds((layers, 2, d_ff), F32), sds((layers, 4, d_model), F32), sds((layers, 2, d_ff), F32), sds((layers, 4, d_model), F32),
            sds((1, tok), F32), sds((tok, d_model), F32), sds((SPILLED, tok, d_ff), F32))
    shuffled = [pltpu.VMEM((group, layers, 2, LANES), F32), pltpu.VMEM((group // 2, layers, 4, LANES), F32)]
    scratch = [
        pltpu.VMEM((units, *grid, *tile), BF16),
        pltpu.VMEM((2, tok, d_ff), F32),
        pltpu.VMEM((layers, tok, d_model), BF16),
        pltpu.VMEM((layers, tok, d_ff), BF16),
        pltpu.VMEM((tok, d_model), F32),
        pltpu.VMEM((len(LATER) + 1, tok, d_model), BF16),
        pltpu.VMEM((G_SLOTS, *grid, *tile), BF16),
        pltpu.VMEM((units, nz, ny, nx, *tile), BF16),
        pltpu.VMEM((units - heavy, nx - 1, nz, ny, *tile), BF16),
        pltpu.VMEM((heavy, nz - 1, ny, nx, *tile), BF16),
        pltpu.VMEM((units, max(ny, nx) - 1, max(nz, nx), *tile), BF16),
        pltpu.VMEM((units, max(nz, nx) - 1, *tile), BF16),
        *shuffled, *shuffled,
        pltpu.VMEM((layers, 2, d_ff), F32), pltpu.VMEM((layers, 4, d_model), F32),
        pltpu.VMEM((units, *tile), F32), pltpu.VMEM((units, *tile), F32),
        pltpu.VMEM((1, tok), F32),
        dma((7,)), dma((recvs,)), dma((6 + units,)), dma((recvs,)), dma((8,)), dma((4 + SPILLED,)),
    ]
    return pl.pallas_call(
        functools.partial(step_kernel, grid, 1.0 / (n_dev * tok * d_model)),
        out_shape=outs, in_specs=[hbm] * 8, out_specs=[hbm] * 7, scratch_shapes=scratch,
        compiler_params=pltpu.CompilerParams(collective_id=0, has_side_effects=True, vmem_limit_bytes=67043328),
        name="train_step")


def hand_over(*refs):
    n = len(refs) // 2
    for src, dst in zip(refs[:n], refs[n:]):
        if len(dst.shape) < len(src.shape):
            dst[...] = src[0, :]
        else:
            dst[...] = src[...]


def solution(mesh):
    n_dev = mesh.shape["data"]
    w_spec = P(None, "data", None)
    row_spec = P("data", None)

    def device_step(w_one, w_two, mom_one, mom_two, x_zero, y_zero, x_one, y_one):
        tok, d_model = x_zero.shape
        step = make_step(GRID, w_one.shape[0], tok, d_model, w_one.shape[2], n_dev)
        made = step(w_one, w_two, mom_one, mom_two, x_zero, y_zero, x_one, y_one)[:6]
        outs = [jax.ShapeDtypeStruct(v.shape, v.dtype) for v in made]
        outs[4] = jax.ShapeDtypeStruct((tok,), F32)
        vmem = pl.BlockSpec(memory_space=pltpu.VMEM)
        return pl.pallas_call(hand_over, out_shape=tuple(outs), in_specs=[vmem] * 6, out_specs=[vmem] * 6, name="hand_over")(*made)

    return jax.shard_map(device_step, mesh=mesh, in_specs=(w_spec, w_spec, w_spec, w_spec, row_spec, row_spec, row_spec, row_spec),
                         out_specs=(w_spec, w_spec, w_spec, w_spec, P("data"), row_spec), check_vma=False)
```
